32 devices in a mesh: pipe: 2 (over x), dp: 8 (over z, y), tensor: 2 (over core).
Axes of the slice: x: 2, y: 2, z: 4, core: 2. Of those that a mesh axis runs over, the one named last changes fastest.
Arguments:
- inputs: bfloat16 [2, 8, 256, 1536], P(None, 'dp'), may hold values from -6 to 6
- cotangents: bfloat16 [2, 8, 256, 1536], P(None, 'dp'), may hold values from -6 to 6
- norm_scales: float32 [2, 1536, 2], P('pipe'), may hold values from 0.5 to 1.5
- w_query: bfloat16 [2, 1536, 1536], P('pipe', None, 'tensor'), may hold values from -0.15625 to 0.15625
- key_weight: bfloat16 [2, 1536, 768], P('pipe', None, 'tensor'), may hold values from -0.15625 to 0.15625
- value_weight: bfloat16 [2, 1536, 768], P('pipe', None, 'tensor'), may hold values from -0.15625 to 0.15625
- w_out: bfloat16 [2, 1536, 1536], P('pipe', None, 'tensor'), may hold values from -0.875 to 0.875
- w_gate: bfloat16 [2, 1536, 4096], P('pipe', None, 'tensor'), may hold values from -0.15625 to 0.15625
- w_up: bfloat16 [2, 1536, 4096], P('pipe', None, 'tensor'), may hold values from -0.15625 to 0.15625
- down_weight: bfloat16 [2, 1536, 4096], P('pipe', None, 'tensor'), may hold values from -0.09375 to 0.09375
Outputs:
- section_out: bfloat16 [2, 2, 8, 256, 1536], P('pipe', None, 'dp')
- section_in_grad: bfloat16 [2, 2, 8, 256, 1536], P('pipe', None, 'dp')
- grad_scales: float32 [2, 1536, 2], P('pipe', 'dp')
- grad_query: float32 [2, 1536, 1536], P('pipe', 'dp', 'tensor')
- grad_key: float32 [2, 1536, 768], P('pipe', 'dp', 'tensor')
- value_weight_gradient: float32 [2, 1536, 768], P('pipe', 'dp', 'tensor')
- grad_out: float32 [2, 1536, 1536], P('pipe', 'dp', 'tensor')
- grad_gate: float32 [2, 1536, 4096], P('pipe', 'dp', 'tensor')
- grad_up: float32 [2, 1536, 4096], P('pipe', 'dp', 'tensor')
- grad_down: float32 [2, 1536, 4096], P('pipe', 'dp', 'tensor')
The draws below stay inside these ranges and needn't reach their ends.
All inputs are finite; a program needn't handle non-finite values.
Results may differ from the reference program's by a relative error of at most 0.03.
Values may be sent and summed in bfloat16 or wider, within the bound.
A program may use at most 256 MiB of HBM per device.

```python
import jax
import jax.numpy as jnp
from jax import lax

MODEL_WIDTH = 1536
HQ = 16
KEY_VALUE_HEADS = 8
HEAD_SIZE = 96
FF = 4096
SEQ = 256
MICRO = 2
SEQS = 8
SECTION_COUNT = 2


def spiked(values, own_key, source, target, shards_of, factor):
    def block_of(dim):
        return (jnp.arange(values.shape[dim]) // (values.shape[dim] // shards_of)).reshape((-1,) + (1,) * (values.ndim - 1 - dim))

    first = jax.random.permutation(own_key, shards_of)[block_of(target)]
    far = (block_of(target) + shards_of // 2) % shards_of
    return jnp.where((block_of(source) == first) | (block_of(source) == far), factor * values, values)


def block_levels(key, shape, shards, low, largest):
    factor_of, own = 1.0, jax.random.fold_in(key, 6)
    for axis_at, parts in shards:
        draws = jnp.exp(jax.random.uniform(jax.random.fold_in(own, axis_at), (parts,), jnp.float32, low / len(shards), largest / len(shards)))
        factor_of = factor_of * jnp.repeat(draws, shape[axis_at] // parts).reshape([-1 if axis == axis_at else 1 for axis in range(len(shape))])
    return factor_of


def scatter_about(own_key, extent, spread, limit, split=(), kind=jnp.bfloat16):
    drawn = spread * jax.random.normal(own_key, extent, jnp.float32)
    if split:
        drawn = drawn * block_levels(own_key, extent, split, -0.22, 0.18)
    return jnp.clip(drawn, -limit, limit).astype(kind)


def noise_with(key, shape, width, most, cuts, heavy, held_as=jnp.bfloat16):
    drawn = width * jax.random.normal(key, shape, jnp.float32)
    if cuts:
        drawn = drawn * block_levels(key, shape, cuts, -0.22, 0.18)
    return jnp.clip(spiked(drawn, jax.random.fold_in(key, 3), *heavy), -most, most).astype(held_as)


def setup_inputs(seed: int = 0) -> dict:
    streams_of = jax.random.split(jax.random.key(seed), 11)
    inputs = noise_with(streams_of[0], (MICRO, SEQS, SEQ, MODEL_WIDTH), 1.0, 6.0, ((1, 8),), (1, 3, 8, 2.0))
    cotangents = noise_with(streams_of[1], (MICRO, SEQS, SEQ, MODEL_WIDTH), 1.0, 6.0, ((1, 8),), (1, 3, 8, 2.0))
    norm_scales = jnp.clip(1.0 + 0.1 * jax.random.normal(streams_of[2], (SECTION_COUNT, MODEL_WIDTH, 2), jnp.float32), 0.5, 1.5)
    w_query = scatter_about(streams_of[3], (SECTION_COUNT, MODEL_WIDTH, HQ * HEAD_SIZE), MODEL_WIDTH ** -0.5, 0.15625, ((0, 2), (2, 2)))
    key_weight = scatter_about(streams_of[4], (SECTION_COUNT, MODEL_WIDTH, KEY_VALUE_HEADS * HEAD_SIZE), MODEL_WIDTH ** -0.5, 0.15625, ((0, 2), (2, 2)))
    value_weight = scatter_about(streams_of[5], (SECTION_COUNT, MODEL_WIDTH, KEY_VALUE_HEADS * HEAD_SIZE), MODEL_WIDTH ** -0.5, 0.15625, ((0, 2), (2, 2)))
    w_out = scatter_about(streams_of[6], (SECTION_COUNT, MODEL_WIDTH, HQ * HEAD_SIZE), (HQ * HEAD_SIZE * 8 // SEQ) ** -0.5, 0.875, ((0, 2), (2, 2)))
    w_gate = scatter_about(streams_of[7], (SECTION_COUNT, MODEL_WIDTH, FF), MODEL_WIDTH ** -0.5, 0.15625, ((0, 2), (2, 2)))
    w_up = scatter_about(streams_of[8], (SECTION_COUNT, MODEL_WIDTH, FF), MODEL_WIDTH ** -0.5, 0.15625, ((0, 2), (2, 2)))
    down_weight = scatter_about(streams_of[9], (SECTION_COUNT, MODEL_WIDTH, FF), FF ** -0.5, 0.09375, ((0, 2), (2, 2)))
    return dict(inputs=inputs, cotangents=cotangents, norm_scales=norm_scales, w_query=w_query, key_weight=key_weight, value_weight=value_weight, w_out=w_out, w_gate=w_gate, w_up=w_up, down_weight=down_weight)


EPS = 1e-05
THETA = 100000.0

def rope_tables(length, size):
    positions = jnp.arange(length, dtype=jnp.float32)
    freqs = THETA ** (-(jnp.arange(size // 2, dtype=jnp.float32) * 2.0 / size))
    angles = positions[:, None] * freqs[None, :]
    cosine = jnp.concatenate([jnp.cos(angles), jnp.cos(angles)], axis=-1)
    sine = jnp.concatenate([jnp.sin(angles), jnp.sin(angles)], axis=-1)
    return (cosine[:, None, :], sine[:, None, :])

def rotate(values, cosine, sine):
    half = values.shape[-1] // 2
    turned = jnp.concatenate([-values[..., half:], values[..., :half]], axis=-1)
    return values * cosine + turned * sine

def rotate_back(grads, cosine, sine):
    half = grads.shape[-1] // 2
    moved = grads * sine
    turned = jnp.concatenate([moved[..., half:], -moved[..., :half]], axis=-1)
    return grads * cosine + turned

def rounded(values):
    return lax.optimization_barrier(values.astype(jnp.bfloat16))

def times_t(left, right):
    return lax.dot_general(left, right, (((1,), (1,)), ((), ())), preferred_element_type=jnp.float32)

def over_rows(left, right):
    return lax.dot_general(left, right, (((0,), (0,)), ((), ())), preferred_element_type=jnp.float32)

def norm_rows(values, gain):
    scale = lax.rsqrt(lax.optimization_barrier(jnp.mean(values * values, axis=-1, keepdims=True)) + EPS)
    return (scale, rounded(values * scale * gain))

def score_table(query, keys):
    length = query.shape[0]
    scores = jnp.einsum('qgrd,kgd->grqk', query.astype(jnp.float32), keys.astype(jnp.float32)) * HEAD_SIZE ** (-0.5)
    causal = jnp.arange(length)[:, None] >= jnp.arange(length)[None, :]
    return (scores, causal)

def forward_layer(hidden, params):
    scales, w_query, key_weight, value_weight, w_out, w_gate, w_up, down_weight = params
    length = hidden.shape[0]
    groups = key_weight.shape[1] // HEAD_SIZE
    wide = hidden.astype(jnp.float32)
    scale_one, normed_one = norm_rows(wide, scales[:, 0])
    cosine, sine = rope_tables(length, HEAD_SIZE)
    query = rounded(rotate(jnp.dot(normed_one, w_query, preferred_element_type=jnp.float32).reshape(length, -1, HEAD_SIZE), cosine, sine)).reshape(length, groups, -1, HEAD_SIZE)
    keys = rounded(rotate(jnp.dot(normed_one, key_weight, preferred_element_type=jnp.float32).reshape(length, groups, HEAD_SIZE), cosine, sine))
    values = rounded(jnp.dot(normed_one, value_weight, preferred_element_type=jnp.float32)).reshape(length, groups, HEAD_SIZE)
    scores, causal = score_table(query, keys)
    log_total = jnp.log(lax.optimization_barrier(jnp.sum(jnp.where(causal, jnp.exp(scores), 0.0), axis=-1)))
    probs = rounded(jnp.where(causal, jnp.exp(scores - log_total[..., None]), 0.0))
    mixed = rounded(jnp.einsum('grqk,kgd->qgrd', probs.astype(jnp.float32), values.astype(jnp.float32))).reshape(length, -1)
    middle = wide + times_t(mixed, w_out)
    scale_two, normed_two = norm_rows(middle, scales[:, 1])
    gate = jnp.dot(normed_two, w_gate, preferred_element_type=jnp.float32)
    upward = jnp.dot(normed_two, w_up, preferred_element_type=jnp.float32)
    activated = rounded(gate * jax.nn.sigmoid(gate) * upward)
    result = (middle + times_t(activated, down_weight)).astype(jnp.bfloat16)
    record = (hidden, scale_one, normed_one, query, keys, values, mixed, log_total, middle, scale_two, normed_two, gate, upward, activated)
    return (record, result)

def backward_layer(record, cotangent, params):
    hidden, scale_one, normed_one, query, keys, values, mixed, log_total, middle, scale_two, normed_two, gate, upward, activated = record
    scales, w_query, key_weight, value_weight, w_out, w_gate, w_up, down_weight = params
    length = hidden.shape[0]
    groups = keys.shape[1]
    grad_down = over_rows(cotangent, activated)
    d_act = jnp.dot(cotangent, down_weight, preferred_element_type=jnp.float32)
    sig = jax.nn.sigmoid(gate)
    d_gate = rounded(d_act * upward * sig * (1.0 + gate * (1.0 - sig)))
    d_up = rounded(d_act * gate * sig)
    grad_gate = over_rows(normed_two, d_gate)
    grad_up = over_rows(normed_two, d_up)
    d_normed = times_t(d_gate, w_gate) + times_t(d_up, w_up)
    weighted = d_normed * scales[:, 1]
    gain_two = lax.optimization_barrier(jnp.sum(d_normed * middle * scale_two, axis=0))
    d_middle = cotangent.astype(jnp.float32) + scale_two * weighted - middle * scale_two ** 3 * lax.optimization_barrier(jnp.mean(weighted * middle, axis=-1, keepdims=True))
    d_mid_low = rounded(d_middle)
    grad_out = over_rows(d_mid_low, mixed)
    d_mixed = rounded(jnp.dot(d_mid_low, w_out, preferred_element_type=jnp.float32))
    d_heads = d_mixed.astype(jnp.float32).reshape(length, groups, -1, HEAD_SIZE)
    scores, causal = score_table(query, keys)
    probs = jnp.where(causal, jnp.exp(scores - log_total[..., None]), 0.0)
    probs_low = rounded(probs).astype(jnp.float32)
    d_probs = jnp.einsum('qgrd,kgd->grqk', d_heads, values.astype(jnp.float32))
    d_values = jnp.einsum('grqk,qgrd->kgd', probs_low, d_heads)
    delta = lax.optimization_barrier(jnp.sum(d_heads * mixed.astype(jnp.float32).reshape(length, groups, -1, HEAD_SIZE), axis=-1))
    d_scores = rounded(probs * (d_probs - jnp.transpose(delta, (1, 2, 0))[..., None]) * HEAD_SIZE ** (-0.5)).astype(jnp.float32)
    cosine, sine = rope_tables(length, HEAD_SIZE)
    d_query = rounded(rotate_back(jnp.einsum('grqk,kgd->qgrd', d_scores, keys.astype(jnp.float32)).reshape(length, -1, HEAD_SIZE), cosine, sine)).reshape(length, -1)
    d_keys = rounded(rotate_back(jnp.einsum('grqk,qgrd->kgd', d_scores, query.astype(jnp.float32)), cosine, sine)).reshape(length, -1)
    d_vals = rounded(d_values).reshape(length, -1)
    grad_query = over_rows(normed_one, d_query)
    grad_key = over_rows(normed_one, d_keys)
    value_weight_gradient = over_rows(normed_one, d_vals)
    d_first = times_t(d_query, w_query) + times_t(d_keys, key_weight) + times_t(d_vals, value_weight)
    weighted_one = d_first * scales[:, 0]
    wide = hidden.astype(jnp.float32)
    gain_one = lax.optimization_barrier(jnp.sum(d_first * wide * scale_one, axis=0))
    d_hidden = (d_middle + scale_one * weighted_one - wide * scale_one ** 3 * lax.optimization_barrier(jnp.mean(weighted_one * wide, axis=-1, keepdims=True))).astype(jnp.bfloat16)
    gain_grads = jnp.stack([gain_one, gain_two], axis=1)
    return (d_hidden, (gain_grads, grad_query, grad_key, value_weight_gradient, grad_out, grad_gate, grad_up, grad_down))

def reference(inputs, cotangents, norm_scales, w_query, key_weight, value_weight, w_out, w_gate, w_up, down_weight):
    every = (norm_scales, w_query, key_weight, value_weight, w_out, w_gate, w_up, down_weight)
    section_zero = tuple((item[0] for item in every))
    section_one = tuple((item[1] for item in every))
    count = MICRO * SEQS
    sources = inputs.reshape(count, SEQ, MODEL_WIDTH)
    targets = cotangents.reshape(count, SEQ, MODEL_WIDTH)

    def one_sequence(carry, pair):
        source, target = pair
        record_zero, out_zero = forward_layer(source, section_zero)
        record_one, out_one = forward_layer(out_zero, section_one)
        grad_one, parts_one = backward_layer(record_one, target, section_one)
        grad_zero, parts_zero = backward_layer(record_zero, grad_one, section_zero)
        carry = jax.tree.map(lambda total, extra: total + extra, carry, (parts_zero, parts_one))
        return (carry, (out_zero, out_one, grad_zero, grad_one))
    start = jax.tree.map(lambda item: jnp.zeros(item.shape, jnp.float32), (section_zero, section_one))
    sums, outputs = lax.scan(one_sequence, start, (sources, targets))
    out_zero, out_one, grad_zero, grad_one = outputs
    section_out = jnp.stack([out_zero, out_one]).reshape(2, MICRO, SEQS, SEQ, MODEL_WIDTH)
    section_in_grad = jnp.stack([grad_zero, grad_one]).reshape(2, MICRO, SEQS, SEQ, MODEL_WIDTH)
    grads = [jnp.stack([left, right]) for left, right in zip(sums[0], sums[1])]
    return (section_out, section_in_grad, grads[0], grads[1], grads[2], grads[3], grads[4], grads[5], grads[6], grads[7])
```

```python
import jax
import jax.numpy as jnp
from jax import lax
from jax.experimental import pallas as pl
from jax.experimental.pallas import tpu as pltpu
from jax.sharding import PartitionSpec as P

HEAD_SIZE = 96


EPS = 1e-05
THETA = 100000.0


def passed_along(value, axis, by):
    peers = lax.axis_size(axis)
    pairs = [(i, i + by) for i in range(peers) if 0 <= i + by < peers]
    return lax.ppermute(value, axis, pairs)


def rope_tables(length, size):
    positions = jnp.arange(length, dtype=jnp.float32)
    freqs = THETA ** (-(jnp.arange(size // 2, dtype=jnp.float32) * 2.0 / size))
    angles = positions[:, None] * freqs[None, :]
    cosine = jnp.concatenate([jnp.cos(angles), jnp.cos(angles)], axis=-1)
    sine = jnp.concatenate([jnp.sin(angles), jnp.sin(angles)], axis=-1)
    return (cosine[:, None, :], sine[:, None, :])


def rotate(values, cosine, sine):
    half = values.shape[-1] // 2
    turned = jnp.concatenate([-values[..., half:], values[..., :half]], axis=-1)
    return values * cosine + turned * sine


def rotate_back(grads, cosine, sine):
    half = grads.shape[-1] // 2
    moved = grads * sine
    turned = jnp.concatenate([moved[..., half:], -moved[..., :half]], axis=-1)
    return grads * cosine + turned


def times_t(left, right):
    return lax.dot_general(
        left, right, (((1,), (1,)), ((), ())), preferred_element_type=jnp.float32
    )


def over_rows(left, right):
    return lax.dot_general(
        left, right, (((0,), (0,)), ((), ())), preferred_element_type=jnp.float32
    )


def heads_total(partial_value):
    low = partial_value.astype(jnp.bfloat16)
    total = low.astype(jnp.float32)
    peers = lax.axis_size("tensor")
    for by in range(1, peers):
        other = lax.ppermute(low, "tensor", [(i, (i + by) % peers) for i in range(peers)])
        total = total + other.astype(jnp.float32)
    return total


inputs_total = heads_total


def bit_orders(bits):
    plain = list(range(bits))
    if bits < 2:
        return [plain]
    swapped = [1, 0] + plain[2:]
    return [plain, plain, plain, swapped]


def halving_kernel(widths, blocks, bits, axis, *refs):
    count = len(widths)
    grads, outs = refs[:count], refs[count : 2 * count]
    rest = refs[2 * count :]
    local, got = rest[:count], rest[count : count + count * bits]
    load_sem, send_sem, recv_sem = rest[count + count * bits :]
    me = lax.axis_index(axis)
    own = [lax.rem(lax.div(me, 2**bit), 2) for bit in range(bits)]
    flip = [me + (1 - 2 * own[bit]) * 2**bit for bit in range(bits)]
    barrier = pltpu.get_barrier_semaphore()
    for bit in range(bits):
        pl.semaphore_signal(
            barrier, inc=1, device_id={axis: flip[bit]}, device_id_type=pl.DeviceIdType.MESH
        )
    pl.semaphore_wait(barrier, bits)
    orders = bit_orders(bits)
    chunks = []
    for which, width in enumerate(widths):
        for at in range(grads[which].shape[-1] // width):
            chunks.append((which, at))
    plans = [orders[number % len(orders)] for number in range(len(chunks))]

    def place(fixed, free):
        return tuple(fixed[bit] if bit in fixed else slice(None) for bit in reversed(range(bits)))

    loads, sends = [], {}
    for number, (which, at) in enumerate(chunks):
        first = plans[number][0]
        width = widths[which]
        columns = pl.ds(at * width, width)
        theirs = place({first: 1 - own[first]}, None)
        mine = place({first: own[first]}, None)
        send = pltpu.make_async_remote_copy(
            src_ref=grads[which].at[theirs + (slice(None), columns)],
            dst_ref=got[which * bits].at[at],
            send_sem=send_sem.at[number, 0],
            recv_sem=recv_sem.at[number, 0],
            device_id={axis: flip[first]},
            device_id_type=pl.DeviceIdType.MESH,
        )
        send.start()
        sends[number, 0] = send
        load = pltpu.make_async_copy(
            grads[which].at[mine + (slice(None), columns)], local[which].at[at], load_sem.at[number]
        )
        load.start()
        loads.append(load)

    def step(number, level):
        which, at = chunks[number]
        order = plans[number]
        width = widths[which]
        block = blocks[which]
        if level == 0:
            loads[number].wait()
        sends[number, level].wait_recv()
        done = order[: level + 1]
        left = [bit for bit in reversed(range(bits)) if bit not in done]
        before = [bit for bit in reversed(range(bits)) if bit not in order[:level]]
        received = got[which * bits + level].at[at]
        kept_first = order[0]
        axes = [bit for bit in reversed(range(bits)) if bit != kept_first]
        rows = block if block % 64 else 64

        def view(fixed):
            return tuple(fixed[bit] for bit in axes)

        for combo in range(2 ** len(left)):
            fixed = {bit: (combo >> index) & 1 for index, bit in enumerate(left)}
            for bit in done:
                fixed[bit] = own[bit]
            spot = view(fixed)
            from_spot = tuple(fixed[bit] for bit in left)

            def add(piece, _):
                where = pl.ds(pl.multiple_of(piece * rows, rows), rows)
                a = local[which][(at,) + spot + (where, slice(None))].astype(jnp.float32)
                b = received[from_spot + (where, slice(None))].astype(jnp.float32)
                if level == bits - 1:
                    outs[which][where, pl.ds(at * width, width)] = (a + b).astype(jnp.bfloat16)
                else:
                    local[which][(at,) + spot + (where, slice(None))] = (a + b).astype(jnp.bfloat16)
                return 0

            lax.fori_loop(0, block // rows, add, 0)
        if level < bits - 1:
            following = order[level + 1]
            source = []
            for bit in axes:
                if bit in done:
                    source.append(own[bit])
                elif bit == following:
                    source.append(1 - own[bit])
                else:
                    source.append(slice(None))
            send = pltpu.make_async_remote_copy(
                src_ref=local[which].at[(at,) + tuple(source)],
                dst_ref=got[which * bits + level + 1].at[at],
                send_sem=send_sem.at[number, level + 1],
                recv_sem=recv_sem.at[number, level + 1],
                device_id={axis: flip[following]},
                device_id_type=pl.DeviceIdType.MESH,
            )
            send.start()
            sends[number, level + 1] = send

    for tick in range(len(chunks) + bits - 1):
        for level in range(bits):
            number = tick - level
            if 0 <= number < len(chunks):
                step(number, level)
    for send in sends.values():
        send.wait_send()


def scattered(grads, axis):
    peers = lax.axis_size(axis)
    bits = peers.bit_length() - 1
    blocks = [grad.shape[0] // peers for grad in grads]
    widths = []
    for grad in grads:
        columns = grad.shape[1]
        widths.append(next(w for w in (256, 384, 128) if columns % w == 0))
    shaped = [
        grad.reshape((2,) * bits + (block, grad.shape[1])) for grad, block in zip(grads, blocks)
    ]
    pieces = [grad.shape[1] // width for grad, width in zip(grads, widths)]
    scratch = [
        pltpu.VMEM((piece,) + (2,) * (bits - 1) + (block, width), jnp.bfloat16)
        for piece, block, width in zip(pieces, blocks, widths)
    ]
    for piece, block, width in zip(pieces, blocks, widths):
        for level in range(bits):
            scratch.append(
                pltpu.VMEM((piece,) + (2,) * (bits - 1 - level) + (block, width), jnp.bfloat16)
            )
    total = sum(pieces)
    scratch += [
        pltpu.SemaphoreType.DMA((total,)),
        pltpu.SemaphoreType.DMA((total, bits)),
        pltpu.SemaphoreType.DMA((total, bits)),
    ]

    def kernel(*refs):
        halving_kernel(widths, blocks, bits, axis, *refs)

    return pl.pallas_call(
        kernel,
        out_shape=[
            jax.ShapeDtypeStruct((block, grad.shape[1]), jnp.bfloat16)
            for grad, block in zip(grads, blocks)
        ],
        in_specs=[pl.BlockSpec(memory_space=pl.ANY)] * len(grads),
        out_specs=[pl.BlockSpec(memory_space=pltpu.VMEM)] * len(grads),
        scratch_shapes=scratch,
        compiler_params=pltpu.CompilerParams(
            collective_id=0, has_side_effects=True, vmem_limit_bytes=60 * 2**20
        ),
    )(*shaped)


def norm_rows(values, gain):
    scale = lax.rsqrt(jnp.mean(values * values, axis=-1, keepdims=True) + EPS)
    return (scale, (values * scale * gain).astype(jnp.bfloat16))


def score_table(query, keys):
    length = query.shape[0]
    scores = jnp.einsum(
        "qgrd,kgd->grqk", query, keys, preferred_element_type=jnp.float32
    ) * HEAD_SIZE ** (-0.5)
    causal = jnp.arange(length)[:, None] >= jnp.arange(length)[None, :]
    return (scores, causal)


def forward_layer(hidden, params):
    scales, w_query, key_weight, value_weight, w_out, w_gate, w_up, down_weight = params
    length = hidden.shape[0]
    groups = key_weight.shape[1] // HEAD_SIZE
    wide = hidden.astype(jnp.float32)
    scale_one, normed_one = norm_rows(wide, scales[:, 0])
    cosine, sine = rope_tables(length, HEAD_SIZE)
    query = (
        rotate(
            jnp.dot(normed_one, w_query, preferred_element_type=jnp.float32).reshape(
                length, -1, HEAD_SIZE
            ),
            cosine,
            sine,
        )
        .astype(jnp.bfloat16)
        .reshape(length, groups, -1, HEAD_SIZE)
    )
    keys = rotate(
        jnp.dot(normed_one, key_weight, preferred_element_type=jnp.float32).reshape(
            length, groups, HEAD_SIZE
        ),
        cosine,
        sine,
    ).astype(jnp.bfloat16)
    values = (
        jnp.dot(normed_one, value_weight, preferred_element_type=jnp.float32)
        .astype(jnp.bfloat16)
        .reshape(length, groups, HEAD_SIZE)
    )
    scores, causal = score_table(query, keys)
    log_total = jnp.log(jnp.sum(jnp.where(causal, jnp.exp(scores), 0.0), axis=-1))
    probs = jnp.where(causal, jnp.exp(scores - log_total[..., None]), 0.0).astype(jnp.bfloat16)
    mixed = (
        jnp.einsum("grqk,kgd->qgrd", probs, values, preferred_element_type=jnp.float32)
        .astype(jnp.bfloat16)
        .reshape(length, -1)
    )
    middle = wide + heads_total(times_t(mixed, w_out))
    scale_two, normed_two = norm_rows(middle, scales[:, 1])
    gate = jnp.dot(normed_two, w_gate, preferred_element_type=jnp.float32)
    upward = jnp.dot(normed_two, w_up, preferred_element_type=jnp.float32)
    activated = (gate * jax.nn.sigmoid(gate) * upward).astype(jnp.bfloat16)
    result = (middle + heads_total(times_t(activated, down_weight))).astype(jnp.bfloat16)
    record = (
        hidden,
        scale_one,
        normed_one,
        query,
        keys,
        values,
        mixed,
        log_total,
        middle,
        scale_two,
        normed_two,
        gate,
        upward,
        activated,
    )
    return (record, result)


def backward_feedforward(record, cotangent, params):
    (
        hidden,
        scale_one,
        normed_one,
        query,
        keys,
        values,
        mixed,
        log_total,
        middle,
        scale_two,
        normed_two,
        gate,
        upward,
        activated,
    ) = record
    scales, w_query, key_weight, value_weight, w_out, w_gate, w_up, down_weight = params
    d_act = jnp.dot(cotangent, down_weight, preferred_element_type=jnp.float32)
    sig = jax.nn.sigmoid(gate)
    d_gate = (d_act * upward * sig * (1.0 + gate * (1.0 - sig))).astype(jnp.bfloat16)
    d_up = (d_act * gate * sig).astype(jnp.bfloat16)
    d_normed = inputs_total(times_t(d_gate, w_gate) + times_t(d_up, w_up))
    weighted = d_normed * scales[:, 1]
    gain_two = jnp.sum(d_normed * middle * scale_two, axis=0)
    d_middle = (
        cotangent.astype(jnp.float32)
        + scale_two * weighted
        - middle * scale_two**3 * jnp.mean(weighted * middle, axis=-1, keepdims=True)
    )
    return (d_middle, (normed_two, d_gate, d_up, cotangent, activated, gain_two))


def backward_attention(record, d_middle, params):
    (
        hidden,
        scale_one,
        normed_one,
        query,
        keys,
        values,
        mixed,
        log_total,
        middle,
        scale_two,
        normed_two,
        gate,
        upward,
        activated,
    ) = record
    scales, w_query, key_weight, value_weight, w_out, w_gate, w_up, down_weight = params
    length = hidden.shape[0]
    groups = keys.shape[1]
    d_mid_low = d_middle.astype(jnp.bfloat16)
    d_mixed = jnp.dot(d_mid_low, w_out, preferred_element_type=jnp.float32).astype(jnp.bfloat16)
    d_heads = d_mixed.reshape(length, groups, -1, HEAD_SIZE)
    scores, causal = score_table(query, keys)
    probs = jnp.where(causal, jnp.exp(scores - log_total[..., None]), 0.0)
    d_probs = jnp.einsum("qgrd,kgd->grqk", d_heads, values, preferred_element_type=jnp.float32)
    d_values = jnp.einsum(
        "grqk,qgrd->kgd", probs.astype(jnp.bfloat16), d_heads, preferred_element_type=jnp.float32
    )
    delta = jnp.sum(
        d_heads.astype(jnp.float32)
        * mixed.reshape(length, groups, -1, HEAD_SIZE).astype(jnp.float32),
        axis=-1,
    )
    d_scores = (
        probs * (d_probs - jnp.transpose(delta, (1, 2, 0))[..., None]) * HEAD_SIZE ** (-0.5)
    ).astype(jnp.bfloat16)
    cosine, sine = rope_tables(length, HEAD_SIZE)
    d_query = (
        rotate_back(
            jnp.einsum(
                "grqk,kgd->qgrd", d_scores, keys, preferred_element_type=jnp.float32
            ).reshape(length, -1, HEAD_SIZE),
            cosine,
            sine,
        )
        .astype(jnp.bfloat16)
        .reshape(length, -1)
    )
    d_keys = (
        rotate_back(
            jnp.einsum("grqk,qgrd->kgd", d_scores, query, preferred_element_type=jnp.float32),
            cosine,
            sine,
        )
        .astype(jnp.bfloat16)
        .reshape(length, -1)
    )
    d_vals = d_values.astype(jnp.bfloat16).reshape(length, -1)
    d_first = inputs_total(
        times_t(d_query, w_query) + times_t(d_keys, key_weight) + times_t(d_vals, value_weight)
    )
    weighted_one = d_first * scales[:, 0]
    wide = hidden.astype(jnp.float32)
    gain_one = jnp.sum(d_first * wide * scale_one, axis=0)
    d_hidden = (
        d_middle
        + scale_one * weighted_one
        - wide * scale_one**3 * jnp.mean(weighted_one * wide, axis=-1, keepdims=True)
    ).astype(jnp.bfloat16)
    return (d_hidden, (normed_one, d_query, d_keys, d_vals, d_mid_low, mixed, gain_one))


def body(
    inputs,
    cotangents,
    norm_scales,
    w_query,
    key_weight,
    value_weight,
    w_out,
    w_gate,
    w_up,
    down_weight,
):
    params = (
        norm_scales[0],
        w_query[0],
        key_weight[0],
        value_weight[0],
        w_out[0],
        w_gate[0],
        w_up[0],
        down_weight[0],
    )
    section_index = lax.axis_index("pipe")
    is_first = section_index == 0
    micros = inputs.shape[0]
    length = inputs.shape[2]
    width = inputs.shape[3]
    incoming = jnp.zeros((length, width), jnp.bfloat16)
    saved = []
    results = []
    for step_index in range(micros + 1):
        own_input = inputs[min(step_index, micros - 1), 0]
        record, result = forward_layer(jnp.where(is_first, own_input, incoming), params)
        saved.append(record)
        results.append(result)
        if step_index < micros:
            incoming = passed_along(result, "pipe", 1)
    stacked = jax.tree.map(lambda *entries: jnp.stack(entries), *saved)
    returned = jnp.zeros((length, width), jnp.bfloat16)
    in_grads = []
    parts = []
    for step_index in range(micros + 1):
        micro_index = step_index - 1 + section_index
        slot_index = jnp.clip(micro_index + section_index, 0, micros)
        record = jax.tree.map(
            lambda entry: lax.dynamic_index_in_dim(entry, slot_index, 0, keepdims=False), stacked
        )
        cotangent = jnp.where(is_first, returned, cotangents[min(step_index, micros - 1), 0])
        d_middle, ffn_part = backward_feedforward(record, cotangent, params)
        d_hidden, attn_part = backward_attention(record, d_middle, params)
        parts.append(ffn_part + attn_part)
        in_grads.append(d_hidden)
        if step_index < micros:
            returned = passed_along(d_hidden, "pipe", -1)
    kept = jax.tree.map(
        lambda *entries: lax.dynamic_slice_in_dim(
            jnp.stack(entries), 1 - section_index, micros, 0
        ),
        *parts,
    )
    (
        normed_two,
        d_gate,
        d_up,
        cotangent,
        activated,
        gain_two,
        normed_one,
        d_query,
        d_keys,
        d_vals,
        d_mid_low,
        mixed,
        gain_one,
    ) = (entry.reshape(-1, entry.shape[-1]) for entry in kept)
    dp_size = lax.axis_size("dp")
    gains = jnp.stack([gain_one.sum(axis=0), gain_two.sum(axis=0)], axis=1)
    gains = gains.astype(jnp.bfloat16).reshape(dp_size, -1)
    gain_size = gains.shape[1]
    gains = jnp.pad(gains, ((0, 0), (0, 2048 - gain_size))).reshape(dp_size * 16, 128)
    grads = [
        over_rows(normed_one, d_query),
        over_rows(normed_one, d_keys),
        over_rows(normed_one, d_vals),
        over_rows(d_mid_low, mixed),
        over_rows(normed_two, d_gate),
        over_rows(normed_two, d_up),
        over_rows(cotangent, activated),
    ]
    shards = scattered([gains] + [grad.astype(jnp.bfloat16) for grad in grads], "dp")
    shards = [shard.astype(jnp.float32) for shard in shards]
    grad_scales = shards[0].reshape(-1)[:gain_size].reshape(1, -1, 2)
    shards = [shard[None] for shard in shards[1:]]
    (
        grad_query,
        grad_key,
        value_weight_gradient,
        grad_out,
        grad_gate,
        grad_up,
        grad_down,
    ) = shards
    section_out = lax.dynamic_slice_in_dim(jnp.stack(results), section_index, micros, 0).reshape(
        1, micros, 1, length, width
    )
    section_in_grad = lax.dynamic_slice_in_dim(
        jnp.stack(in_grads), 1 - section_index, micros, 0
    ).reshape(1, micros, 1, length, width)
    return (
        section_out,
        section_in_grad,
        grad_scales,
        grad_query,
        grad_key,
        value_weight_gradient,
        grad_out,
        grad_gate,
        grad_up,
        grad_down,
    )


def solution(mesh):
    placed = (
        P(None, "dp", None, None),
        P(None, "dp", None, None),
        P("pipe", None, None),
        P("pipe", None, "tensor"),
        P("pipe", None, "tensor"),
        P("pipe", None, "tensor"),
        P("pipe", None, "tensor"),
        P("pipe", None, "tensor"),
        P("pipe", None, "tensor"),
        P("pipe", None, "tensor"),
    )
    return jax.shard_map(
        body,
        mesh=mesh,
        in_specs=placed,
        out_specs=(
            P("pipe", None, "dp", None, None),
            P("pipe", None, "dp", None, None),
            P("pipe", "dp", None),
            P("pipe", "dp", "tensor"),
            P("pipe", "dp", "tensor"),
            P("pipe", "dp", "tensor"),
            P("pipe", "dp", "tensor"),
            P("pipe", "dp", "tensor"),
            P("pipe", "dp", "tensor"),
            P("pipe", "dp", "tensor"),
        ),
        check_vma=False,
    )
```

```python
import functools

import jax
import jax.numpy as jnp
import numpy as np
from jax import lax
from jax.experimental import pallas as pl
from jax.experimental.pallas import tpu as pltpu
from jax.sharding import PartitionSpec as P

HEAD_SIZE = 96
HALF = HEAD_SIZE // 2
LANES = 128
HIDDEN_STEPS = 4
SEND_PIECES = 3

EPS = 1e-05
THETA = 100000.0
MESH = pl.DeviceIdType.MESH
MIB = 2**20
SCALE = HEAD_SIZE ** (-0.5)


def rope_tables(length):
    freqs = (THETA ** (-(np.arange(HALF, dtype=np.float64) * 2.0 / HEAD_SIZE))).astype(np.float32)
    angles = np.arange(length, dtype=np.float32)[:, None] * freqs[None, :]
    cosine, sine = np.cos(angles), np.sin(angles)
    room = np.zeros((length, LANES // 2 - HALF), np.float32)
    cosines = np.concatenate([cosine, room, cosine, room], axis=1)
    sines = np.concatenate([-sine, room, sine, room], axis=1)
    return np.stack([cosines, sines]).astype(np.float32)


def dot(left, right):
    return lax.dot_general(
        left, right, (((1,), (0,)), ((), ())), preferred_element_type=jnp.float32
    )


def times_t(left, right):
    return lax.dot_general(
        left, right, (((1,), (1,)), ((), ())), preferred_element_type=jnp.float32
    )


def over_rows(left, right):
    return lax.dot_general(
        left, right, (((0,), (0,)), ((), ())), preferred_element_type=jnp.float32
    )


def spread(values, head):
    room = jnp.zeros((values.shape[0], LANES // 2 - HALF), values.dtype)
    at = head * HEAD_SIZE
    return jnp.concatenate(
        [values[:, at : at + HALF], room, values[:, at + HALF : at + HEAD_SIZE], room], axis=1
    )


def gathered(heads):
    parts = []
    for head in heads:
        parts += [head[:, :HALF], head[:, LANES // 2 : LANES // 2 + HALF]]
    return jnp.concatenate(parts, axis=1)


def turned(values, cosine, sine):
    return values * cosine + pltpu.roll(values, LANES // 2, 1) * sine


def turned_back(values, cosine, sine):
    return values * cosine - pltpu.roll(values, LANES // 2, 1) * sine


def rsqrt_mean(values):
    return lax.rsqrt(jnp.mean(values * values, axis=-1, keepdims=True) + EPS)


class Exchange:
    def __init__(self, number, send, got, send_sem, recv_sem):
        self.number, self.send, self.got = number, send, got
        self.send_sem, self.recv_sem = send_sem, recv_sem
        self.width = send.shape[1] // SEND_PIECES

    def copy(self, piece):
        columns = pl.ds(piece * self.width, self.width)
        return pltpu.make_async_remote_copy(
            src_ref=self.send.at[:, columns],
            dst_ref=self.got.at[self.number, :, columns],
            send_sem=self.send_sem.at[self.number, piece],
            recv_sem=self.recv_sem.at[self.number, piece],
            device_id={"tensor": 1 - lax.axis_index("tensor")},
            device_id_type=MESH,
        )

    def start(self, piece, partial_value):
        columns = pl.ds(piece * self.width, self.width)
        self.send[:, columns] = partial_value.astype(jnp.bfloat16)
        self.copy(piece).start()

    def wait(self):
        for piece in range(SEND_PIECES):
            self.copy(piece).wait()

    def total(self):
        return self.send[...].astype(jnp.float32) + self.got[self.number].astype(jnp.float32)


def half_copy(source, target, rows, send_sem, recv_sem, device):
    return pltpu.make_async_remote_copy(
        src_ref=source.at[rows],
        dst_ref=target.at[rows],
        send_sem=send_sem,
        recv_sem=recv_sem,
        device_id=device,
        device_id_type=MESH,
    )


def passed_on(xin, micro, sems, stage_from):
    tensor = lax.axis_index("tensor")
    rows = xin.shape[1] // 2
    send_sem, recv_sem, pair_send, pair_recv = sems
    slot = xin.at[micro]
    mine = pl.ds(pl.multiple_of(tensor * rows, rows), rows)
    theirs = pl.ds(pl.multiple_of((1 - tensor) * rows, rows), rows)
    half_copy(
        slot, slot, mine, send_sem.at[micro], recv_sem.at[micro], {"pipe": stage_from}
    ).wait_recv()
    copy = half_copy(
        slot, slot, mine, pair_send.at[micro], pair_recv.at[micro], {"tensor": 1 - tensor}
    )
    copy.start()
    half_copy(
        slot, slot, theirs, pair_send.at[micro], pair_recv.at[micro], {"tensor": 1 - tensor}
    ).wait_recv()
    copy.wait_send()


def sent_on(source, xin, micro, sems, stage_to):
    tensor = lax.axis_index("tensor")
    rows = xin.shape[1] // 2
    mine = pl.ds(pl.multiple_of(tensor * rows, rows), rows)
    return half_copy(
        source.at[micro], xin.at[micro], mine, sems[0].at[micro], sems[1].at[micro], {"pipe": stage_to}
    )


def greet(devices):
    barrier = pltpu.get_barrier_semaphore()
    for device in devices:
        pl.semaphore_signal(barrier, inc=1, device_id=device, device_id_type=MESH)
    pl.semaphore_wait(barrier, len(devices))


def forward_kernel(
    own,
    micros,
    inp,
    cot,
    gains,
    tables,
    wq,
    wk,
    wv,
    wo,
    wg,
    wu,
    wd,
    result_out,
    hidden_out,
    n1_out,
    q_out,
    k_out,
    v_out,
    o_out,
    middle_out,
    n2_out,
    gate_out,
    up_out,
    act_out,
    other_out,
    other,
    xin,
    res,
    send,
    got,
    middle,
    acc,
    n2_buf,
    send_sem,
    recv_sem,
    x_send,
    x_recv,
    xp_send,
    xp_recv,
    far_send,
    far_recv,
    near_send,
    near_recv,
):
    micro, step = pl.program_id(0), pl.program_id(1)
    pipe, tensor, data = lax.axis_index("pipe"), lax.axis_index("tensor"), lax.axis_index("dp")
    peers = lax.axis_size("dp")
    partner = lax.rem(data + peers // 2, peers)
    sems = (x_send, x_recv, xp_send, xp_recv)
    length = inp.shape[1]

    def far_copy(source):
        return pltpu.make_async_remote_copy(
            src_ref=source.at[tensor],
            dst_ref=other.at[tensor],
            send_sem=far_send,
            recv_sem=far_recv,
            device_id={"dp": partner},
            device_id_type=MESH,
        )

    def near_copy(which):
        return pltpu.make_async_remote_copy(
            src_ref=other.at[which],
            dst_ref=other.at[which],
            send_sem=near_send,
            recv_sem=near_recv,
            device_id={"tensor": 1 - tensor},
            device_id_type=MESH,
        )

    @pl.when((micro == 0) & (step == 0))
    def _():
        greet([{"tensor": 1 - tensor}, {"pipe": 1 - pipe}, {"dp": partner}])

        @pl.when(pipe == 0)
        def _():
            far_copy(inp).start()

        @pl.when(pipe == 1)
        def _():
            far_copy(cot).start()

    @pl.when((micro == own) & (step == 0))
    def _():
        far_copy(inp).wait()
        near_copy(tensor).start()
        near_copy(1 - tensor).wait_recv()
        near_copy(tensor).wait_send()
        other_out[...] = other[...]

    @pl.when(step == 0)
    def _():
        @pl.when((pipe == 0) & (micro < own))
        def _():
            hidden_out[0] = inp[jnp.minimum(micro, own - 1)]

        @pl.when((pipe == 0) & (micro >= own))
        def _():
            hidden_out[0] = other[jnp.maximum(micro - own, 0)]

        @pl.when(pipe == 1)
        def _():
            passed_on(xin, micro, sems, 0)
            hidden_out[0] = xin[micro]

        wide = hidden_out[0].astype(jnp.float32)
        n1 = (wide * rsqrt_mean(wide) * gains[0:1, :]).astype(jnp.bfloat16)
        n1_out[0] = n1
        query = dot(n1, wq[...])
        keys = dot(n1, wk[...])
        values = dot(n1, wv[...])
        cosine, sine = tables[0], tables[1]
        cosine2 = jnp.concatenate([cosine, cosine], axis=0)
        sine2 = jnp.concatenate([sine, sine], axis=0)
        groups = k_out.shape[1]
        at_q = lax.rem(lax.broadcasted_iota(jnp.int32, (2 * length, length), 0), length)
        at_k = lax.broadcasted_iota(jnp.int32, (2 * length, length), 1)
        causal = at_q >= at_k
        outs = []
        for group in range(groups):
            q = jnp.concatenate([spread(query, 2 * group), spread(query, 2 * group + 1)], axis=0)
            q = turned(q, cosine2, sine2).astype(jnp.bfloat16)
            k = turned(spread(keys, group), cosine, sine).astype(jnp.bfloat16)
            v = spread(values, group).astype(jnp.bfloat16)
            q_out[0, group] = q
            k_out[0, group] = k
            v_out[0, group] = v
            weights = jnp.where(causal, jnp.exp(times_t(q, k) * SCALE), 0.0)
            total = jnp.sum(weights, axis=-1, keepdims=True)
            probs = (weights * (1.0 / total)).astype(jnp.bfloat16)
            mixed = dot(probs, v)
            outs += [mixed[:length], mixed[length:]]
        mixed = gathered(outs).astype(jnp.bfloat16)
        o_out[0] = mixed
        swap = Exchange(2 * micro, send, got, send_sem, recv_sem)
        for piece in range(SEND_PIECES):
            swap.start(piece, times_t(mixed, wo[piece * swap.width : (piece + 1) * swap.width, :]))
        swap.wait()
        both = hidden_out[0].astype(jnp.float32) + swap.total()
        middle[...] = both
        middle_out[0] = both
        n2 = (both * rsqrt_mean(both) * gains[1:2, :]).astype(jnp.bfloat16)
        n2_buf[...] = n2
        n2_out[0] = n2

    @pl.when(step > 0)
    def _():
        n2 = n2_buf[...]
        gate = dot(n2, wg[...])
        up = dot(n2, wu[...])
        act = (gate * jax.nn.sigmoid(gate) * up).astype(jnp.bfloat16)
        gate_out[0] = gate.astype(jnp.bfloat16)
        up_out[0] = up.astype(jnp.bfloat16)
        act_out[0] = act

        @pl.when(step == 1)
        def _():
            acc[...] = times_t(act, wd[...])

        @pl.when((step > 1) & (step < HIDDEN_STEPS))
        def _():
            acc[...] += times_t(act, wd[...])

        @pl.when(step == HIDDEN_STEPS)
        def _():
            swap = Exchange(2 * micro + 1, send, got, send_sem, recv_sem)
            for piece in range(SEND_PIECES):
                columns = slice(piece * swap.width, (piece + 1) * swap.width)
                swap.start(piece, acc[:, columns] + times_t(act, wd[columns, :]))
            swap.wait()
            result = (middle[...] + swap.total()).astype(jnp.bfloat16)
            result_out[0] = result

            @pl.when(pipe == 0)
            def _():
                res[micro] = result
                sent_on(res, xin, micro, sems, 1).start()

            @pl.when((pipe == 0) & (micro == micros - 1))
            def _():
                for which in range(micros):
                    sent_on(res, xin, which, sems, 1).wait_send()


def backward_kernel(
    own,
    micros,
    cot,
    other,
    gains,
    tables,
    hidden,
    q_in,
    k_in,
    v_in,
    middle,
    gate_in,
    up_in,
    wq,
    wk,
    wv,
    wo,
    wg,
    wu,
    wd,
    grad_out,
    g_out,
    low_out,
    dgate_out,
    dup_out,
    dq_out,
    dk_out,
    dv_out,
    gain_out,
    xin,
    res,
    send,
    got,
    d_middle,
    acc,
    send_sem,
    recv_sem,
    x_send,
    x_recv,
    xp_send,
    xp_recv,
):
    micro, step = pl.program_id(0), pl.program_id(1)
    pipe, tensor = lax.axis_index("pipe"), lax.axis_index("tensor")
    sems = (x_send, x_recv, xp_send, xp_recv)
    length = hidden.shape[1]

    @pl.when((micro == 0) & (step == 0))
    def _():
        greet([{"tensor": 1 - tensor}, {"pipe": 1 - pipe}])
        gain_out[...] = jnp.zeros_like(gain_out)

    @pl.when(step == 0)
    def _():
        @pl.when((pipe == 1) & (micro < own))
        def _():
            g_out[0] = cot[jnp.minimum(micro, own - 1)]

        @pl.when((pipe == 1) & (micro >= own))
        def _():
            g_out[0] = other[jnp.maximum(micro - own, 0)]

        @pl.when(pipe == 0)
        def _():
            passed_on(xin, micro, sems, 1)
            g_out[0] = xin[micro]

    @pl.when(step < HIDDEN_STEPS)
    def _():
        d_act = dot(g_out[0], wd[...])
        gate = gate_in[0].astype(jnp.float32)
        up = up_in[0].astype(jnp.float32)
        sig = jax.nn.sigmoid(gate)
        d_gate = (d_act * up * sig * (1.0 + gate * (1.0 - sig))).astype(jnp.bfloat16)
        d_up = (d_act * gate * sig).astype(jnp.bfloat16)
        dgate_out[0] = d_gate
        dup_out[0] = d_up

        @pl.when(step == 0)
        def _():
            acc[...] = times_t(d_gate, wg[...]) + times_t(d_up, wu[...])

        @pl.when((step > 0) & (step < HIDDEN_STEPS - 1))
        def _():
            acc[...] += times_t(d_gate, wg[...]) + times_t(d_up, wu[...])

        @pl.when(step == HIDDEN_STEPS - 1)
        def _():
            swap = Exchange(2 * micro, send, got, send_sem, recv_sem)
            for piece in range(SEND_PIECES):
                columns = slice(piece * swap.width, (piece + 1) * swap.width)
                swap.start(
                    piece,
                    acc[:, columns] + times_t(d_gate, wg[columns, :]) + times_t(d_up, wu[columns, :]),
                )
            swap.wait()
            d_normed = swap.total()
            mid = middle[0]
            scale = rsqrt_mean(mid)
            gain_out[1:2, :] += jnp.sum(d_normed * mid * scale, axis=0, keepdims=True)
            weighted = d_normed * gains[1:2, :]
            inner = jnp.mean(weighted * mid, axis=-1, keepdims=True)
            total = g_out[0].astype(jnp.float32) + scale * weighted - mid * (scale**3 * inner)
            d_middle[...] = total
            low_out[0] = total.astype(jnp.bfloat16)

    @pl.when(step == HIDDEN_STEPS)
    def _():
        d_mixed = dot(low_out[0], wo[...]).astype(jnp.bfloat16).astype(jnp.float32)
        cosine, sine = tables[0], tables[1]
        cosine2 = jnp.concatenate([cosine, cosine], axis=0)
        sine2 = jnp.concatenate([sine, sine], axis=0)
        at_k = lax.broadcasted_iota(jnp.int32, (length, 2 * length), 0)
        at_q = lax.rem(lax.broadcasted_iota(jnp.int32, (length, 2 * length), 1), length)
        causal = at_q >= at_k
        d_queries, d_keys, d_values = [], [], []
        for group in range(k_in.shape[1]):
            q, k, v = q_in[0, group], k_in[0, group], v_in[0, group]
            d_head = jnp.concatenate(
                [spread(d_mixed, 2 * group), spread(d_mixed, 2 * group + 1)], axis=0
            ).astype(jnp.bfloat16)
            weights = jnp.where(causal, jnp.exp(times_t(k, q) * SCALE), 0.0)
            probs = weights * (1.0 / jnp.sum(weights, axis=0, keepdims=True))
            d_probs = times_t(v, d_head)
            moved = probs * d_probs
            delta = jnp.sum(moved, axis=0, keepdims=True)
            d_scores = ((moved - probs * delta) * SCALE).astype(jnp.bfloat16)
            d_values.append(dot(probs.astype(jnp.bfloat16), d_head))
            d_keys.append(turned_back(dot(d_scores, q), cosine, sine))
            d_query = turned_back(over_rows(d_scores, k), cosine2, sine2)
            d_queries += [d_query[:length], d_query[length:]]
        d_query = gathered(d_queries).astype(jnp.bfloat16)
        d_key = gathered(d_keys).astype(jnp.bfloat16)
        d_value = gathered(d_values).astype(jnp.bfloat16)
        dq_out[0] = d_query
        dk_out[0] = d_key
        dv_out[0] = d_value
        swap = Exchange(2 * micro + 1, send, got, send_sem, recv_sem)
        for piece in range(SEND_PIECES):
            rows = slice(piece * swap.width, (piece + 1) * swap.width)
            swap.start(
                piece,
                times_t(d_query, wq[rows, :]) + times_t(d_key, wk[rows, :]) + times_t(d_value, wv[rows, :]),
            )
        swap.wait()
        d_first = swap.total()
        wide = hidden[0].astype(jnp.float32)
        scale = rsqrt_mean(wide)
        gain_out[0:1, :] += jnp.sum(d_first * wide * scale, axis=0, keepdims=True)
        weighted = d_first * gains[0:1, :]
        inner = jnp.mean(weighted * wide, axis=-1, keepdims=True)
        d_hidden = (d_middle[...] + scale * weighted - wide * (scale**3 * inner)).astype(jnp.bfloat16)
        grad_out[0] = d_hidden

        @pl.when(pipe == 1)
        def _():
            res[micro] = d_hidden
            sent_on(res, xin, micro, sems, 0).start()

        @pl.when((pipe == 1) & (micro == micros - 1))
        def _():
            for which in range(micros):
                sent_on(res, xin, which, sems, 0).wait_send()


def forward(inputs, cotangents, gains, tables, weights):
    own, length, width = inputs.shape
    micros = 2 * own
    wq, wk, wv, wo, wg, wu, wd = weights
    groups = wk.shape[1] // HEAD_SIZE
    hidden = wg.shape[1]
    block = hidden // HIDDEN_STEPS
    low, wide = jnp.bfloat16, jnp.float32

    def whole(array):
        return pl.BlockSpec(
            array.shape, lambda m, s: (0,) * array.ndim, pipeline_mode=pl.Buffered(1)
        )

    def streamed(array):
        return pl.BlockSpec((width, block), lambda m, s: (0, jnp.maximum(s - 1, 0)))

    def by_micro(*shape):
        return pl.BlockSpec((1,) + shape, lambda m, s: (m,) + (0,) * len(shape))

    by_block = pl.BlockSpec((1, length, block), lambda m, s: (m, 0, jnp.maximum(s - 1, 0)))
    shapes = [
        ((length, width), low),
        ((length, width), low),
        ((length, width), low),
        ((groups, 2 * length, LANES), low),
        ((groups, length, LANES), low),
        ((groups, length, LANES), low),
        ((length, wq.shape[1]), low),
        ((length, width), wide),
        ((length, width), low),
    ]
    out_shape = [jax.ShapeDtypeStruct((micros,) + shape, kind) for shape, kind in shapes]
    out_specs = [by_micro(*shape) for shape, _ in shapes]
    out_shape += [jax.ShapeDtypeStruct((micros, length, hidden), low)] * 3
    out_specs += [by_block] * 3
    out_shape.append(jax.ShapeDtypeStruct(inputs.shape, low))
    out_specs.append(whole(inputs))
    return pl.pallas_call(
        functools.partial(forward_kernel, own, micros),
        grid=(micros, HIDDEN_STEPS + 1),
        out_shape=out_shape,
        in_specs=[
            whole(inputs),
            pl.BlockSpec(memory_space=pl.ANY),
            whole(gains),
            whole(tables),
            whole(wq),
            whole(wk),
            whole(wv),
            whole(wo),
            streamed(wg),
            streamed(wu),
            streamed(wd),
        ],
        out_specs=out_specs,
        scratch_shapes=[
            pltpu.VMEM((own, length, width), low),
            pltpu.VMEM((micros, length, width), low),
            pltpu.VMEM((micros, length, width), low),
            pltpu.VMEM((length, width), low),
            pltpu.VMEM((2 * micros, length, width), low),
            pltpu.VMEM((length, width), wide),
            pltpu.VMEM((length, width), wide),
            pltpu.VMEM((length, width), low),
            pltpu.SemaphoreType.DMA((2 * micros, SEND_PIECES)),
            pltpu.SemaphoreType.DMA((2 * micros, SEND_PIECES)),
            pltpu.SemaphoreType.DMA((micros,)),
            pltpu.SemaphoreType.DMA((micros,)),
            pltpu.SemaphoreType.DMA((micros,)),
            pltpu.SemaphoreType.DMA((micros,)),
            pltpu.SemaphoreType.DMA,
            pltpu.SemaphoreType.DMA,
            pltpu.SemaphoreType.DMA,
            pltpu.SemaphoreType.DMA,
        ],
        compiler_params=pltpu.CompilerParams(
            collective_id=0, has_side_effects=True, vmem_limit_bytes=62 * MIB
        ),
    )(inputs, cotangents, gains, tables, wq, wk, wv, wo, wg, wu, wd)


def backward(cotangents, other, gains, tables, record, weights):
    own, length, width = cotangents.shape
    micros = 2 * own
    wq, wk, wv, wo, wg, wu, wd = weights
    groups = wk.shape[1] // HEAD_SIZE
    hidden = wg.shape[1]
    block = hidden // HIDDEN_STEPS
    low, wide = jnp.bfloat16, jnp.float32

    def whole(array):
        return pl.BlockSpec(
            array.shape, lambda m, s: (0,) * array.ndim, pipeline_mode=pl.Buffered(1)
        )

    def streamed(array):
        return pl.BlockSpec((width, block), lambda m, s: (0, jnp.minimum(s, HIDDEN_STEPS - 1)))

    def by_micro(*shape):
        return pl.BlockSpec((1,) + shape, lambda m, s: (m,) + (0,) * len(shape))

    by_block = pl.BlockSpec(
        (1, length, block), lambda m, s: (m, 0, jnp.minimum(s, HIDDEN_STEPS - 1))
    )
    shapes = [
        ((length, width), low),
        ((length, width), low),
        ((length, width), low),
        None,
        None,
        ((length, wq.shape[1]), low),
        ((length, wk.shape[1]), low),
        ((length, wv.shape[1]), low),
    ]
    out_shape, out_specs = [], []
    for entry in shapes:
        if entry is None:
            out_shape.append(jax.ShapeDtypeStruct((micros, length, hidden), low))
            out_specs.append(by_block)
        else:
            out_shape.append(jax.ShapeDtypeStruct((micros,) + entry[0], entry[1]))
            out_specs.append(by_micro(*entry[0]))
    out_shape.append(jax.ShapeDtypeStruct(gains.shape, wide))
    out_specs.append(whole(gains))
    return pl.pallas_call(
        functools.partial(backward_kernel, own, micros),
        grid=(micros, HIDDEN_STEPS + 1),
        out_shape=out_shape,
        in_specs=[
            whole(cotangents),
            whole(other),
            whole(gains),
            whole(tables),
            by_micro(length, width),
            by_micro(groups, 2 * length, LANES),
            by_micro(groups, length, LANES),
            by_micro(groups, length, LANES),
            by_micro(length, width),
            by_block,
            by_block,
            whole(wq),
            whole(wk),
            whole(wv),
            whole(wo),
            streamed(wg),
            streamed(wu),
            streamed(wd),
        ],
        out_specs=out_specs,
        scratch_shapes=[
            pltpu.VMEM((micros, length, width), low),
            pltpu.VMEM((micros, length, width), low),
            pltpu.VMEM((length, width), low),
            pltpu.VMEM((2 * micros, length, width), low),
            pltpu.VMEM((length, width), wide),
            pltpu.VMEM((length, width), wide),
            pltpu.SemaphoreType.DMA((2 * micros, SEND_PIECES)),
            pltpu.SemaphoreType.DMA((2 * micros, SEND_PIECES)),
            pltpu.SemaphoreType.DMA((micros,)),
            pltpu.SemaphoreType.DMA((micros,)),
            pltpu.SemaphoreType.DMA((micros,)),
            pltpu.SemaphoreType.DMA((micros,)),
        ],
        compiler_params=pltpu.CompilerParams(
            collective_id=1, has_side_effects=True, vmem_limit_bytes=62 * MIB
        ),
    )(cotangents, other, gains, tables, *record, wq, wk, wv, wo, wg, wu, wd)


WINDOW = 4
LAG = 3


def halving_kernel(widths, blocks, bits, axis, *refs):
    count = len(widths)
    grads, outs = refs[:count], refs[count : 2 * count]
    rest = refs[2 * count :]
    local, got = rest[:count], rest[count : count + count * bits]
    load_sem, send_sem, recv_sem = rest[count + count * bits :]
    me = lax.axis_index(axis)
    own = [lax.rem(lax.div(me, 2**bit), 2) for bit in range(bits)]
    flip = [me + (1 - 2 * own[bit]) * 2**bit for bit in range(bits)]
    greet([{axis: flip[bit]} for bit in range(bits)])
    plain = list(range(bits))
    orders = [plain] if bits < 2 else [plain, [1, 0] + plain[2:]]
    chunks = []
    for which, width in enumerate(widths):
        for at in range(grads[which].shape[-1] // width):
            chunks.append((which, at))
    plans = [orders[number % len(orders)] for number in range(len(chunks))]

    def place(fixed):
        return tuple(fixed[bit] if bit in fixed else slice(None) for bit in reversed(range(bits)))

    loads, sends = {}, {}

    def send(number, level, source, bit):
        which, at = chunks[number]
        copy = pltpu.make_async_remote_copy(
            src_ref=source,
            dst_ref=got[which * bits + level].at[at],
            send_sem=send_sem.at[number, level],
            recv_sem=recv_sem.at[number, level],
            device_id={axis: flip[bit]},
            device_id_type=MESH,
        )
        copy.start()
        sends[number, level] = copy

    def begin(number):
        which, at = chunks[number]
        first = plans[number][0]
        columns = pl.ds(at * widths[which], widths[which])
        send(
            number,
            0,
            grads[which].at[place({first: 1 - own[first]}) + (slice(None), columns)],
            first,
        )
        load = pltpu.make_async_copy(
            grads[which].at[place({first: own[first]}) + (slice(None), columns)],
            local[which].at[at],
            load_sem.at[number],
        )
        load.start()
        loads[number] = load

    def step(number, level):
        which, at = chunks[number]
        order = plans[number]
        width = widths[which]
        block = blocks[which]
        if level == 0:
            loads[number].wait()
        sends[number, level].wait_recv()
        done = order[: level + 1]
        left = [bit for bit in reversed(range(bits)) if bit not in done]
        received = got[which * bits + level].at[at]
        axes = [bit for bit in reversed(range(bits)) if bit != order[0]]
        rows = 64 if block % 64 == 0 else block
        for combo in range(2 ** len(left)):
            fixed = {bit: (combo >> index) & 1 for index, bit in enumerate(left)}
            for bit in done:
                fixed[bit] = own[bit]
            spot = (at,) + tuple(fixed[bit] for bit in axes)
            from_spot = tuple(fixed[bit] for bit in left)

            def add(piece, _):
                where = pl.ds(pl.multiple_of(piece * rows, rows), rows)
                a = local[which][spot + (where, slice(None))].astype(jnp.float32)
                b = received[from_spot + (where, slice(None))].astype(jnp.float32)
                if level == bits - 1:
                    outs[which][where, pl.ds(at * width, width)] = (a + b).astype(jnp.bfloat16)
                else:
                    local[which][spot + (where, slice(None))] = (a + b).astype(jnp.bfloat16)
                return 0

            lax.fori_loop(0, block // rows, add, 0)
        if level < bits - 1:
            following = order[level + 1]
            source = []
            for bit in axes:
                if bit in done:
                    source.append(own[bit])
                elif bit == following:
                    source.append(1 - own[bit])
                else:
                    source.append(slice(None))
            send(number, level + 1, local[which].at[(at,) + tuple(source)], following)

    total = len(chunks)
    for number in range(min(WINDOW, total)):
        begin(number)
    for tick in range(total + LAG * (bits - 1)):
        for level in range(bits):
            number = tick - LAG * level
            if 0 <= number < total:
                step(number, level)
        if tick + WINDOW < total:
            begin(tick + WINDOW)
    for copy in sends.values():
        copy.wait_send()


def scattered(grads, axis, bits):
    blocks = [grad.shape[0] // 2**bits for grad in grads]
    widths = [next(w for w in (256, 384, 128) if grad.shape[1] % w == 0) for grad in grads]
    shaped = [
        grad.reshape((2,) * bits + (block, grad.shape[1])) for grad, block in zip(grads, blocks)
    ]
    pieces = [grad.shape[1] // width for grad, width in zip(grads, widths)]
    scratch = [
        pltpu.VMEM((piece,) + (2,) * (bits - 1) + (block, width), jnp.bfloat16)
        for piece, block, width in zip(pieces, blocks, widths)
    ]
    for piece, block, width in zip(pieces, blocks, widths):
        for level in range(bits):
            scratch.append(
                pltpu.VMEM((piece,) + (2,) * (bits - 1 - level) + (block, width), jnp.bfloat16)
            )
    total = sum(pieces)
    scratch += [
        pltpu.SemaphoreType.DMA((total,)),
        pltpu.SemaphoreType.DMA((total, bits)),
        pltpu.SemaphoreType.DMA((total, bits)),
    ]
    return pl.pallas_call(
        functools.partial(halving_kernel, widths, blocks, bits, axis),
        out_shape=[
            jax.ShapeDtypeStruct((block, grad.shape[1]), jnp.bfloat16)
            for grad, block in zip(grads, blocks)
        ],
        in_specs=[pl.BlockSpec(memory_space=pl.ANY)] * len(grads),
        out_specs=[pl.BlockSpec(memory_space=pltpu.VMEM)] * len(grads),
        scratch_shapes=scratch,
        compiler_params=pltpu.CompilerParams(
            collective_id=2, has_side_effects=True, vmem_limit_bytes=60 * MIB
        ),
    )(*shaped)


def body(
    inputs,
    cotangents,
    norm_scales,
    w_query,
    key_weight,
    value_weight,
    w_out,
    w_gate,
    w_up,
    down_weight,
):
    weights = (
        w_query[0],
        key_weight[0],
        value_weight[0],
        w_out[0],
        w_gate[0],
        w_up[0],
        down_weight[0],
    )
    micros, _, length, width = inputs.shape
    gains = norm_scales[0].T
    tables = jnp.asarray(rope_tables(length))
    cots = cotangents[:, 0]
    (
        result,
        hidden,
        n1,
        q,
        k,
        v,
        mixed,
        middle,
        n2,
        gate,
        up,
        act,
        other,
    ) = forward(inputs[:, 0], cots, gains, tables, weights)
    grad, g, low, d_gate, d_up, d_q, d_k, d_v, gain = backward(
        cots, other, gains, tables, (hidden, q, k, v, middle, gate, up), weights
    )
    peers = lax.axis_size("dp")
    bits = peers.bit_length() - 2
    top = lax.div(lax.axis_index("dp"), peers // 2)

    def rows_of(values):
        flat = values.reshape(-1, values.shape[-1])
        size = flat.shape[-1] // 2
        return lax.dynamic_slice_in_dim(flat, top * size, size, 1)

    def flat(values):
        return values.reshape(-1, values.shape[-1])

    gain_rows = lax.dynamic_slice_in_dim(gain, top * (width // 2), width // 2, 1).T
    gain_rows = gain_rows.astype(jnp.bfloat16).reshape(peers // 2, -1)
    gain_size = gain_rows.shape[1]
    gain_rows = jnp.pad(gain_rows, ((0, 0), (0, 16 * LANES - gain_size))).reshape(-1, LANES)
    n1_rows, n2_rows, low_rows, g_rows = rows_of(n1), rows_of(n2), rows_of(low), rows_of(g)
    grads = [
        over_rows(n2_rows, flat(d_gate)),
        over_rows(n2_rows, flat(d_up)),
        over_rows(g_rows, flat(act)),
        over_rows(n1_rows, flat(d_q)),
        over_rows(n1_rows, flat(d_k)),
        over_rows(n1_rows, flat(d_v)),
        over_rows(low_rows, flat(mixed)),
        gain_rows,
    ]
    shards = scattered([item.astype(jnp.bfloat16) for item in grads], "dp", bits)
    shards = [shard.astype(jnp.float32) for shard in shards]
    grad_scales = shards[7].reshape(-1)[:gain_size].reshape(1, -1, 2)
    grad_gate, grad_up, grad_down, grad_query, grad_key, grad_value, grad_proj = (
        shard[None] for shard in shards[:7]
    )
    return (
        result[:micros][None, :, None],
        grad[:micros][None, :, None],
        grad_scales,
        grad_query,
        grad_key,
        grad_value,
        grad_proj,
        grad_gate,
        grad_up,
        grad_down,
    )


def solution(mesh):
    placed = (
        P(None, "dp", None, None),
        P(None, "dp", None, None),
        P("pipe", None, None),
        P("pipe", None, "tensor"),
        P("pipe", None, "tensor"),
        P("pipe", None, "tensor"),
        P("pipe", None, "tensor"),
        P("pipe", None, "tensor"),
        P("pipe", None, "tensor"),
        P("pipe", None, "tensor"),
    )
    return jax.shard_map(
        body,
        mesh=mesh,
        in_specs=placed,
        out_specs=(
            P("pipe", None, "dp", None, None),
            P("pipe", None, "dp", None, None),
            P("pipe", "dp", None),
            P("pipe", "dp", "tensor"),
            P("pipe", "dp", "tensor"),
            P("pipe", "dp", "tensor"),
            P("pipe", "dp", "tensor"),
            P("pipe", "dp", "tensor"),
            P("pipe", "dp", "tensor"),
            P("pipe", "dp", "tensor"),
        ),
        check_vma=False,
    )
```

```python
import functools

import jax
import jax.numpy as jnp
import numpy as np
from jax import lax
from jax.experimental import pallas as pl
from jax.experimental.pallas import tpu as pltpu
from jax.sharding import PartitionSpec as P

HEAD_SIZE = 96
HALF = HEAD_SIZE // 2
LANES = 128
HIDDEN_STEPS = 4
SEND_PIECES = 3

EPS = 1e-05
THETA = 100000.0
MESH = pl.DeviceIdType.MESH
MIB = 2**20
SCALE = HEAD_SIZE ** (-0.5)


def rope_tables(length):
    freqs = (THETA ** (-(np.arange(HALF, dtype=np.float64) * 2.0 / HEAD_SIZE))).astype(np.float32)
    angles = np.arange(length, dtype=np.float32)[:, None] * freqs[None, :]
    cosine, sine = np.cos(angles), np.sin(angles)
    room = np.zeros((length, LANES // 2 - HALF), np.float32)
    cosines = np.concatenate([cosine, room, cosine, room], axis=1)
    sines = np.concatenate([-sine, room, sine, room], axis=1)
    return np.stack([cosines, sines]).astype(np.float32)


def dot(left, right):
    return lax.dot_general(
        left, right, (((1,), (0,)), ((), ())), preferred_element_type=jnp.float32
    )


def times_t(left, right):
    return lax.dot_general(
        left, right, (((1,), (1,)), ((), ())), preferred_element_type=jnp.float32
    )


def over_rows(left, right):
    return lax.dot_general(
        left, right, (((0,), (0,)), ((), ())), preferred_element_type=jnp.float32
    )


def spread(values, head):
    room = jnp.zeros((values.shape[0], LANES // 2 - HALF), values.dtype)
    at = head * HEAD_SIZE
    return jnp.concatenate(
        [values[:, at : at + HALF], room, values[:, at + HALF : at + HEAD_SIZE], room], axis=1
    )


def gathered(heads):
    parts = []
    for head in heads:
        parts += [head[:, :HALF], head[:, LANES // 2 : LANES // 2 + HALF]]
    return jnp.concatenate(parts, axis=1)


def turned(values, cosine, sine):
    return values * cosine + pltpu.roll(values, LANES // 2, 1) * sine


def turned_back(values, cosine, sine):
    return values * cosine - pltpu.roll(values, LANES // 2, 1) * sine


def rsqrt_mean(values):
    return lax.rsqrt(jnp.mean(values * values, axis=-1, keepdims=True) + EPS)


class Exchange:
    def __init__(self, number, send, got, send_sem, recv_sem):
        self.number, self.send, self.got = number, send, got
        self.send_sem, self.recv_sem = send_sem, recv_sem
        self.width = send.shape[1] // SEND_PIECES

    def copy(self, piece):
        columns = pl.ds(piece * self.width, self.width)
        return pltpu.make_async_remote_copy(
            src_ref=self.send.at[:, columns],
            dst_ref=self.got.at[self.number, :, columns],
            send_sem=self.send_sem.at[self.number, piece],
            recv_sem=self.recv_sem.at[self.number, piece],
            device_id={"tensor": 1 - lax.axis_index("tensor")},
            device_id_type=MESH,
        )

    def start(self, piece, partial_value):
        columns = pl.ds(piece * self.width, self.width)
        self.send[:, columns] = partial_value.astype(jnp.bfloat16)
        self.copy(piece).start()

    def wait(self):
        for piece in range(SEND_PIECES):
            self.copy(piece).wait()

    def total(self):
        return self.send[...].astype(jnp.float32) + self.got[self.number].astype(jnp.float32)


def half_copy(source, target, rows, send_sem, recv_sem, device):
    return pltpu.make_async_remote_copy(
        src_ref=source.at[rows],
        dst_ref=target.at[rows],
        send_sem=send_sem,
        recv_sem=recv_sem,
        device_id=device,
        device_id_type=MESH,
    )


def passed_on(xin, micro, sems, stage_from):
    tensor = lax.axis_index("tensor")
    rows = xin.shape[1] // 2
    send_sem, recv_sem, pair_send, pair_recv = sems
    slot = xin.at[micro]
    mine = pl.ds(pl.multiple_of(tensor * rows, rows), rows)
    theirs = pl.ds(pl.multiple_of((1 - tensor) * rows, rows), rows)
    half_copy(
        slot, slot, mine, send_sem.at[micro], recv_sem.at[micro], {"pipe": stage_from}
    ).wait_recv()
    copy = half_copy(
        slot, slot, mine, pair_send.at[micro], pair_recv.at[micro], {"tensor": 1 - tensor}
    )
    copy.start()
    half_copy(
        slot, slot, theirs, pair_send.at[micro], pair_recv.at[micro], {"tensor": 1 - tensor}
    ).wait_recv()
    copy.wait_send()


def sent_on(source, xin, micro, sems, stage_to):
    tensor = lax.axis_index("tensor")
    rows = xin.shape[1] // 2
    mine = pl.ds(pl.multiple_of(tensor * rows, rows), rows)
    return half_copy(
        source.at[micro], xin.at[micro], mine, sems[0].at[micro], sems[1].at[micro], {"pipe": stage_to}
    )


def greet(devices):
    barrier = pltpu.get_barrier_semaphore()
    for device in devices:
        pl.semaphore_signal(barrier, inc=1, device_id=device, device_id_type=MESH)
    pl.semaphore_wait(barrier, len(devices))


def forward_kernel(
    micros,
    inp,
    cot,
    gains,
    tables,
    wq,
    wk,
    wv,
    wo,
    wg,
    wu,
    wd,
    result_out,
    hidden_out,
    n1_out,
    q_out,
    k_out,
    v_out,
    o_out,
    middle_out,
    n2_out,
    gate_out,
    up_out,
    act_out,
    other_out,
    other,
    xin,
    res,
    send,
    got,
    middle,
    acc,
    n2_buf,
    send_sem,
    recv_sem,
    x_send,
    x_recv,
    xp_send,
    xp_recv,
    far_send,
    far_recv,
    near_send,
    near_recv,
):
    micro, step = pl.program_id(0), pl.program_id(1)
    pipe, tensor, data = lax.axis_index("pipe"), lax.axis_index("tensor"), lax.axis_index("dp")
    peers = lax.axis_size("dp")
    partner = lax.rem(data + peers // 2, peers)
    sems = (x_send, x_recv, xp_send, xp_recv)
    length = inp.shape[1]

    def far_copy(source):
        return pltpu.make_async_remote_copy(
            src_ref=source.at[tensor],
            dst_ref=other.at[tensor],
            send_sem=far_send,
            recv_sem=far_recv,
            device_id={"dp": partner},
            device_id_type=MESH,
        )

    def near_copy(which):
        return pltpu.make_async_remote_copy(
            src_ref=other.at[which],
            dst_ref=other.at[which],
            send_sem=near_send,
            recv_sem=near_recv,
            device_id={"tensor": 1 - tensor},
            device_id_type=MESH,
        )

    @pl.when((micro == 0) & (step == 0))
    def _():
        greet([{"tensor": 1 - tensor}, {"pipe": 1 - pipe}, {"dp": partner}])

        @pl.when(pipe == 0)
        def _():
            far_copy(inp).start()

        @pl.when(pipe == 1)
        def _():
            far_copy(cot).start()

    @pl.when((micro == micros - 1) & (step == HIDDEN_STEPS))
    def _():
        far_copy(inp).wait()
        near_copy(tensor).start()
        near_copy(1 - tensor).wait_recv()
        near_copy(tensor).wait_send()
        other_out[...] = other[...]

    @pl.when(step == 0)
    def _():
        @pl.when(pipe == 0)
        def _():
            hidden_out[0] = inp[micro]

        @pl.when(pipe == 1)
        def _():
            passed_on(xin, micro, sems, 0)
            hidden_out[0] = xin[micro]

        wide = hidden_out[0].astype(jnp.float32)
        n1 = (wide * rsqrt_mean(wide) * gains[0:1, :]).astype(jnp.bfloat16)
        n1_out[0] = n1
        query = dot(n1, wq[...])
        keys = dot(n1, wk[...])
        values = dot(n1, wv[...])
        cosine, sine = tables[0], tables[1]
        cosine2 = jnp.concatenate([cosine, cosine], axis=0)
        sine2 = jnp.concatenate([sine, sine], axis=0)
        groups = k_out.shape[1]
        at_q = lax.rem(lax.broadcasted_iota(jnp.int32, (2 * length, length), 0), length)
        at_k = lax.broadcasted_iota(jnp.int32, (2 * length, length), 1)
        causal = at_q >= at_k
        outs = []
        for group in range(groups):
            q = jnp.concatenate([spread(query, 2 * group), spread(query, 2 * group + 1)], axis=0)
            q = turned(q, cosine2, sine2).astype(jnp.bfloat16)
            k = turned(spread(keys, group), cosine, sine).astype(jnp.bfloat16)
            v = spread(values, group).astype(jnp.bfloat16)
            q_out[0, group] = q
            k_out[0, group] = k
            v_out[0, group] = v
            weights = jnp.where(causal, jnp.exp(times_t(q, k) * SCALE), 0.0)
            total = jnp.sum(weights, axis=-1, keepdims=True)
            probs = (weights * (1.0 / total)).astype(jnp.bfloat16)
            mixed = dot(probs, v)
            outs += [mixed[:length], mixed[length:]]
        mixed = gathered(outs).astype(jnp.bfloat16)
        o_out[0] = mixed
        swap = Exchange(2 * micro, send, got, send_sem, recv_sem)
        for piece in range(SEND_PIECES):
            swap.start(piece, times_t(mixed, wo[piece * swap.width : (piece + 1) * swap.width, :]))
        swap.wait()
        both = hidden_out[0].astype(jnp.float32) + swap.total()
        middle[...] = both
        middle_out[0] = both
        n2 = (both * rsqrt_mean(both) * gains[1:2, :]).astype(jnp.bfloat16)
        n2_buf[...] = n2
        n2_out[0] = n2

    @pl.when(step > 0)
    def _():
        n2 = n2_buf[...]
        gate = dot(n2, wg[...])
        up = dot(n2, wu[...])
        act = (gate * jax.nn.sigmoid(gate) * up).astype(jnp.bfloat16)
        gate_out[0] = gate.astype(jnp.bfloat16)
        up_out[0] = up.astype(jnp.bfloat16)
        act_out[0] = act

        @pl.when(step == 1)
        def _():
            acc[...] = times_t(act, wd[...])

        @pl.when((step > 1) & (step < HIDDEN_STEPS))
        def _():
            acc[...] += times_t(act, wd[...])

        @pl.when(step == HIDDEN_STEPS)
        def _():
            swap = Exchange(2 * micro + 1, send, got, send_sem, recv_sem)
            for piece in range(SEND_PIECES):
                columns = slice(piece * swap.width, (piece + 1) * swap.width)
                swap.start(piece, acc[:, columns] + times_t(act, wd[columns, :]))
            swap.wait()
            result = (middle[...] + swap.total()).astype(jnp.bfloat16)
            result_out[0] = result

            @pl.when(pipe == 0)
            def _():
                res[micro] = result
                sent_on(res, xin, micro, sems, 1).start()

            @pl.when((pipe == 0) & (micro == micros - 1))
            def _():
                for which in range(micros):
                    sent_on(res, xin, which, sems, 1).wait_send()


def attention_backward(d_mixed, group, q, k, v, trig, causal, with_output):
    cosine, sine, cosine2, sine2 = trig
    d_head = jnp.concatenate(
        [spread(d_mixed, 2 * group), spread(d_mixed, 2 * group + 1)], axis=0
    ).astype(jnp.bfloat16)
    weights = jnp.where(causal, jnp.exp(times_t(k, q) * SCALE), 0.0)
    probs = weights * (1.0 / jnp.sum(weights, axis=0, keepdims=True))
    moved = probs * times_t(v, d_head)
    delta = jnp.sum(moved, axis=0, keepdims=True)
    d_scores = ((moved - probs * delta) * SCALE).astype(jnp.bfloat16)
    rounded = probs.astype(jnp.bfloat16)
    d_value = dot(rounded, d_head)
    d_key = turned_back(dot(d_scores, q), cosine, sine)
    d_query = turned_back(over_rows(d_scores, k), cosine2, sine2)
    length = k.shape[0]
    mixed = over_rows(rounded, v) if with_output else d_query
    return (
        [d_query[:length], d_query[length:]],
        d_key,
        d_value,
        [mixed[:length], mixed[length:]],
    )


def backward_kernel(
    own,
    cot,
    other,
    gains,
    tables,
    n1_own,
    n2_own,
    hidden,
    q_in,
    k_in,
    v_in,
    middle,
    gate_in,
    up_in,
    wq,
    wk,
    wv,
    wo,
    wg,
    wu,
    wd,
    grad_out,
    g_out,
    low_out,
    dgate_out,
    dup_out,
    dq_out,
    dk_out,
    dv_out,
    n1_out,
    n2_out,
    act_out,
    mixed_out,
    gain_out,
    xin,
    res,
    low_buf,
    far_buf,
    far_gain,
    send,
    got,
    d_middle,
    acc,
    send_sem,
    recv_sem,
    x_send,
    x_recv,
    xp_send,
    xp_recv,
    far_send,
    far_recv,
    near_send,
    near_recv,
    gain_send,
    gain_recv,
):
    micro, step = pl.program_id(0), pl.program_id(1)
    pipe, tensor, data = lax.axis_index("pipe"), lax.axis_index("tensor"), lax.axis_index("dp")
    peers = lax.axis_size("dp")
    partner = lax.rem(data + peers // 2, peers)
    sems = (x_send, x_recv, xp_send, xp_recv)
    length = hidden.shape[1]
    rows = length // 2
    mine = pl.ds(pl.multiple_of(tensor * rows, rows), rows)
    theirs = pl.ds(pl.multiple_of((1 - tensor) * rows, rows), rows)
    is_own = micro < own
    late = jnp.maximum(micro - own, 0)
    early = jnp.minimum(micro, own - 1)

    def far(source, kind, which):
        return half_copy(
            source,
            far_buf.at[kind, which],
            mine,
            far_send.at[kind, which],
            far_recv.at[kind, which],
            {"dp": partner},
        )

    def received(kind, which):
        slot = far_buf.at[kind, which]
        sem = near_send.at[kind, which], near_recv.at[kind, which], {"tensor": 1 - tensor}
        far(slot, kind, which).wait_recv()
        copy = half_copy(slot, slot, mine, *sem)
        copy.start()
        half_copy(slot, slot, theirs, *sem).wait_recv()
        copy.wait_send()

    def gain_copy():
        return pltpu.make_async_remote_copy(
            src_ref=gain_out,
            dst_ref=far_gain,
            send_sem=gain_send,
            recv_sem=gain_recv,
            device_id={"dp": partner},
            device_id_type=MESH,
        )

    @pl.when((micro == 0) & (step == 0))
    def _():
        greet([{"tensor": 1 - tensor}, {"pipe": 1 - pipe}, {"dp": partner}])
        gain_out[...] = jnp.zeros_like(gain_out)
        for which in range(own):
            far(n2_own.at[which], 0, which).start()

        @pl.when(pipe == 1)
        def _():
            for which in range(own):
                far(n1_own.at[which], 1, which).start()

    @pl.when(is_own & (step == 0))
    def _():
        @pl.when(pipe == 1)
        def _():
            g_out[0] = cot[early]

        @pl.when(pipe == 0)
        def _():
            passed_on(xin, early, sems, 1)
            far(xin.at[early], 1, early).start()
            g_out[0] = xin[early]

    @pl.when((micro >= own) & (step == 0))
    def _():
        received(0, late)
        received(1, late)
        n2_out[0] = far_buf[0, late]

        @pl.when(pipe == 1)
        def _():
            g_out[0] = other[late]
            n1_out[0] = far_buf[1, late]

        @pl.when(pipe == 0)
        def _():
            g_out[0] = far_buf[1, late]
            wide = other[late].astype(jnp.float32)
            n1_out[0] = (wide * rsqrt_mean(wide) * gains[0:1, :]).astype(jnp.bfloat16)

    def hidden_grads(gate, up):
        d_act = dot(g_out[0], wd[...])
        sig = jax.nn.sigmoid(gate)
        d_gate = (d_act * up * sig * (1.0 + gate * (1.0 - sig))).astype(jnp.bfloat16)
        d_up = (d_act * gate * sig).astype(jnp.bfloat16)
        dgate_out[0] = d_gate
        dup_out[0] = d_up
        return d_gate, d_up, sig

    @pl.when((micro >= own) & (step < HIDDEN_STEPS))
    def _():
        n2 = n2_out[0]
        gate, up = dot(n2, wg[...]), dot(n2, wu[...])
        sig = hidden_grads(gate, up)[2]
        act_out[0] = (gate * sig * up).astype(jnp.bfloat16)

    @pl.when(is_own & (step < HIDDEN_STEPS))
    def _():
        d_gate, d_up, _ = hidden_grads(
            gate_in[0].astype(jnp.float32), up_in[0].astype(jnp.float32)
        )

        @pl.when(step == 0)
        def _():
            acc[...] = times_t(d_gate, wg[...]) + times_t(d_up, wu[...])

        @pl.when((step > 0) & (step < HIDDEN_STEPS - 1))
        def _():
            acc[...] += times_t(d_gate, wg[...]) + times_t(d_up, wu[...])

        @pl.when(step == HIDDEN_STEPS - 1)
        def _():
            swap = Exchange(2 * micro, send, got, send_sem, recv_sem)
            for piece in range(SEND_PIECES):
                columns = slice(piece * swap.width, (piece + 1) * swap.width)
                swap.start(
                    piece,
                    acc[:, columns] + times_t(d_gate, wg[columns, :]) + times_t(d_up, wu[columns, :]),
                )
            swap.wait()
            d_normed = swap.total()
            mid = middle[0]
            scale = rsqrt_mean(mid)
            gain_out[1:2, :] += jnp.sum(d_normed * mid * scale, axis=0, keepdims=True)
            weighted = d_normed * gains[1:2, :]
            inner = jnp.mean(weighted * mid, axis=-1, keepdims=True)
            total = g_out[0].astype(jnp.float32) + scale * weighted - mid * (scale**3 * inner)
            d_middle[...] = total
            low = total.astype(jnp.bfloat16)
            low_out[0] = low
            low_buf[early] = low
            far(low_buf.at[early], 2, early).start()

    def trig_and_mask():
        cosine, sine = tables[0], tables[1]
        trig = (
            cosine,
            sine,
            jnp.concatenate([cosine, cosine], axis=0),
            jnp.concatenate([sine, sine], axis=0),
        )
        at_k = lax.broadcasted_iota(jnp.int32, (length, 2 * length), 0)
        at_q = lax.rem(lax.broadcasted_iota(jnp.int32, (length, 2 * length), 1), length)
        return trig, at_q >= at_k

    groups = k_in.shape[1]

    @pl.when((micro >= own) & (step == HIDDEN_STEPS))
    def _():
        received(2, late)
        low = far_buf[2, late]
        low_out[0] = low
        n1 = n1_out[0]
        query, keys, values = dot(n1, wq[...]), dot(n1, wk[...]), dot(n1, wv[...])
        d_mixed = dot(low, wo[...]).astype(jnp.bfloat16).astype(jnp.float32)
        trig, causal = trig_and_mask()
        cosine, sine, cosine2, sine2 = trig
        d_queries, d_keys, d_values, outs = [], [], [], []
        for group in range(groups):
            q = jnp.concatenate([spread(query, 2 * group), spread(query, 2 * group + 1)], axis=0)
            q = turned(q, cosine2, sine2).astype(jnp.bfloat16)
            k = turned(spread(keys, group), cosine, sine).astype(jnp.bfloat16)
            v = spread(values, group).astype(jnp.bfloat16)
            parts = attention_backward(d_mixed, group, q, k, v, trig, causal, True)
            d_queries += parts[0]
            d_keys.append(parts[1])
            d_values.append(parts[2])
            outs += parts[3]
        dq_out[0] = gathered(d_queries).astype(jnp.bfloat16)
        dk_out[0] = gathered(d_keys).astype(jnp.bfloat16)
        dv_out[0] = gathered(d_values).astype(jnp.bfloat16)
        mixed_out[0] = gathered(outs).astype(jnp.bfloat16)

    @pl.when(is_own & (step == HIDDEN_STEPS))
    def _():
        d_mixed = dot(low_out[0], wo[...]).astype(jnp.bfloat16).astype(jnp.float32)
        trig, causal = trig_and_mask()
        d_queries, d_keys, d_values = [], [], []
        for group in range(groups):
            parts = attention_backward(
                d_mixed, group, q_in[0, group], k_in[0, group], v_in[0, group], trig, causal, False
            )
            d_queries += parts[0]
            d_keys.append(parts[1])
            d_values.append(parts[2])
        d_query = gathered(d_queries).astype(jnp.bfloat16)
        d_key = gathered(d_keys).astype(jnp.bfloat16)
        d_value = gathered(d_values).astype(jnp.bfloat16)
        dq_out[0] = d_query
        dk_out[0] = d_key
        dv_out[0] = d_value
        swap = Exchange(2 * micro + 1, send, got, send_sem, recv_sem)
        for piece in range(SEND_PIECES):
            part = slice(piece * swap.width, (piece + 1) * swap.width)
            swap.start(
                piece,
                times_t(d_query, wq[part, :]) + times_t(d_key, wk[part, :]) + times_t(d_value, wv[part, :]),
            )
        swap.wait()
        d_first = swap.total()
        wide = hidden[0].astype(jnp.float32)
        scale = rsqrt_mean(wide)
        gain_out[0:1, :] += jnp.sum(d_first * wide * scale, axis=0, keepdims=True)
        weighted = d_first * gains[0:1, :]
        inner = jnp.mean(weighted * wide, axis=-1, keepdims=True)
        d_hidden = (d_middle[...] + scale * weighted - wide * (scale**3 * inner)).astype(jnp.bfloat16)
        grad_out[0] = d_hidden

        @pl.when(pipe == 1)
        def _():
            res[early] = d_hidden
            sent_on(res, xin, early, sems, 0).start()

        @pl.when(micro == own - 1)
        def _():
            gain_copy().start()

    @pl.when((micro == 2 * own - 1) & (step == HIDDEN_STEPS))
    def _():
        gain_copy().wait()
        gain_out[...] += far_gain[...]
        for which in range(own):
            for kind in range(3):
                far(low_buf.at[which], kind, which).wait_send()

        @pl.when(pipe == 1)
        def _():
            for which in range(own):
                sent_on(res, xin, which, sems, 0).wait_send()


def forward(inputs, cotangents, gains, tables, weights):
    micros, length, width = inputs.shape
    wq, wk, wv, wo, wg, wu, wd = weights
    groups = wk.shape[1] // HEAD_SIZE
    hidden = wg.shape[1]
    block = hidden // HIDDEN_STEPS
    low, wide = jnp.bfloat16, jnp.float32

    def whole(array):
        return pl.BlockSpec(
            array.shape, lambda m, s: (0,) * array.ndim, pipeline_mode=pl.Buffered(1)
        )

    def streamed(array):
        return pl.BlockSpec((width, block), lambda m, s: (0, jnp.maximum(s - 1, 0)))

    def by_micro(*shape):
        return pl.BlockSpec((1,) + shape, lambda m, s: (m,) + (0,) * len(shape))

    by_block = pl.BlockSpec((1, length, block), lambda m, s: (m, 0, jnp.maximum(s - 1, 0)))
    shapes = [
        ((length, width), low),
        ((length, width), low),
        ((length, width), low),
        ((groups, 2 * length, LANES), low),
        ((groups, length, LANES), low),
        ((groups, length, LANES), low),
        ((length, wq.shape[1]), low),
        ((length, width), wide),
        ((length, width), low),
    ]
    out_shape = [jax.ShapeDtypeStruct((micros,) + shape, kind) for shape, kind in shapes]
    out_specs = [by_micro(*shape) for shape, _ in shapes]
    out_shape += [jax.ShapeDtypeStruct((micros, length, hidden), low)] * 3
    out_specs += [by_block] * 3
    out_shape.append(jax.ShapeDtypeStruct(inputs.shape, low))
    out_specs.append(whole(inputs))
    return pl.pallas_call(
        functools.partial(forward_kernel, micros),
        grid=(micros, HIDDEN_STEPS + 1),
        out_shape=out_shape,
        in_specs=[
            whole(inputs),
            pl.BlockSpec(memory_space=pl.ANY),
            whole(gains),
            whole(tables),
            whole(wq),
            whole(wk),
            whole(wv),
            whole(wo),
            streamed(wg),
            streamed(wu),
            streamed(wd),
        ],
        out_specs=out_specs,
        scratch_shapes=[
            pltpu.VMEM((micros, length, width), low),
            pltpu.VMEM((micros, length, width), low),
            pltpu.VMEM((micros, length, width), low),
            pltpu.VMEM((length, width), low),
            pltpu.VMEM((2 * micros, length, width), low),
            pltpu.VMEM((length, width), wide),
            pltpu.VMEM((length, width), wide),
            pltpu.VMEM((length, width), low),
            pltpu.SemaphoreType.DMA((2 * micros, SEND_PIECES)),
            pltpu.SemaphoreType.DMA((2 * micros, SEND_PIECES)),
            pltpu.SemaphoreType.DMA((micros,)),
            pltpu.SemaphoreType.DMA((micros,)),
            pltpu.SemaphoreType.DMA((micros,)),
            pltpu.SemaphoreType.DMA((micros,)),
            pltpu.SemaphoreType.DMA,
            pltpu.SemaphoreType.DMA,
            pltpu.SemaphoreType.DMA,
            pltpu.SemaphoreType.DMA,
        ],
        compiler_params=pltpu.CompilerParams(
            collective_id=0, has_side_effects=True, vmem_limit_bytes=62 * MIB
        ),
    )(inputs, cotangents, gains, tables, wq, wk, wv, wo, wg, wu, wd)


def backward(cotangents, other, gains, tables, n1, n2, record, weights):
    own, length, width = cotangents.shape
    micros = 2 * own
    wq, wk, wv, wo, wg, wu, wd = weights
    groups = wk.shape[1] // HEAD_SIZE
    hidden = wg.shape[1]
    block = hidden // HIDDEN_STEPS
    last = HIDDEN_STEPS - 1
    low, wide = jnp.bfloat16, jnp.float32

    def whole(array):
        return pl.BlockSpec(
            array.shape, lambda m, s: (0,) * array.ndim, pipeline_mode=pl.Buffered(1)
        )

    def streamed(array):
        return pl.BlockSpec((width, block), lambda m, s: (0, jnp.minimum(s, last)))

    def of_all(*shape):
        return pl.BlockSpec((1,) + shape, lambda m, s: (m,) + (0,) * len(shape))

    def of_own(*shape):
        return pl.BlockSpec(
            (1,) + shape, lambda m, s: (jnp.minimum(m, own - 1),) + (0,) * len(shape)
        )

    def of_other(*shape):
        return pl.BlockSpec(
            (1,) + shape, lambda m, s: (jnp.maximum(m - own, 0),) + (0,) * len(shape)
        )

    shape = (1, length, block)
    block_all = pl.BlockSpec(shape, lambda m, s: (m, 0, jnp.minimum(s, last)))
    block_own = pl.BlockSpec(
        shape,
        lambda m, s: (jnp.minimum(m, own - 1), 0, jnp.where(m < own, jnp.minimum(s, last), last)),
    )
    block_other = pl.BlockSpec(
        shape,
        lambda m, s: (jnp.maximum(m - own, 0), 0, jnp.where(m < own, 0, jnp.minimum(s, last))),
    )
    heads, pairs = wq.shape[1], wk.shape[1]
    outs = [
        (own, (width,), of_own(length, width)),
        (micros, (width,), of_all(length, width)),
        (micros, (width,), of_all(length, width)),
        (micros, (hidden,), block_all),
        (micros, (hidden,), block_all),
        (micros, (heads,), of_all(length, heads)),
        (micros, (pairs,), of_all(length, pairs)),
        (micros, (pairs,), of_all(length, pairs)),
        (own, (width,), of_other(length, width)),
        (own, (width,), of_other(length, width)),
        (own, (hidden,), block_other),
        (own, (heads,), of_other(length, heads)),
    ]
    out_shape = [jax.ShapeDtypeStruct((lead, length) + rest, low) for lead, rest, _ in outs]
    out_specs = [spec for _, _, spec in outs]
    out_shape.append(jax.ShapeDtypeStruct(gains.shape, wide))
    out_specs.append(whole(gains))
    row = pltpu.SemaphoreType.DMA((own,))
    grid_of = pltpu.SemaphoreType.DMA((3, own))
    swaps = pltpu.SemaphoreType.DMA((2 * own, SEND_PIECES))
    return pl.pallas_call(
        functools.partial(backward_kernel, own),
        grid=(micros, HIDDEN_STEPS + 1),
        out_shape=out_shape,
        in_specs=[
            whole(cotangents),
            whole(other),
            whole(gains),
            whole(tables),
            pl.BlockSpec(memory_space=pl.ANY),
            pl.BlockSpec(memory_space=pl.ANY),
            of_own(length, width),
            of_own(groups, 2 * length, LANES),
            of_own(groups, length, LANES),
            of_own(groups, length, LANES),
            of_own(length, width),
            block_own,
            block_own,
            whole(wq),
            whole(wk),
            whole(wv),
            whole(wo),
            streamed(wg),
            streamed(wu),
            streamed(wd),
        ],
        out_specs=out_specs,
        scratch_shapes=[
            pltpu.VMEM((own, length, width), low),
            pltpu.VMEM((own, length, width), low),
            pltpu.VMEM((own, length, width), low),
            pltpu.VMEM((3, own, length, width), low),
            pltpu.VMEM(gains.shape, wide),
            pltpu.VMEM((length, width), low),
            pltpu.VMEM((2 * own, length, width), low),
            pltpu.VMEM((length, width), wide),
            pltpu.VMEM((length, width), wide),
            swaps,
            swaps,
            row,
            row,
            row,
            row,
            grid_of,
            grid_of,
            grid_of,
            grid_of,
            pltpu.SemaphoreType.DMA,
            pltpu.SemaphoreType.DMA,
        ],
        compiler_params=pltpu.CompilerParams(
            collective_id=1, has_side_effects=True, vmem_limit_bytes=62 * MIB
        ),
    )(cotangents, other, gains, tables, n1, n2, *record, wq, wk, wv, wo, wg, wu, wd)


WINDOW = 4
LAG = 3


def halving_kernel(widths, blocks, bits, axis, *refs):
    count = len(widths)
    grads, outs = refs[:count], refs[count : 2 * count]
    rest = refs[2 * count :]
    local, got = rest[:count], rest[count : count + count * bits]
    load_sem, send_sem, recv_sem = rest[count + count * bits :]
    me = lax.axis_index(axis)
    own = [lax.rem(lax.div(me, 2**bit), 2) for bit in range(bits)]
    flip = [me + (1 - 2 * own[bit]) * 2**bit for bit in range(bits)]
    greet([{axis: flip[bit]} for bit in range(bits)])
    plain = list(range(bits))
    orders = [plain] if bits < 2 else [plain, [1, 0] + plain[2:]]
    chunks = []
    for which, width in enumerate(widths):
        for at in range(grads[which].shape[-1] // width):
            chunks.append((which, at))
    plans = [orders[number % len(orders)] for number in range(len(chunks))]

    def place(fixed):
        return tuple(fixed[bit] if bit in fixed else slice(None) for bit in reversed(range(bits)))

    loads, sends = {}, {}

    def send(number, level, source, bit):
        which, at = chunks[number]
        copy = pltpu.make_async_remote_copy(
            src_ref=source,
            dst_ref=got[which * bits + level].at[at],
            send_sem=send_sem.at[number, level],
            recv_sem=recv_sem.at[number, level],
            device_id={axis: flip[bit]},
            device_id_type=MESH,
        )
        copy.start()
        sends[number, level] = copy

    def begin(number):
        which, at = chunks[number]
        first = plans[number][0]
        columns = pl.ds(at * widths[which], widths[which])
        send(
            number,
            0,
            grads[which].at[place({first: 1 - own[first]}) + (slice(None), columns)],
            first,
        )
        load = pltpu.make_async_copy(
            grads[which].at[place({first: own[first]}) + (slice(None), columns)],
            local[which].at[at],
            load_sem.at[number],
        )
        load.start()
        loads[number] = load

    def step(number, level):
        which, at = chunks[number]
        order = plans[number]
        width = widths[which]
        block = blocks[which]
        if level == 0:
            loads[number].wait()
        sends[number, level].wait_recv()
        done = order[: level + 1]
        left = [bit for bit in reversed(range(bits)) if bit not in done]
        received = got[which * bits + level].at[at]
        axes = [bit for bit in reversed(range(bits)) if bit != order[0]]
        rows = 64 if block % 64 == 0 else block
        for combo in range(2 ** len(left)):
            fixed = {bit: (combo >> index) & 1 for index, bit in enumerate(left)}
            for bit in done:
                fixed[bit] = own[bit]
            spot = (at,) + tuple(fixed[bit] for bit in axes)
            from_spot = tuple(fixed[bit] for bit in left)

            def add(piece, _):
                where = pl.ds(pl.multiple_of(piece * rows, rows), rows)
                a = local[which][spot + (where, slice(None))].astype(jnp.float32)
                b = received[from_spot + (where, slice(None))].astype(jnp.float32)
                if level == bits - 1:
                    outs[which][where, pl.ds(at * width, width)] = (a + b).astype(jnp.bfloat16)
                else:
                    local[which][spot + (where, slice(None))] = (a + b).astype(jnp.bfloat16)
                return 0

            lax.fori_loop(0, block // rows, add, 0)
        if level < bits - 1:
            following = order[level + 1]
            source = []
            for bit in axes:
                if bit in done:
                    source.append(own[bit])
                elif bit == following:
                    source.append(1 - own[bit])
                else:
                    source.append(slice(None))
            send(number, level + 1, local[which].at[(at,) + tuple(source)], following)

    total = len(chunks)
    for number in range(min(WINDOW, total)):
        begin(number)
    for tick in range(total + LAG * (bits - 1)):
        for level in range(bits):
            number = tick - LAG * level
            if 0 <= number < total:
                step(number, level)
        if tick + WINDOW < total:
            begin(tick + WINDOW)
    for copy in sends.values():
        copy.wait_send()


def scattered(grads, axis, bits):
    blocks = [grad.shape[0] // 2**bits for grad in grads]
    widths = [next(w for w in (256, 384, 128) if grad.shape[1] % w == 0) for grad in grads]
    shaped = [
        grad.reshape((2,) * bits + (block, grad.shape[1])) for grad, block in zip(grads, blocks)
    ]
    pieces = [grad.shape[1] // width for grad, width in zip(grads, widths)]
    scratch = [
        pltpu.VMEM((piece,) + (2,) * (bits - 1) + (block, width), jnp.bfloat16)
        for piece, block, width in zip(pieces, blocks, widths)
    ]
    for piece, block, width in zip(pieces, blocks, widths):
        for level in range(bits):
            scratch.append(
                pltpu.VMEM((piece,) + (2,) * (bits - 1 - level) + (block, width), jnp.bfloat16)
            )
    total = sum(pieces)
    scratch += [
        pltpu.SemaphoreType.DMA((total,)),
        pltpu.SemaphoreType.DMA((total, bits)),
        pltpu.SemaphoreType.DMA((total, bits)),
    ]
    return pl.pallas_call(
        functools.partial(halving_kernel, widths, blocks, bits, axis),
        out_shape=[
            jax.ShapeDtypeStruct((block, grad.shape[1]), jnp.bfloat16)
            for grad, block in zip(grads, blocks)
        ],
        in_specs=[pl.BlockSpec(memory_space=pl.ANY)] * len(grads),
        out_specs=[pl.BlockSpec(memory_space=pltpu.VMEM)] * len(grads),
        scratch_shapes=scratch,
        compiler_params=pltpu.CompilerParams(
            collective_id=2, has_side_effects=True, vmem_limit_bytes=60 * MIB
        ),
    )(*shaped)


def body(
    inputs,
    cotangents,
    norm_scales,
    w_query,
    key_weight,
    value_weight,
    w_out,
    w_gate,
    w_up,
    down_weight,
):
    weights = (
        w_query[0],
        key_weight[0],
        value_weight[0],
        w_out[0],
        w_gate[0],
        w_up[0],
        down_weight[0],
    )
    micros, _, length, width = inputs.shape
    gains = norm_scales[0].T
    tables = jnp.asarray(rope_tables(length))
    cots = cotangents[:, 0]
    (
        result,
        hidden,
        n1,
        q,
        k,
        v,
        mixed,
        middle,
        n2,
        gate,
        up,
        act,
        other,
    ) = forward(inputs[:, 0], cots, gains, tables, weights)
    grad, g, low, d_gate, d_up, d_q, d_k, d_v, n1_far, n2_far, act_far, mixed_far, gain = backward(
        cots, other, gains, tables, n1, n2, (hidden, q, k, v, middle, gate, up), weights
    )
    n1, n2, act, mixed = (
        jnp.concatenate(pair)
        for pair in ((n1, n1_far), (n2, n2_far), (act, act_far), (mixed, mixed_far))
    )
    peers = lax.axis_size("dp")
    bits = peers.bit_length() - 2
    top = lax.div(lax.axis_index("dp"), peers // 2)

    def rows_of(values):
        flat = values.reshape(-1, values.shape[-1])
        size = flat.shape[-1] // 2
        return lax.dynamic_slice_in_dim(flat, top * size, size, 1)

    def flat(values):
        return values.reshape(-1, values.shape[-1])

    gain_rows = lax.dynamic_slice_in_dim(gain, top * (width // 2), width // 2, 1).T
    gain_rows = gain_rows.astype(jnp.bfloat16).reshape(peers // 2, -1)
    gain_size = gain_rows.shape[1]
    gain_rows = jnp.pad(gain_rows, ((0, 0), (0, 16 * LANES - gain_size))).reshape(-1, LANES)
    n1_rows, n2_rows, low_rows, g_rows = rows_of(n1), rows_of(n2), rows_of(low), rows_of(g)
    grads = [
        over_rows(n2_rows, flat(d_gate)),
        over_rows(n2_rows, flat(d_up)),
        over_rows(g_rows, flat(act)),
        over_rows(n1_rows, flat(d_q)),
        over_rows(n1_rows, flat(d_k)),
        over_rows(n1_rows, flat(d_v)),
        over_rows(low_rows, flat(mixed)),
        gain_rows,
    ]
    shards = scattered([item.astype(jnp.bfloat16) for item in grads], "dp", bits)
    shards = [shard.astype(jnp.float32) for shard in shards]
    grad_scales = shards[7].reshape(-1)[:gain_size].reshape(1, -1, 2)
    grad_gate, grad_up, grad_down, grad_query, grad_key, grad_value, grad_proj = (
        shard[None] for shard in shards[:7]
    )
    return (
        result[None, :, None],
        grad[None, :, None],
        grad_scales,
        grad_query,
        grad_key,
        grad_value,
        grad_proj,
        grad_gate,
        grad_up,
        grad_down,
    )


def solution(mesh):
    placed = (
        P(None, "dp", None, None),
        P(None, "dp", None, None),
        P("pipe", None, None),
        P("pipe", None, "tensor"),
        P("pipe", None, "tensor"),
        P("pipe", None, "tensor"),
        P("pipe", None, "tensor"),
        P("pipe", None, "tensor"),
        P("pipe", None, "tensor"),
        P("pipe", None, "tensor"),
    )
    return jax.shard_map(
        body,
        mesh=mesh,
        in_specs=placed,
        out_specs=(
            P("pipe", None, "dp", None, None),
            P("pipe", None, "dp", None, None),
            P("pipe", "dp", None),
            P("pipe", "dp", "tensor"),
            P("pipe", "dp", "tensor"),
            P("pipe", "dp", "tensor"),
            P("pipe", "dp", "tensor"),
            P("pipe", "dp", "tensor"),
            P("pipe", "dp", "tensor"),
            P("pipe", "dp", "tensor"),
        ),
        check_vma=False,
    )
```

```python
import functools

import jax
import jax.numpy as jnp
import numpy as np
from jax import lax
from jax.experimental import pallas as pl
from jax.experimental.pallas import tpu as pltpu
from jax.sharding import PartitionSpec as P

HEAD_SIZE = 96
HALF = HEAD_SIZE // 2
LANES = 128
HIDDEN_STEPS = 4
SEND_PIECES = 3

EPS = 1e-05
THETA = 100000.0
MESH = pl.DeviceIdType.MESH
MIB = 2**20
SCALE = HEAD_SIZE ** (-0.5)


def rope_tables(length):
    freqs = (THETA ** (-(np.arange(HALF, dtype=np.float64) * 2.0 / HEAD_SIZE))).astype(np.float32)
    angles = np.arange(length, dtype=np.float32)[:, None] * freqs[None, :]
    cosine, sine = np.cos(angles), np.sin(angles)
    room = np.zeros((length, LANES // 2 - HALF), np.float32)
    cosines = np.concatenate([cosine, room, cosine, room], axis=1)
    sines = np.concatenate([-sine, room, sine, room], axis=1)
    return np.stack([cosines, sines]).astype(np.float32)


def dot(left, right):
    return lax.dot_general(
        left, right, (((1,), (0,)), ((), ())), preferred_element_type=jnp.float32
    )


def times_t(left, right):
    return lax.dot_general(
        left, right, (((1,), (1,)), ((), ())), preferred_element_type=jnp.float32
    )


def over_rows(left, right):
    return lax.dot_general(
        left, right, (((0,), (0,)), ((), ())), preferred_element_type=jnp.float32
    )


def spread(values, head):
    room = jnp.zeros((values.shape[0], LANES // 2 - HALF), values.dtype)
    at = head * HEAD_SIZE
    return jnp.concatenate(
        [values[:, at : at + HALF], room, values[:, at + HALF : at + HEAD_SIZE], room], axis=1
    )


def gathered(heads):
    parts = []
    for head in heads:
        parts += [head[:, :HALF], head[:, LANES // 2 : LANES // 2 + HALF]]
    return jnp.concatenate(parts, axis=1)


def turned(values, cosine, sine):
    return values * cosine + pltpu.roll(values, LANES // 2, 1) * sine


def turned_back(values, cosine, sine):
    return values * cosine - pltpu.roll(values, LANES // 2, 1) * sine


def rsqrt_mean(values):
    return lax.rsqrt(jnp.mean(values * values, axis=-1, keepdims=True) + EPS)


class Exchange:
    def __init__(self, number, send, got, send_sem, recv_sem):
        self.number, self.send, self.got = number, send, got
        self.send_sem, self.recv_sem = send_sem, recv_sem
        self.width = send.shape[1] // SEND_PIECES

    def copy(self, piece):
        columns = pl.ds(piece * self.width, self.width)
        return pltpu.make_async_remote_copy(
            src_ref=self.send.at[:, columns],
            dst_ref=self.got.at[self.number, :, columns],
            send_sem=self.send_sem.at[self.number, piece],
            recv_sem=self.recv_sem.at[self.number, piece],
            device_id={"tensor": 1 - lax.axis_index("tensor")},
            device_id_type=MESH,
        )

    def start(self, piece, partial_value):
        columns = pl.ds(piece * self.width, self.width)
        self.send[:, columns] = partial_value.astype(jnp.bfloat16)
        self.copy(piece).start()

    def wait(self):
        for piece in range(SEND_PIECES):
            self.copy(piece).wait()

    def total(self):
        return self.send[...].astype(jnp.float32) + self.got[self.number].astype(jnp.float32)


def half_copy(source, target, rows, send_sem, recv_sem, device):
    return pltpu.make_async_remote_copy(
        src_ref=source.at[rows],
        dst_ref=target.at[rows],
        send_sem=send_sem,
        recv_sem=recv_sem,
        device_id=device,
        device_id_type=MESH,
    )


def passed_on(xin, micro, sems, stage_from):
    tensor = lax.axis_index("tensor")
    rows = xin.shape[1] // 2
    send_sem, recv_sem, pair_send, pair_recv = sems
    slot = xin.at[micro]
    mine = pl.ds(pl.multiple_of(tensor * rows, rows), rows)
    theirs = pl.ds(pl.multiple_of((1 - tensor) * rows, rows), rows)
    half_copy(
        slot, slot, mine, send_sem.at[micro], recv_sem.at[micro], {"pipe": stage_from}
    ).wait_recv()
    copy = half_copy(
        slot, slot, mine, pair_send.at[micro], pair_recv.at[micro], {"tensor": 1 - tensor}
    )
    copy.start()
    half_copy(
        slot, slot, theirs, pair_send.at[micro], pair_recv.at[micro], {"tensor": 1 - tensor}
    ).wait_recv()
    copy.wait_send()


def sent_on(source, xin, micro, sems, stage_to):
    tensor = lax.axis_index("tensor")
    rows = xin.shape[1] // 2
    mine = pl.ds(pl.multiple_of(tensor * rows, rows), rows)
    return half_copy(
        source.at[micro], xin.at[micro], mine, sems[0].at[micro], sems[1].at[micro], {"pipe": stage_to}
    )


def greet(devices):
    barrier = pltpu.get_barrier_semaphore()
    for device in devices:
        pl.semaphore_signal(barrier, inc=1, device_id=device, device_id_type=MESH)
    pl.semaphore_wait(barrier, len(devices))


class FarCopies:
    def __init__(self, sources, buffers, sems, partner):
        self.sources, self.buffers, self.sems, self.partner = sources, buffers, sems, partner
        tensor = lax.axis_index("tensor")
        self.pair = {"tensor": 1 - tensor}
        rows = buffers.shape[1] // 2
        self.mine = pl.ds(pl.multiple_of(tensor * rows, rows), rows)
        self.theirs = pl.ds(pl.multiple_of((1 - tensor) * rows, rows), rows)

    def far(self, which, source=None):
        source = self.sources.at[which] if source is None else source
        sems = self.sems.at[which, 0], self.sems.at[which, 1]
        return half_copy(source, self.buffers.at[which], self.mine, *sems, {"dp": self.partner})

    def near(self, which, rows):
        slot = self.buffers.at[which]
        sems = self.sems.at[which, 2], self.sems.at[which, 3]
        return half_copy(slot, slot, rows, *sems, self.pair)

    def start(self, which, source=None):
        self.far(which, source).start()

    def receive(self, which):
        self.far(which, self.buffers.at[which]).wait()
        self.near(which, self.mine).start()
        self.near(which, self.theirs).wait_recv()
        self.near(which, self.mine).wait_send()


def forward_kernel(
    micros,
    inp,
    cot,
    gains,
    tables,
    wq,
    wk,
    wv,
    wo,
    wg,
    wu,
    wd,
    result_out,
    hidden_out,
    n1_out,
    q_out,
    k_out,
    v_out,
    o_out,
    middle_out,
    n2_out,
    gate_out,
    up_out,
    act_out,
    other_out,
    far_out,
    other,
    first_buf,
    far_buf,
    xin,
    res,
    send,
    got,
    middle,
    acc,
    n2_buf,
    send_sem,
    recv_sem,
    x_send,
    x_recv,
    xp_send,
    xp_recv,
    far_send,
    far_recv,
    near_send,
    near_recv,
    far_sems,
):
    micro, step = pl.program_id(0), pl.program_id(1)
    pipe, tensor, data = lax.axis_index("pipe"), lax.axis_index("tensor"), lax.axis_index("dp")
    peers = lax.axis_size("dp")
    partner = lax.rem(data + peers // 2, peers)
    sems = (x_send, x_recv, xp_send, xp_recv)
    length = inp.shape[1]

    def far_copy(source):
        return pltpu.make_async_remote_copy(
            src_ref=source.at[tensor],
            dst_ref=other.at[tensor],
            send_sem=far_send,
            recv_sem=far_recv,
            device_id={"dp": partner},
            device_id_type=MESH,
        )

    def near_copy(which):
        return pltpu.make_async_remote_copy(
            src_ref=other.at[which],
            dst_ref=other.at[which],
            send_sem=near_send,
            recv_sem=near_recv,
            device_id={"tensor": 1 - tensor},
            device_id_type=MESH,
        )

    far = FarCopies(first_buf, far_buf, far_sems, partner)

    @pl.when((micro == 0) & (step == 0))
    def _():
        greet([{"tensor": 1 - tensor}, {"pipe": 1 - pipe}, {"dp": partner}])

        @pl.when(pipe == 0)
        def _():
            far_copy(inp).start()

        @pl.when(pipe == 1)
        def _():
            far_copy(cot).start()

    @pl.when((micro == micros - 1) & (step == HIDDEN_STEPS))
    def _():
        far_copy(inp).wait()
        near_copy(tensor).start()
        near_copy(1 - tensor).wait_recv()
        near_copy(tensor).wait_send()
        other_out[...] = other[...]
        far.receive(1)
        far_out[1] = far_buf[1]

        @pl.when(pipe == 1)
        def _():
            far.receive(0)
            far_out[0] = far_buf[0]

        @pl.when(pipe == 0)
        def _():
            far_out[0] = jnp.zeros_like(far_out[0])

    @pl.when(step == 0)
    def _():
        @pl.when(pipe == 0)
        def _():
            hidden_out[0] = inp[micro]

        @pl.when(pipe == 1)
        def _():
            passed_on(xin, micro, sems, 0)
            hidden_out[0] = xin[micro]

        wide = hidden_out[0].astype(jnp.float32)
        n1 = (wide * rsqrt_mean(wide) * gains[0:1, :]).astype(jnp.bfloat16)
        n1_out[0] = n1

        @pl.when((pipe == 1) & (micro == 0))
        def _():
            first_buf[0] = n1
            far.start(0)

        query = dot(n1, wq[...])
        keys = dot(n1, wk[...])
        values = dot(n1, wv[...])
        cosine, sine = tables[0], tables[1]
        cosine2 = jnp.concatenate([cosine, cosine], axis=0)
        sine2 = jnp.concatenate([sine, sine], axis=0)
        groups = k_out.shape[1]
        at_q = lax.rem(lax.broadcasted_iota(jnp.int32, (2 * length, length), 0), length)
        at_k = lax.broadcasted_iota(jnp.int32, (2 * length, length), 1)
        causal = at_q >= at_k
        outs = []
        for group in range(groups):
            q = jnp.concatenate([spread(query, 2 * group), spread(query, 2 * group + 1)], axis=0)
            q = turned(q, cosine2, sine2).astype(jnp.bfloat16)
            k = turned(spread(keys, group), cosine, sine).astype(jnp.bfloat16)
            v = spread(values, group).astype(jnp.bfloat16)
            q_out[0, group] = q
            k_out[0, group] = k
            v_out[0, group] = v
            weights = jnp.where(causal, jnp.exp(times_t(q, k) * SCALE), 0.0)
            total = jnp.sum(weights, axis=-1, keepdims=True)
            probs = (weights * (1.0 / total)).astype(jnp.bfloat16)
            mixed = dot(probs, v)
            outs += [mixed[:length], mixed[length:]]
        mixed = gathered(outs).astype(jnp.bfloat16)
        o_out[0] = mixed
        swap = Exchange(2 * micro, send, got, send_sem, recv_sem)
        for piece in range(SEND_PIECES):
            swap.start(piece, times_t(mixed, wo[piece * swap.width : (piece + 1) * swap.width, :]))
        swap.wait()
        both = hidden_out[0].astype(jnp.float32) + swap.total()
        middle[...] = both
        middle_out[0] = both
        n2 = (both * rsqrt_mean(both) * gains[1:2, :]).astype(jnp.bfloat16)
        n2_buf[...] = n2
        n2_out[0] = n2

        @pl.when(micro == 0)
        def _():
            first_buf[1] = n2
            far.start(1)


    @pl.when(step > 0)
    def _():
        n2 = n2_buf[...]
        gate = dot(n2, wg[...])
        up = dot(n2, wu[...])
        act = (gate * jax.nn.sigmoid(gate) * up).astype(jnp.bfloat16)
        gate_out[0] = gate.astype(jnp.bfloat16)
        up_out[0] = up.astype(jnp.bfloat16)
        act_out[0] = act

        @pl.when(step == 1)
        def _():
            acc[...] = times_t(act, wd[...])

        @pl.when((step > 1) & (step < HIDDEN_STEPS))
        def _():
            acc[...] += times_t(act, wd[...])

        @pl.when(step == HIDDEN_STEPS)
        def _():
            swap = Exchange(2 * micro + 1, send, got, send_sem, recv_sem)
            for piece in range(SEND_PIECES):
                columns = slice(piece * swap.width, (piece + 1) * swap.width)
                swap.start(piece, acc[:, columns] + times_t(act, wd[columns, :]))
            swap.wait()
            result = (middle[...] + swap.total()).astype(jnp.bfloat16)
            result_out[0] = result

            @pl.when(pipe == 0)
            def _():
                res[micro] = result
                sent_on(res, xin, micro, sems, 1).start()

            @pl.when((pipe == 0) & (micro == micros - 1))
            def _():
                for which in range(micros):
                    sent_on(res, xin, which, sems, 1).wait_send()


def attention_backward(d_mixed, group, q, k, v, trig, causal, with_output):
    cosine, sine, cosine2, sine2 = trig
    d_head = jnp.concatenate(
        [spread(d_mixed, 2 * group), spread(d_mixed, 2 * group + 1)], axis=0
    ).astype(jnp.bfloat16)
    weights = jnp.where(causal, jnp.exp(times_t(k, q) * SCALE), 0.0)
    probs = weights * (1.0 / jnp.sum(weights, axis=0, keepdims=True))
    moved = probs * times_t(v, d_head)
    delta = jnp.sum(moved, axis=0, keepdims=True)
    d_scores = ((moved - probs * delta) * SCALE).astype(jnp.bfloat16)
    rounded = probs.astype(jnp.bfloat16)
    d_value = dot(rounded, d_head)
    d_key = turned_back(dot(d_scores, q), cosine, sine)
    d_query = turned_back(over_rows(d_scores, k), cosine2, sine2)
    length = k.shape[0]
    mixed = over_rows(rounded, v) if with_output else d_query
    return (
        [d_query[:length], d_query[length:]],
        d_key,
        d_value,
        [mixed[:length], mixed[length:]],
    )


def backward_kernel(
    micros,
    cot,
    other,
    far_first,
    gains,
    tables,
    n1_own,
    n2_own,
    hidden,
    q_in,
    k_in,
    v_in,
    middle,
    gate_in,
    up_in,
    wq,
    wk,
    wv,
    wo,
    wg,
    wu,
    wd,
    grad_out,
    g_out,
    low_out,
    dgate_out,
    dup_out,
    dq_out,
    dk_out,
    dv_out,
    n1_far,
    n2_far,
    g_far,
    gain_out,
    xin,
    res,
    far_buf,
    far_gain,
    send,
    got,
    d_middle,
    acc,
    send_sem,
    recv_sem,
    x_send,
    x_recv,
    xp_send,
    xp_recv,
    far_sems,
    gain_send,
    gain_recv,
):
    micro, step = pl.program_id(0), pl.program_id(1)
    pipe, tensor, data = lax.axis_index("pipe"), lax.axis_index("tensor"), lax.axis_index("dp")
    peers = lax.axis_size("dp")
    partner = lax.rem(data + peers // 2, peers)
    sems = (x_send, x_recv, xp_send, xp_recv)
    length = hidden.shape[1]
    last = micros - 1
    far = FarCopies(xin, far_buf, far_sems, partner)

    def gain_copy():
        return pltpu.make_async_remote_copy(
            src_ref=gain_out,
            dst_ref=far_gain,
            send_sem=gain_send,
            recv_sem=gain_recv,
            device_id={"dp": partner},
            device_id_type=MESH,
        )

    @pl.when((micro == 0) & (step == 0))
    def _():
        greet([{"tensor": 1 - tensor}, {"pipe": 1 - pipe}, {"dp": partner}])
        gain_out[...] = jnp.zeros_like(gain_out)
        for which in range(1, micros):
            far.start(micros + which, n2_own.at[which])

        @pl.when(pipe == 1)
        def _():
            for which in range(1, micros):
                far.start(which, n1_own.at[which])
            g_far[...] = other[...]
            n1_far[0] = far_first[0]

        @pl.when(pipe == 0)
        def _():
            for which in range(micros):
                wide = other[which].astype(jnp.float32)
                n1_far[which] = (wide * rsqrt_mean(wide) * gains[0:1, :]).astype(jnp.bfloat16)

        n2_far[0] = far_first[1]

    @pl.when(step == 0)
    def _():
        @pl.when(pipe == 1)
        def _():
            g_out[0] = cot[micro]

        @pl.when(pipe == 0)
        def _():
            passed_on(xin, micro, sems, 1)
            far.start(micro)
            g_out[0] = xin[micro]

    @pl.when(step < HIDDEN_STEPS)
    def _():
        gate, up = gate_in[0].astype(jnp.float32), up_in[0].astype(jnp.float32)
        d_act = dot(g_out[0], wd[...])
        sig = jax.nn.sigmoid(gate)
        d_gate = (d_act * up * sig * (1.0 + gate * (1.0 - sig))).astype(jnp.bfloat16)
        d_up = (d_act * gate * sig).astype(jnp.bfloat16)
        dgate_out[0] = d_gate
        dup_out[0] = d_up

        @pl.when(step == 0)
        def _():
            acc[...] = times_t(d_gate, wg[...]) + times_t(d_up, wu[...])

        @pl.when((step > 0) & (step < HIDDEN_STEPS - 1))
        def _():
            acc[...] += times_t(d_gate, wg[...]) + times_t(d_up, wu[...])

        @pl.when(step == HIDDEN_STEPS - 1)
        def _():
            swap = Exchange(2 * micro, send, got, send_sem, recv_sem)
            for piece in range(SEND_PIECES):
                columns = slice(piece * swap.width, (piece + 1) * swap.width)
                swap.start(
                    piece,
                    acc[:, columns] + times_t(d_gate, wg[columns, :]) + times_t(d_up, wu[columns, :]),
                )
            swap.wait()
            d_normed = swap.total()
            mid = middle[0]
            scale = rsqrt_mean(mid)
            gain_out[1:2, :] += jnp.sum(d_normed * mid * scale, axis=0, keepdims=True)
            weighted = d_normed * gains[1:2, :]
            inner = jnp.mean(weighted * mid, axis=-1, keepdims=True)
            total = g_out[0].astype(jnp.float32) + scale * weighted - mid * (scale**3 * inner)
            d_middle[...] = total
            low_out[0] = total.astype(jnp.bfloat16)

    @pl.when(step == HIDDEN_STEPS)
    def _():
        d_mixed = dot(low_out[0], wo[...]).astype(jnp.bfloat16).astype(jnp.float32)
        trig, causal = trig_and_mask(tables, length)
        d_queries, d_keys, d_values = [], [], []
        for group in range(k_in.shape[1]):
            parts = attention_backward(
                d_mixed, group, q_in[0, group], k_in[0, group], v_in[0, group], trig, causal, False
            )
            d_queries += parts[0]
            d_keys.append(parts[1])
            d_values.append(parts[2])
        d_query = gathered(d_queries).astype(jnp.bfloat16)
        d_key = gathered(d_keys).astype(jnp.bfloat16)
        d_value = gathered(d_values).astype(jnp.bfloat16)
        dq_out[0] = d_query
        dk_out[0] = d_key
        dv_out[0] = d_value
        swap = Exchange(2 * micro + 1, send, got, send_sem, recv_sem)
        for piece in range(SEND_PIECES):
            part = slice(piece * swap.width, (piece + 1) * swap.width)
            swap.start(
                piece,
                times_t(d_query, wq[part, :]) + times_t(d_key, wk[part, :]) + times_t(d_value, wv[part, :]),
            )
        swap.wait()
        d_first = swap.total()
        wide = hidden[0].astype(jnp.float32)
        scale = rsqrt_mean(wide)
        gain_out[0:1, :] += jnp.sum(d_first * wide * scale, axis=0, keepdims=True)
        weighted = d_first * gains[0:1, :]
        inner = jnp.mean(weighted * wide, axis=-1, keepdims=True)
        d_hidden = (d_middle[...] + scale * weighted - wide * (scale**3 * inner)).astype(jnp.bfloat16)
        grad_out[0] = d_hidden

        @pl.when(pipe == 1)
        def _():
            res[micro] = d_hidden
            sent_on(res, xin, micro, sems, 0).start()

        @pl.when(micro == last)
        def _():
            gain_copy().start()
            for which in range(1, micros):
                far.receive(micros + which)
                n2_far[which] = far_buf[micros + which]

            @pl.when(pipe == 1)
            def _():
                for which in range(1, micros):
                    far.receive(which)
                    n1_far[which] = far_buf[which]

            @pl.when(pipe == 0)
            def _():
                for which in range(micros):
                    far.receive(which)
                    g_far[which] = far_buf[which]

            gain_copy().wait()
            gain_out[...] += far_gain[...]

            @pl.when(pipe == 1)
            def _():
                for which in range(micros):
                    sent_on(res, xin, which, sems, 0).wait_send()


def trig_and_mask(tables, length):
    cosine, sine = tables[0], tables[1]
    trig = (
        cosine,
        sine,
        jnp.concatenate([cosine, cosine], axis=0),
        jnp.concatenate([sine, sine], axis=0),
    )
    at_k = lax.broadcasted_iota(jnp.int32, (length, 2 * length), 0)
    at_q = lax.rem(lax.broadcasted_iota(jnp.int32, (length, 2 * length), 1), length)
    return trig, at_q >= at_k


def forward(inputs, cotangents, gains, tables, weights):
    micros, length, width = inputs.shape
    wq, wk, wv, wo, wg, wu, wd = weights
    groups = wk.shape[1] // HEAD_SIZE
    hidden = wg.shape[1]
    block = hidden // HIDDEN_STEPS
    low, wide = jnp.bfloat16, jnp.float32

    def whole(array):
        return pl.BlockSpec(
            array.shape, lambda m, s: (0,) * array.ndim, pipeline_mode=pl.Buffered(1)
        )

    def streamed(array):
        return pl.BlockSpec((width, block), lambda m, s: (0, jnp.maximum(s - 1, 0)))

    def by_micro(*shape):
        return pl.BlockSpec((1,) + shape, lambda m, s: (m,) + (0,) * len(shape))

    by_block = pl.BlockSpec((1, length, block), lambda m, s: (m, 0, jnp.maximum(s - 1, 0)))
    shapes = [
        ((length, width), low),
        ((length, width), low),
        ((length, width), low),
        ((groups, 2 * length, LANES), low),
        ((groups, length, LANES), low),
        ((groups, length, LANES), low),
        ((length, wq.shape[1]), low),
        ((length, width), wide),
        ((length, width), low),
    ]
    out_shape = [jax.ShapeDtypeStruct((micros,) + shape, kind) for shape, kind in shapes]
    out_specs = [by_micro(*shape) for shape, _ in shapes]
    out_shape += [jax.ShapeDtypeStruct((micros, length, hidden), low)] * 3
    out_specs += [by_block] * 3
    out_shape += [jax.ShapeDtypeStruct(inputs.shape, low)] * 2
    out_specs += [whole(inputs)] * 2
    return pl.pallas_call(
        functools.partial(forward_kernel, micros),
        grid=(micros, HIDDEN_STEPS + 1),
        out_shape=out_shape,
        in_specs=[
            whole(inputs),
            pl.BlockSpec(memory_space=pl.ANY),
            whole(gains),
            whole(tables),
            whole(wq),
            whole(wk),
            whole(wv),
            whole(wo),
            streamed(wg),
            streamed(wu),
            streamed(wd),
        ],
        out_specs=out_specs,
        scratch_shapes=[
            pltpu.VMEM((micros, length, width), low),
            pltpu.VMEM((2, length, width), low),
            pltpu.VMEM((2, length, width), low),
            pltpu.VMEM((micros, length, width), low),
            pltpu.VMEM((micros, length, width), low),
            pltpu.VMEM((length, width), low),
            pltpu.VMEM((2 * micros, length, width), low),
            pltpu.VMEM((length, width), wide),
            pltpu.VMEM((length, width), wide),
            pltpu.VMEM((length, width), low),
            pltpu.SemaphoreType.DMA((2 * micros, SEND_PIECES)),
            pltpu.SemaphoreType.DMA((2 * micros, SEND_PIECES)),
            pltpu.SemaphoreType.DMA((micros,)),
            pltpu.SemaphoreType.DMA((micros,)),
            pltpu.SemaphoreType.DMA((micros,)),
            pltpu.SemaphoreType.DMA((micros,)),
            pltpu.SemaphoreType.DMA,
            pltpu.SemaphoreType.DMA,
            pltpu.SemaphoreType.DMA,
            pltpu.SemaphoreType.DMA,
            pltpu.SemaphoreType.DMA((2, 4)),
        ],
        compiler_params=pltpu.CompilerParams(
            collective_id=0, has_side_effects=True, vmem_limit_bytes=62 * MIB
        ),
    )(inputs, cotangents, gains, tables, wq, wk, wv, wo, wg, wu, wd)


def backward(cotangents, other, far_first, gains, tables, n1, n2, record, weights):
    micros, length, width = cotangents.shape
    wq, wk, wv, wo, wg, wu, wd = weights
    groups = wk.shape[1] // HEAD_SIZE
    hidden = wg.shape[1]
    block = hidden // HIDDEN_STEPS
    last = HIDDEN_STEPS - 1
    low, wide = jnp.bfloat16, jnp.float32

    def whole(array):
        return pl.BlockSpec(
            array.shape, lambda m, s: (0,) * array.ndim, pipeline_mode=pl.Buffered(1)
        )

    def streamed(array):
        return pl.BlockSpec((width, block), lambda m, s: (0, jnp.minimum(s, last)))

    def by_micro(*shape):
        return pl.BlockSpec((1,) + shape, lambda m, s: (m,) + (0,) * len(shape))

    by_block = pl.BlockSpec((1, length, block), lambda m, s: (m, 0, jnp.minimum(s, last)))
    heads, pairs = wq.shape[1], wk.shape[1]
    columns = [width, width, width, hidden, hidden, heads, pairs, pairs, width, width, width]
    specs = [by_micro(length, width)] * 3 + [by_block] * 2
    specs += [by_micro(length, heads)] + [by_micro(length, pairs)] * 2 + [whole(other)] * 3
    out_shape = [jax.ShapeDtypeStruct((micros, length, size), low) for size in columns]
    out_shape.append(jax.ShapeDtypeStruct(gains.shape, wide))
    row = pltpu.SemaphoreType.DMA((micros,))
    swaps = pltpu.SemaphoreType.DMA((2 * micros, SEND_PIECES))
    return pl.pallas_call(
        functools.partial(backward_kernel, micros),
        grid=(micros, HIDDEN_STEPS + 1),
        out_shape=out_shape,
        in_specs=[
            whole(cotangents),
            whole(other),
            whole(far_first),
            whole(gains),
            whole(tables),
            pl.BlockSpec(memory_space=pl.ANY),
            pl.BlockSpec(memory_space=pl.ANY),
            by_micro(length, width),
            by_micro(groups, 2 * length, LANES),
            by_micro(groups, length, LANES),
            by_micro(groups, length, LANES),
            by_micro(length, width),
            by_block,
            by_block,
            whole(wq),
            whole(wk),
            whole(wv),
            whole(wo),
            streamed(wg),
            streamed(wu),
            streamed(wd),
        ],
        out_specs=specs + [whole(gains)],
        scratch_shapes=[
            pltpu.VMEM((micros, length, width), low),
            pltpu.VMEM((micros, length, width), low),
            pltpu.VMEM((2 * micros, length, width), low),
            pltpu.VMEM(gains.shape, wide),
            pltpu.VMEM((length, width), low),
            pltpu.VMEM((2 * micros, length, width), low),
            pltpu.VMEM((length, width), wide),
            pltpu.VMEM((length, width), wide),
            swaps,
            swaps,
            row,
            row,
            row,
            row,
            pltpu.SemaphoreType.DMA((2 * micros, 4)),
            pltpu.SemaphoreType.DMA,
            pltpu.SemaphoreType.DMA,
        ],
        compiler_params=pltpu.CompilerParams(
            collective_id=1, has_side_effects=True, vmem_limit_bytes=62 * MIB
        ),
    )(cotangents, other, far_first, gains, tables, n1, n2, *record, wq, wk, wv, wo, wg, wu, wd)


BLOCKS = 8
PART = 3 * LANES


class Halving:
    def __init__(self, bits, local, got, sems, outputs):
        self.bits, self.local, self.got, self.sems, self.outputs = bits, local, got, sems, outputs
        me = lax.axis_index("dp")
        self.own = [lax.rem(lax.div(me, 2**bit), 2) for bit in range(bits)]
        self.flip = [me + (1 - 2 * self.own[bit]) * 2**bit for bit in range(bits)]
        plain = list(range(bits))
        self.orders = [plain, [1, 0] + plain[2:] if bits > 1 else plain]

    def copy(self, block, half, level):
        order = self.orders[half]
        done, now = order[:level], order[level]
        spot = []
        for bit in reversed(range(self.bits)):
            if bit in done:
                spot.append(self.own[bit])
            else:
                spot.append(1 - self.own[bit] if bit == now else slice(None))
        return pltpu.make_async_remote_copy(
            src_ref=self.local.at[(block, half) + tuple(spot)],
            dst_ref=self.got[level].at[block, half],
            send_sem=self.sems.at[block, half, level, 0],
            recv_sem=self.sems.at[block, half, level, 1],
            device_id={"dp": self.flip[now]},
            device_id_type=MESH,
        )

    def begin(self, block):
        for half in range(2):
            self.copy(block, half, 0).start()

    def advance(self, block, level):
        for half in range(2):
            order = self.orders[half]
            self.copy(block, half, level).wait()
            done = order[: level + 1]
            left = [bit for bit in reversed(range(self.bits)) if bit not in done]
            rows = self.local.shape[-2]
            piece = 64 if rows % 64 == 0 else rows
            for combo in range(2 ** len(left)):
                fixed = {bit: (combo >> index) & 1 for index, bit in enumerate(left)}
                from_spot = (block, half) + tuple(fixed[bit] for bit in left)
                for bit in done:
                    fixed[bit] = self.own[bit]
                spot = (block, half) + tuple(fixed[bit] for bit in reversed(range(self.bits)))

                def add(index, _):
                    where = pl.ds(pl.multiple_of(index * piece, piece), piece)
                    a = self.local[spot + (where, slice(None))].astype(jnp.float32)
                    b = self.got[level][from_spot + (where, slice(None))].astype(jnp.float32)
                    if level == self.bits - 1:
                        self.outputs(block, half, where, (a + b).astype(jnp.bfloat16))
                    else:
                        self.local[spot + (where, slice(None))] = (a + b).astype(jnp.bfloat16)
                    return 0

                lax.fori_loop(0, rows // piece, add, 0)
            if level < self.bits - 1:
                self.copy(block, half, level + 1).start()


def gradient_kernel(
    bits,
    micros,
    n1_rows,
    n2_rows,
    g_rows,
    low_rows,
    low_own,
    act_own,
    dgate_own,
    dup_own,
    dq_own,
    dk_own,
    dv_own,
    o_own,
    n1_far,
    n2_far,
    g_far,
    tables,
    gain_in,
    wq,
    wk,
    wv,
    wo,
    wg,
    wu,
    wd,
    gate_out,
    up_out,
    down_out,
    q_out,
    k_out,
    v_out,
    o_out,
    gain_out,
    far_low,
    heads_far,
    local,
    *rest,
):
    step = pl.program_id(0)
    got, small_got = rest[:bits], rest[bits + 1 : 2 * bits + 1]
    small = rest[bits]
    far_sems, sems, small_sems = rest[2 * bits + 1 :]
    tensor, data = lax.axis_index("tensor"), lax.axis_index("dp")
    peers = lax.axis_size("dp")
    partner = lax.rem(data + peers // 2, peers)
    length, width = far_low.shape[1:]
    size = width // 2
    rows = local.shape[-2]
    top = lax.div(data, peers // 2)
    lanes = pl.ds(pl.multiple_of(top * size, LANES), size)
    far = FarCopies(low_own, far_low, far_sems, partner)
    count = local.shape[0]

    def small_output(block, half, where, value):
        gain_out[half, where, :] = value

    def output(block, half, where, value):
        if isinstance(block, int):
            target, at = [
                [(q_out, 0), (q_out, PART)],
                [(k_out, 0), (v_out, 0)],
                [(o_out, 0), (o_out, PART)],
            ][block - BLOCKS][half]
            target[where, at : at + PART] = value
        else:
            at = pl.ds(pl.multiple_of(block * 2 * LANES + half * LANES, LANES), LANES)
            for index, target in enumerate((gate_out, up_out, down_out)):
                target[where, at] = value[:, index * LANES : (index + 1) * LANES]

    halving = Halving(bits, local, got, sems, output)
    gains = Halving(bits, small, small_got, small_sems, small_output)

    @pl.when(step == 0)
    def _():
        greet(
            [{"tensor": 1 - tensor}, {"dp": partner}] + [{"dp": halving.flip[bit]} for bit in range(bits)]
        )
        for which in range(micros):
            far.start(which)
        small[...] = gain_in[...]
        gains.begin(0)

    def blocked(value):
        return value.astype(jnp.bfloat16).reshape((2,) * bits + (rows, value.shape[1]))

    @pl.when(step < BLOCKS)
    def _():
        n2, g = n2_far[...], g_far[...]
        gate, up = dot(n2, wg[...]), dot(n2, wu[...])
        d_act = dot(g, wd[...])
        sig = jax.nn.sigmoid(gate)
        act = (gate * sig * up).astype(jnp.bfloat16)
        d_gate = (d_act * up * sig * (1.0 + gate * (1.0 - sig))).astype(jnp.bfloat16)
        d_up = (d_act * gate * sig).astype(jnp.bfloat16)
        parts = (
            (n2_rows, dgate_own, n2_far, d_gate),
            (n2_rows, dup_own, n2_far, d_up),
            (g_rows, act_own, g_far, act),
        )
        for index, (left, right, left_far, right_far) in enumerate(parts):
            total = over_rows(left[...], right[...]) + over_rows(left_far[:, lanes], right_far)
            for half in range(2):
                spot = (step, half) + (slice(None),) * (bits + 1)
                local[spot + (slice(index * LANES, (index + 1) * LANES),)] = blocked(
                    total[:, half * LANES : (half + 1) * LANES]
                )
        halving.begin(step)

    @pl.when((step > 0) & (step <= BLOCKS))
    def _():
        halving.advance(step - 1, 0)

    @pl.when((step >= BLOCKS) & (step < BLOCKS + micros))
    def _():
        which = step - BLOCKS
        far.receive(which)
        low = far_low[which]
        n1 = n1_far[pl.ds(pl.multiple_of(which * length, length), length), :]
        query, keys, values = dot(n1, wq[...]), dot(n1, wk[...]), dot(n1, wv[...])
        d_mixed = dot(low, wo[...]).astype(jnp.bfloat16).astype(jnp.float32)
        trig, causal = trig_and_mask(tables, length)
        cosine, sine, cosine2, sine2 = trig
        d_queries, d_keys, d_values, outs = [], [], [], []
        for group in range(wk.shape[1] // HEAD_SIZE):
            q = jnp.concatenate([spread(query, 2 * group), spread(query, 2 * group + 1)], axis=0)
            q = turned(q, cosine2, sine2).astype(jnp.bfloat16)
            k = turned(spread(keys, group), cosine, sine).astype(jnp.bfloat16)
            v = spread(values, group).astype(jnp.bfloat16)
            parts = attention_backward(d_mixed, group, q, k, v, trig, causal, True)
            d_queries += parts[0]
            d_keys.append(parts[1])
            d_values.append(parts[2])
            outs += parts[3]
        at = 0
        for item in (d_queries, d_keys, d_values, outs):
            item = gathered(item).astype(jnp.bfloat16)
            heads_far[which, :, at : at + item.shape[1]] = item
            at += item.shape[1]

    @pl.when(step == BLOCKS + micros)
    def _():
        low_far = far_low[:, :, lanes].reshape(micros * length, size)
        right_far = heads_far[...].reshape(micros * length, heads_far.shape[2])
        plan = [
            (n1_rows, dq_own, 0),
            (n1_rows, dq_own, PART),
            (n1_rows, dk_own, 0),
            (n1_rows, dv_own, 0),
            (low_rows, o_own, 0),
            (low_rows, o_own, PART),
        ]
        for index, (left, right, at) in enumerate(plan):
            left_far = low_far if left is low_rows else n1_far[:, lanes]
            total = over_rows(left[...], right[:, at : at + PART]) + over_rows(
                left_far, right_far[:, index * PART : (index + 1) * PART]
            )
            local[BLOCKS + index // 2, index % 2] = blocked(total)
            if index % 2:
                halving.begin(BLOCKS + index // 2)
        gains.advance(0, 0)
        for level in range(1, bits):

            def advanced(block, _):
                halving.advance(block, level)
                return 0

            lax.fori_loop(0, BLOCKS, advanced, 0)
            gains.advance(0, level)
        for level in range(bits):
            for block in range(BLOCKS, count):
                halving.advance(block, level)


def gradients(bits, n1_far, low_own, own, far, tables, gain, weights):
    wq, wk, wv, wo, wg, wu, wd = weights
    micros, length, width = low_own.shape
    n1_rows, n2_rows, g_rows, low_rows, act, d_gate, d_up, d_q, d_k, d_v, mixed = own
    n2_far, g_far = far
    hidden = wg.shape[1]
    block = hidden // BLOCKS
    rows = width // 2 ** (bits + 1)
    low = jnp.bfloat16
    count = BLOCKS + (d_q.shape[1] + d_k.shape[1] + d_v.shape[1] + mixed.shape[1]) // (2 * PART)

    def whole(array):
        return pl.BlockSpec(array.shape, lambda s: (0,) * array.ndim, pipeline_mode=pl.Buffered(1))

    def streamed(array):
        return pl.BlockSpec((array.shape[0], block), lambda s: (0, jnp.minimum(s, BLOCKS - 1)))

    any_space = pl.BlockSpec(memory_space=pl.ANY)
    args = [
        (n1_rows, whole),
        (n2_rows, whole),
        (g_rows, whole),
        (low_rows, whole),
        (low_own, None),
        (act, streamed),
        (d_gate, streamed),
        (d_up, streamed),
        (d_q, whole),
        (d_k, whole),
        (d_v, whole),
        (mixed, whole),
        (n1_far, whole),
        (n2_far, whole),
        (g_far, whole),
        (tables, whole),
        (gain, whole),
        (wq, whole),
        (wk, whole),
        (wv, whole),
        (wo, whole),
        (wg, streamed),
        (wu, streamed),
        (wd, streamed),
    ]
    sizes = [hidden] * 3 + [d_q.shape[1], d_k.shape[1], d_v.shape[1], mixed.shape[1]]
    out_shape = [jax.ShapeDtypeStruct((rows, size), low) for size in sizes]
    small_rows = gain.shape[-2]
    out_shape.append(jax.ShapeDtypeStruct((2, small_rows, LANES), low))

    def levels(lead, tail):
        return [pltpu.VMEM(lead + (2,) * (bits - 1 - level) + tail, low) for level in range(bits)]

    scratch = [
        pltpu.VMEM((micros, length, width), low),
        pltpu.VMEM((micros, length, (count - BLOCKS) * 2 * PART), low),
        pltpu.VMEM((count, 2) + (2,) * bits + (rows, PART), low),
    ]
    scratch += levels((count, 2), (rows, PART))
    scratch.append(pltpu.VMEM((1, 2) + (2,) * bits + (small_rows, LANES), low))
    scratch += levels((1, 2), (small_rows, LANES))
    scratch += [
        pltpu.SemaphoreType.DMA((micros, 4)),
        pltpu.SemaphoreType.DMA((count, 2, bits, 2)),
        pltpu.SemaphoreType.DMA((1, 2, bits, 2)),
    ]
    return pl.pallas_call(
        functools.partial(gradient_kernel, bits, micros),
        grid=(BLOCKS + micros + 1,),
        out_shape=out_shape,
        in_specs=[any_space if spec is None else spec(array) for array, spec in args],
        out_specs=[whole(shape) for shape in out_shape],
        scratch_shapes=scratch,
        compiler_params=pltpu.CompilerParams(
            collective_id=2, has_side_effects=True, vmem_limit_bytes=63 * MIB
        ),
    )(*(array for array, _ in args))


def body(
    inputs,
    cotangents,
    norm_scales,
    w_query,
    key_weight,
    value_weight,
    w_out,
    w_gate,
    w_up,
    down_weight,
):
    weights = (
        w_query[0],
        key_weight[0],
        value_weight[0],
        w_out[0],
        w_gate[0],
        w_up[0],
        down_weight[0],
    )
    _, _, length, width = inputs.shape
    gains = norm_scales[0].T
    tables = jnp.asarray(rope_tables(length))
    cots = cotangents[:, 0]
    (
        result,
        hidden,
        n1,
        q,
        k,
        v,
        mixed,
        middle,
        n2,
        gate,
        up,
        act,
        other,
        far_first,
    ) = forward(inputs[:, 0], cots, gains, tables, weights)
    grad, g, low, d_gate, d_up, d_q, d_k, d_v, n1_far, n2_far, g_far, gain = backward(
        cots, other, far_first, gains, tables, n1, n2, (hidden, q, k, v, middle, gate, up), weights
    )
    peers = lax.axis_size("dp")
    bits = peers.bit_length() - 2
    top = lax.div(lax.axis_index("dp"), peers // 2)

    def flat(values):
        return values.reshape(-1, values.shape[-1])

    def rows_of(values):
        return lax.dynamic_slice_in_dim(flat(values), top * (width // 2), width // 2, 1)

    gain_rows = lax.dynamic_slice_in_dim(gain, top * (width // 2), width // 2, 1).T
    gain_rows = gain_rows.astype(jnp.bfloat16).reshape(peers // 2, -1)
    gain_size = gain_rows.shape[1]
    gain_rows = jnp.pad(gain_rows, ((0, 0), (0, 16 * LANES - gain_size)))
    gain_rows = gain_rows.reshape((2,) * bits + (16, LANES))
    gain_rows = jnp.stack([gain_rows, jnp.zeros_like(gain_rows)])[None]
    *shards, small = gradients(
        bits,
        flat(n1_far),
        low,
        (rows_of(n1), rows_of(n2), rows_of(g), rows_of(low))
        + tuple(flat(item) for item in (act, d_gate, d_up, d_q, d_k, d_v, mixed)),
        (flat(n2_far), flat(g_far)),
        tables,
        gain_rows,
        weights,
    )
    grad_scales = small[0].astype(jnp.float32).reshape(-1)[:gain_size].reshape(1, -1, 2)
    grad_gate, grad_up, grad_down, grad_query, grad_key, grad_value, grad_proj = (
        shard.astype(jnp.float32)[None] for shard in shards
    )
    return (
        result[None, :, None],
        grad[None, :, None],
        grad_scales,
        grad_query,
        grad_key,
        grad_value,
        grad_proj,
        grad_gate,
        grad_up,
        grad_down,
    )


def solution(mesh):
    placed = (
        P(None, "dp", None, None),
        P(None, "dp", None, None),
        P("pipe", None, None),
        P("pipe", None, "tensor"),
        P("pipe", None, "tensor"),
        P("pipe", None, "tensor"),
        P("pipe", None, "tensor"),
        P("pipe", None, "tensor"),
        P("pipe", None, "tensor"),
        P("pipe", None, "tensor"),
    )
    return jax.shard_map(
        body,
        mesh=mesh,
        in_specs=placed,
        out_specs=(
            P("pipe", None, "dp", None, None),
            P("pipe", None, "dp", None, None),
            P("pipe", "dp", None),
            P("pipe", "dp", "tensor"),
            P("pipe", "dp", "tensor"),
            P("pipe", "dp", "tensor"),
            P("pipe", "dp", "tensor"),
            P("pipe", "dp", "tensor"),
            P("pipe", "dp", "tensor"),
            P("pipe", "dp", "tensor"),
        ),
        check_vma=False,
    )
```

```python
import functools

import jax
import jax.numpy as jnp
import numpy as np
from jax import lax
from jax.experimental import pallas as pl
from jax.experimental.pallas import tpu as pltpu
from jax.sharding import PartitionSpec as P

HEAD_SIZE = 96
HALF = HEAD_SIZE // 2
LANES = 128
FORWARD_STEPS = 2
BACKWARD_STEPS = 2
SEND_PIECES = 3

EPS = 1e-05
THETA = 100000.0
MESH = pl.DeviceIdType.MESH
VMEM_LIMIT = 67043328
SCALE = HEAD_SIZE ** (-0.5)


def rope_tables(length):
    freqs = (THETA ** (-(np.arange(HALF, dtype=np.float64) * 2.0 / HEAD_SIZE))).astype(np.float32)
    angles = np.arange(length, dtype=np.float32)[:, None] * freqs[None, :]
    cosine, sine = np.cos(angles), np.sin(angles)
    room = np.zeros((length, LANES // 2 - HALF), np.float32)
    return np.concatenate([cosine, room, sine, room], axis=1).astype(np.float32)


def dot(left, right):
    return lax.dot_general(
        left, right, (((1,), (0,)), ((), ())), preferred_element_type=jnp.float32
    )


def times_t(left, right):
    return lax.dot_general(
        left, right, (((1,), (1,)), ((), ())), preferred_element_type=jnp.float32
    )


def over_rows(left, right):
    return lax.dot_general(
        left, right, (((0,), (0,)), ((), ())), preferred_element_type=jnp.float32
    )


def spread(values, head):
    room = jnp.zeros((values.shape[0], LANES // 2 - HALF), values.dtype)
    at = head * HEAD_SIZE
    return jnp.concatenate(
        [values[:, at : at + HALF], room, values[:, at + HALF : at + HEAD_SIZE], room], axis=1
    )


def gathered(heads):
    parts = []
    for head in heads:
        parts += [head[:, :HALF], head[:, LANES // 2 : LANES // 2 + HALF]]
    return jnp.concatenate(parts, axis=1)


def turned(values, cosine, sine):
    return values * cosine + pltpu.roll(values, LANES // 2, 1) * sine


def turned_back(values, cosine, sine):
    return values * cosine - pltpu.roll(values, LANES // 2, 1) * sine


def rsqrt_mean(values):
    return lax.rsqrt(jnp.mean(values * values, axis=-1, keepdims=True) + EPS)


class Exchange:
    def __init__(self, number, send, got, send_sem, recv_sem):
        self.number, self.send, self.got = number, send, got
        self.send_sem, self.recv_sem = send_sem, recv_sem
        self.width = send.shape[1] // SEND_PIECES
        self.slot = lax.rem(number, got.shape[0])

    def copy(self, piece):
        columns = pl.ds(piece * self.width, self.width)
        return pltpu.make_async_remote_copy(
            src_ref=self.send.at[:, columns],
            dst_ref=self.got.at[self.slot, :, columns],
            send_sem=self.send_sem.at[self.number, piece],
            recv_sem=self.recv_sem.at[self.number, piece],
            device_id={"tensor": 1 - lax.axis_index("tensor")},
            device_id_type=MESH,
        )

    def start(self, piece, partial_value):
        columns = pl.ds(piece * self.width, self.width)
        self.send[:, columns] = partial_value.astype(jnp.bfloat16)
        self.copy(piece).start()

    def wait(self):
        for piece in range(SEND_PIECES):
            self.copy(piece).wait()

    def total(self):
        return self.send[...].astype(jnp.float32) + self.got[self.slot].astype(jnp.float32)


def half_copy(source, target, rows, send_sem, recv_sem, device):
    return pltpu.make_async_remote_copy(
        src_ref=source.at[rows],
        dst_ref=target.at[rows],
        send_sem=send_sem,
        recv_sem=recv_sem,
        device_id=device,
        device_id_type=MESH,
    )


def passed_on(xin, micro, sems, stage_from):
    tensor = lax.axis_index("tensor")
    rows = xin.shape[1] // 2
    send_sem, recv_sem, pair_send, pair_recv = sems
    slot = xin.at[micro]
    mine = pl.ds(pl.multiple_of(tensor * rows, rows), rows)
    theirs = pl.ds(pl.multiple_of((1 - tensor) * rows, rows), rows)
    half_copy(
        slot, slot, mine, send_sem.at[micro], recv_sem.at[micro], {"pipe": stage_from}
    ).wait_recv()
    copy = half_copy(
        slot, slot, mine, pair_send.at[micro], pair_recv.at[micro], {"tensor": 1 - tensor}
    )
    copy.start()
    half_copy(
        slot, slot, theirs, pair_send.at[micro], pair_recv.at[micro], {"tensor": 1 - tensor}
    ).wait_recv()
    copy.wait_send()


def sent_on(source, xin, micro, sems, stage_to):
    tensor = lax.axis_index("tensor")
    rows = xin.shape[1] // 2
    mine = pl.ds(pl.multiple_of(tensor * rows, rows), rows)
    return half_copy(
        source.at[micro], xin.at[micro], mine, sems[0].at[micro], sems[1].at[micro], {"pipe": stage_to}
    )


class Resident:
    def __init__(self, sources, targets, sems, steps):
        attention, hidden = range(4), range(4, len(sources))
        block = targets[4].shape[1] // steps
        self.copies = {}
        for index in attention:
            self.copies[index, 0] = pltpu.make_async_copy(
                sources[index], targets[index], sems.at[index, 0]
            )
        for index in hidden:
            for step in range(steps):
                columns = pl.ds(step * block, block)
                self.copies[index, step] = pltpu.make_async_copy(
                    sources[index].at[:, columns], targets[index].at[:, columns], sems.at[index, step]
                )
        self.parts = {"attention": [(index, 0) for index in attention]}
        for step in range(steps):
            self.parts[step] = [(index, step) for index in hidden]

    def start(self, *parts):
        for part in parts:
            for key in self.parts[part]:
                self.copies[key].start()

    def wait(self, part):
        for key in self.parts[part]:
            self.copies[key].wait()


def half_lanes(width):
    top = lax.div(lax.axis_index("dp"), lax.axis_size("dp") // 2)
    return pl.ds(pl.multiple_of(top * (width // 2), LANES), width // 2)


def greet(devices):
    barrier = pltpu.get_barrier_semaphore()
    for device in devices:
        pl.semaphore_signal(barrier, inc=1, device_id=device, device_id_type=MESH)
    pl.semaphore_wait(barrier, len(devices))


class FarCopies:
    def __init__(self, sources, buffers, sems, partner):
        self.sources, self.buffers, self.sems, self.partner = sources, buffers, sems, partner
        tensor = lax.axis_index("tensor")
        self.pair = {"tensor": 1 - tensor}
        rows = buffers.shape[1] // 2
        self.mine = pl.ds(pl.multiple_of(tensor * rows, rows), rows)
        self.theirs = pl.ds(pl.multiple_of((1 - tensor) * rows, rows), rows)

    def far(self, which, source=None):
        source = self.sources.at[which] if source is None else source
        sems = self.sems.at[which, 0], self.sems.at[which, 1]
        return half_copy(source, self.buffers.at[which], self.mine, *sems, {"dp": self.partner})

    def near(self, which, rows):
        slot = self.buffers.at[which]
        sems = self.sems.at[which, 2], self.sems.at[which, 3]
        return half_copy(slot, slot, rows, *sems, self.pair)

    def start(self, which, source=None):
        self.far(which, source).start()

    def receive(self, which):
        self.far(which, self.buffers.at[which]).wait()
        self.near(which, self.mine).start()
        self.near(which, self.theirs).wait_recv()
        self.near(which, self.mine).wait_send()


def forward_kernel(
    micros,
    inp,
    cot,
    gains,
    tables,
    *refs,
):
    weights_in, refs = refs[:7], refs[7:]
    forward_steps(micros, inp, cot, gains, tables, weights_in, *refs)


def forward_steps(
    micros,
    inp,
    cot,
    gains,
    tables,
    weights_in,
    result_out,
    hidden_out,
    n1_out,
    q_out,
    k_out,
    v_out,
    o_out,
    middle_out,
    n1_rows,
    n2_rows,
    gate_out,
    up_out,
    act_out,
    other_out,
    far_out,
    other,
    first_buf,
    far_buf,
    xin,
    res,
    send,
    got,
    middle,
    acc,
    n2_buf,
    send_sem,
    recv_sem,
    x_send,
    x_recv,
    xp_send,
    xp_recv,
    far_send,
    far_recv,
    near_send,
    near_recv,
    far_sems,
    weight_sems,
    wq,
    wk,
    wv,
    wo,
    wg,
    wu,
    wd,
):
    micro, step = pl.program_id(0), pl.program_id(1)
    pipe, tensor, data = lax.axis_index("pipe"), lax.axis_index("tensor"), lax.axis_index("dp")
    peers = lax.axis_size("dp")
    partner = lax.rem(data + peers // 2, peers)
    sems = (x_send, x_recv, xp_send, xp_recv)
    length = inp.shape[1]
    lanes = half_lanes(inp.shape[2])

    def far_copy(source):
        return pltpu.make_async_remote_copy(
            src_ref=source.at[tensor],
            dst_ref=other.at[tensor],
            send_sem=far_send,
            recv_sem=far_recv,
            device_id={"dp": partner},
            device_id_type=MESH,
        )

    def near_copy(which):
        return pltpu.make_async_remote_copy(
            src_ref=other.at[which],
            dst_ref=other.at[which],
            send_sem=near_send,
            recv_sem=near_recv,
            device_id={"tensor": 1 - tensor},
            device_id_type=MESH,
        )

    far = FarCopies(first_buf, far_buf, far_sems, partner)

    resident = Resident(weights_in, (wq, wk, wv, wo, wg, wu, wd), weight_sems, FORWARD_STEPS)

    @pl.when((micro == 0) & (step == 0))
    def _():
        resident.start("attention", *range(FORWARD_STEPS))
        greet([{"tensor": 1 - tensor}, {"pipe": 1 - pipe}, {"dp": partner}])

        @pl.when(pipe == 0)
        def _():
            far_copy(inp).start()

        @pl.when(pipe == 1)
        def _():
            far_copy(cot).start()

    @pl.when((micro == 0) & (step == 0))
    def _():
        resident.wait("attention")

    for number in range(FORWARD_STEPS):

        @pl.when((micro == 0) & (step == number + 1))
        def _():
            resident.wait(number)

    @pl.when(step == 0)
    def _():
        @pl.when(pipe == 0)
        def _():
            hidden_out[0] = inp[micro]

        @pl.when(pipe == 1)
        def _():
            passed_on(xin, micro, sems, 0)
            hidden_out[0] = xin[micro]

        wide = hidden_out[0].astype(jnp.float32)
        n1 = (wide * rsqrt_mean(wide) * gains[0:1, :]).astype(jnp.bfloat16)
        n1_out[0] = n1
        n1_rows[0] = n1_out[0, :, lanes]

        @pl.when((pipe == 1) & (micro == 0))
        def _():
            first_buf[0] = n1
            far.start(0)

        query = dot(n1, wq[...])
        keys = dot(n1, wk[...])
        values = dot(n1, wv[...])
        trig, causal = trig_and_mask(tables, length)
        cosine, sine, cosine2, sine2 = trig
        groups = k_out.shape[1]
        outs = []
        for group in range(groups):
            q = jnp.concatenate([spread(query, 2 * group), spread(query, 2 * group + 1)], axis=0)
            q = turned(q, cosine2, sine2).astype(jnp.bfloat16)
            k = turned(spread(keys, group), cosine, sine).astype(jnp.bfloat16)
            v = spread(values, group).astype(jnp.bfloat16)
            q_out[0, group] = q
            k_out[0, group] = k
            v_out[0, group] = v
            weights = jnp.where(causal, jnp.exp(times_t(k, q) * SCALE), 0.0)
            total = jnp.sum(weights, axis=0, keepdims=True)
            probs = (weights * (1.0 / total)).astype(jnp.bfloat16)
            mixed = over_rows(probs, v)
            outs += [mixed[:length], mixed[length:]]
        mixed = gathered(outs).astype(jnp.bfloat16)
        o_out[0] = mixed
        swap = Exchange(2 * micro, send, got, send_sem, recv_sem)
        for piece in range(SEND_PIECES):
            swap.start(piece, times_t(mixed, wo[piece * swap.width : (piece + 1) * swap.width, :]))
        swap.wait()
        both = hidden_out[0].astype(jnp.float32) + swap.total()
        middle[...] = both
        middle_low = both.astype(jnp.bfloat16)
        middle_out[0] = middle_low
        n2 = (both * rsqrt_mean(both) * gains[1:2, :]).astype(jnp.bfloat16)
        n2_buf[...] = n2
        n2_rows[0] = n2_buf[:, lanes]

        @pl.when((pipe == 0) & (micro == 0))
        def _():
            first_buf[0] = middle_low
            far.start(0)


    @pl.when(step > 0)
    def _():
        n2 = n2_buf[...]
        block = wg.shape[1] // FORWARD_STEPS
        columns = pl.ds(pl.multiple_of((step - 1) * block, block), block)
        gate = dot(n2, wg[:, columns])
        up = dot(n2, wu[:, columns])
        act = (gate * jax.nn.sigmoid(gate) * up).astype(jnp.bfloat16)
        gate_out[0] = gate.astype(jnp.bfloat16)
        up_out[0] = up.astype(jnp.bfloat16)
        act_out[0] = act
        product = times_t(act, wd[:, columns])

        @pl.when(step == 1)
        def _():
            acc[...] = product

        @pl.when((step > 1) & (step < FORWARD_STEPS))
        def _():
            acc[...] += product

        @pl.when(step == FORWARD_STEPS)
        def _():
            swap = Exchange(2 * micro + 1, send, got, send_sem, recv_sem)
            for piece in range(SEND_PIECES):
                part = slice(piece * swap.width, (piece + 1) * swap.width)
                swap.start(piece, acc[:, part] + product[:, part])
            swap.wait()
            result = (middle[...] + swap.total()).astype(jnp.bfloat16)
            result_out[0] = result

            @pl.when(pipe == 0)
            def _():
                res[micro] = result
                sent_on(res, xin, micro, sems, 1).start()


    @pl.when((micro == micros - 1) & (step == FORWARD_STEPS))
    def _():
        far_copy(inp).wait()
        near_copy(tensor).start()
        near_copy(1 - tensor).wait_recv()
        near_copy(tensor).wait_send()
        other_out[...] = other[...]
        far.receive(0)
        far_out[...] = far_buf[...]

    @pl.when((pipe == 0) & (micro == micros - 1) & (step == FORWARD_STEPS))
    def _():
        for which in range(micros):
            sent_on(res, xin, which, sems, 1).wait_send()


def attention_backward(d_mixed, group, q, k, v, trig, causal, with_output):
    cosine, sine, cosine2, sine2 = trig
    d_head = jnp.concatenate(
        [spread(d_mixed, 2 * group), spread(d_mixed, 2 * group + 1)], axis=0
    ).astype(jnp.bfloat16)
    weights = jnp.where(causal, jnp.exp(times_t(k, q) * SCALE), 0.0)
    probs = weights * (1.0 / jnp.sum(weights, axis=0, keepdims=True))
    moved = probs * times_t(v, d_head)
    delta = jnp.sum(moved, axis=0, keepdims=True)
    d_scores = ((moved - probs * delta) * SCALE).astype(jnp.bfloat16)
    rounded = probs.astype(jnp.bfloat16)
    d_value = dot(rounded, d_head)
    d_key = turned_back(dot(d_scores, q), cosine, sine)
    d_query = turned_back(over_rows(d_scores, k), cosine2, sine2)
    length = k.shape[0]
    mixed = over_rows(rounded, v) if with_output else d_query
    return (
        [d_query[:length], d_query[length:]],
        d_key,
        d_value,
        [mixed[:length], mixed[length:]],
    )


def backward_kernel(
    micros,
    cot,
    other,
    far_first,
    gains,
    tables,
    n1_own,
    middle_own,
    hidden,
    q_in,
    k_in,
    v_in,
    middle,
    gate_in,
    up_in,
    *refs,
):
    weights_in, refs = refs[:7], refs[7:]
    backward_steps(
        micros,
        cot,
        other,
        far_first,
        gains,
        tables,
        n1_own,
        middle_own,
        hidden,
        q_in,
        k_in,
        v_in,
        middle,
        gate_in,
        up_in,
        weights_in,
        *refs,
    )


def backward_steps(
    micros,
    cot,
    other,
    far_first,
    gains,
    tables,
    n1_own,
    middle_own,
    hidden,
    q_in,
    k_in,
    v_in,
    middle,
    gate_in,
    up_in,
    weights_in,
    grad_out,
    g_rows,
    low_rows,
    dgate_out,
    dup_out,
    dq_out,
    dk_out,
    dv_out,
    n1_far,
    n2_far,
    g_far,
    middle_far,
    gain_out,
    wq,
    wk,
    wv,
    wo,
    wg,
    wu,
    wd,
    xin,
    res,
    far_buf,
    n2_buf,
    far_gain,
    g_buf,
    low_buf,
    send,
    got,
    d_middle,
    acc,
    send_sem,
    recv_sem,
    x_send,
    x_recv,
    xp_send,
    xp_recv,
    far_sems,
    gain_send,
    gain_recv,
    in_sems,
    out_sems,
):
    micro, step = pl.program_id(0), pl.program_id(1)
    pipe, tensor, data = lax.axis_index("pipe"), lax.axis_index("tensor"), lax.axis_index("dp")
    peers = lax.axis_size("dp")
    partner = lax.rem(data + peers // 2, peers)
    sems = (x_send, x_recv, xp_send, xp_recv)
    length = hidden.shape[1]
    lanes = half_lanes(hidden.shape[2])
    last = micros - 1
    far = FarCopies(xin, far_buf, far_sems, partner)

    def gain_copy():
        return pltpu.make_async_remote_copy(
            src_ref=gain_out,
            dst_ref=far_gain,
            send_sem=gain_send,
            recv_sem=gain_recv,
            device_id={"dp": partner},
            device_id_type=MESH,
        )

    resident = Resident(weights_in, (wq, wk, wv, wo, wg, wu, wd), in_sems, BACKWARD_STEPS)

    def write(kind, which, source):
        target = (n1_far, n2_far, g_far, middle_far)[kind]
        return pltpu.make_async_copy(source, target.at[which], out_sems.at[kind, which])

    def far_middle(which, source):
        write(3, which, source).start()
        mid = source[...].astype(jnp.float32)
        n2_buf[which] = (mid * rsqrt_mean(mid) * gains[1:2, :]).astype(jnp.bfloat16)
        write(1, which, n2_buf.at[which]).start()

    @pl.when((micro == 0) & (step == 0))
    def _():
        resident.start(*range(BACKWARD_STEPS), "attention")
        greet([{"tensor": 1 - tensor}, {"pipe": 1 - pipe}, {"dp": partner}])
        gain_out[...] = jnp.zeros_like(gain_out)

        @pl.when(pipe == 1)
        def _():
            for which in range(micros):
                if which:
                    far.start(which, n1_own.at[which])
                far.start(micros + which, middle_own.at[which])
            write(0, 0, far_first.at[0]).start()
            for which in range(micros):
                write(2, which, other.at[which]).start()

        @pl.when(pipe == 0)
        def _():
            for which in range(1, micros):
                far.start(micros + which, middle_own.at[which])
            far_middle(0, far_first.at[0])
            for which in range(micros):
                wide = other[which].astype(jnp.float32)
                res[which] = (wide * rsqrt_mean(wide) * gains[0:1, :]).astype(jnp.bfloat16)
                write(0, which, res.at[which]).start()

    @pl.when(step == 0)
    def _():
        @pl.when(pipe == 1)
        def _():
            g_buf[...] = cot[micro]

        @pl.when(pipe == 0)
        def _():
            passed_on(xin, micro, sems, 1)
            far.start(micro)
            g_buf[...] = xin[micro]

        g_rows[0] = g_buf[:, lanes]

    @pl.when((micro == 0) & (step == BACKWARD_STEPS))
    def _():
        resident.wait("attention")

    for number in range(BACKWARD_STEPS):

        @pl.when((micro == 0) & (step == number))
        def _():
            resident.wait(number)

    @pl.when(step < BACKWARD_STEPS)
    def _():
        gate, up = gate_in[0].astype(jnp.float32), up_in[0].astype(jnp.float32)
        block = wg.shape[1] // BACKWARD_STEPS
        columns = pl.ds(pl.multiple_of(step * block, block), block)
        d_act = dot(g_buf[...], wd[:, columns])
        sig = jax.nn.sigmoid(gate)
        d_gate = (d_act * up * sig * (1.0 + gate * (1.0 - sig))).astype(jnp.bfloat16)
        d_up = (d_act * gate * sig).astype(jnp.bfloat16)
        dgate_out[0] = d_gate
        dup_out[0] = d_up

        product = times_t(d_gate, wg[:, columns]) + times_t(d_up, wu[:, columns])

        @pl.when(step == 0)
        def _():
            acc[...] = product

        @pl.when((step > 0) & (step < BACKWARD_STEPS - 1))
        def _():
            acc[...] += product

        @pl.when(step == BACKWARD_STEPS - 1)
        def _():
            swap = Exchange(2 * micro, send, got, send_sem, recv_sem)
            for piece in range(SEND_PIECES):
                part = slice(piece * swap.width, (piece + 1) * swap.width)
                swap.start(piece, acc[:, part] + product[:, part])
            swap.wait()
            d_normed = swap.total()
            mid = middle[0].astype(jnp.float32)
            scale = rsqrt_mean(mid)
            gain_out[1:2, :] += jnp.sum(d_normed * mid * scale, axis=0, keepdims=True)
            weighted = d_normed * gains[1:2, :]
            inner = jnp.mean(weighted * mid, axis=-1, keepdims=True)
            total = g_buf[...].astype(jnp.float32) + scale * weighted - mid * (scale**3 * inner)
            d_middle[...] = total
            low_buf[...] = total.astype(jnp.bfloat16)
            low_rows[0] = low_buf[:, lanes]

    @pl.when(step == BACKWARD_STEPS)
    def _():
        d_mixed = dot(low_buf[...], wo[...]).astype(jnp.bfloat16).astype(jnp.float32)
        trig, causal = trig_and_mask(tables, length)
        d_queries, d_keys, d_values = [], [], []
        for group in range(k_in.shape[1]):
            parts = attention_backward(
                d_mixed, group, q_in[0, group], k_in[0, group], v_in[0, group], trig, causal, False
            )
            d_queries += parts[0]
            d_keys.append(parts[1])
            d_values.append(parts[2])
        d_query = gathered(d_queries).astype(jnp.bfloat16)
        d_key = gathered(d_keys).astype(jnp.bfloat16)
        d_value = gathered(d_values).astype(jnp.bfloat16)
        dq_out[0] = d_query
        dk_out[0] = d_key
        dv_out[0] = d_value
        swap = Exchange(2 * micro + 1, send, got, send_sem, recv_sem)
        for piece in range(SEND_PIECES):
            part = slice(piece * swap.width, (piece + 1) * swap.width)
            swap.start(
                piece,
                times_t(d_query, wq[part, :]) + times_t(d_key, wk[part, :]) + times_t(d_value, wv[part, :]),
            )
        swap.wait()
        d_first = swap.total()
        wide = hidden[0].astype(jnp.float32)
        scale = rsqrt_mean(wide)
        gain_out[0:1, :] += jnp.sum(d_first * wide * scale, axis=0, keepdims=True)
        weighted = d_first * gains[0:1, :]
        inner = jnp.mean(weighted * wide, axis=-1, keepdims=True)
        d_hidden = (d_middle[...] + scale * weighted - wide * (scale**3 * inner)).astype(jnp.bfloat16)
        grad_out[0] = d_hidden

        @pl.when(pipe == 1)
        def _():
            res[micro] = d_hidden
            sent_on(res, xin, micro, sems, 0).start()

        @pl.when(micro == last)
        def _():
            gain_copy().start()
            for which in range(1, micros):
                far.receive(micros + which)
                far_middle(which, far_buf.at[micros + which])

            @pl.when(pipe == 1)
            def _():
                far.receive(micros)
                far_middle(0, far_buf.at[micros])
                for which in range(1, micros):
                    far.receive(which)
                    write(0, which, far_buf.at[which]).start()

            @pl.when(pipe == 0)
            def _():
                for which in range(micros):
                    far.receive(which)
                    write(2, which, far_buf.at[which]).start()

            for kind in range(4):
                for which in range(micros):
                    write(kind, which, far_buf.at[which]).wait()
            gain_copy().wait()
            gain_out[...] += far_gain[...]

            @pl.when(pipe == 1)
            def _():
                for which in range(micros):
                    sent_on(res, xin, which, sems, 0).wait_send()


def trig_and_mask(tables, length):
    both = tables[...]
    swapped = pltpu.roll(both, LANES // 2, 1)
    first = lax.broadcasted_iota(jnp.int32, both.shape, 1) < LANES // 2
    cosine, sine = jnp.where(first, both, swapped), jnp.where(first, -swapped, both)
    trig = (
        cosine,
        sine,
        jnp.concatenate([cosine, cosine], axis=0),
        jnp.concatenate([sine, sine], axis=0),
    )
    at_k = lax.broadcasted_iota(jnp.int32, (length, 2 * length), 0)
    at_q = lax.rem(lax.broadcasted_iota(jnp.int32, (length, 2 * length), 1), length)
    return trig, at_q >= at_k


def forward(inputs, cotangents, gains, tables, weights):
    micros, length, width = inputs.shape
    wq, wk, wv, wo, wg, wu, wd = weights
    groups = wk.shape[1] // HEAD_SIZE
    hidden = wg.shape[1]
    block = hidden // FORWARD_STEPS
    low, wide = jnp.bfloat16, jnp.float32

    def whole(array):
        return pl.BlockSpec(
            array.shape, lambda m, s: (0,) * array.ndim, pipeline_mode=pl.Buffered(1)
        )

    def by_micro(*shape):
        return pl.BlockSpec((1,) + shape, lambda m, s: (m,) + (0,) * len(shape))

    by_block = pl.BlockSpec((1, length, block), lambda m, s: (m, 0, jnp.maximum(s - 1, 0)))
    shapes = [
        ((length, width), low),
        ((length, width), low),
        ((length, width), low),
        ((groups, 2 * length, LANES), low),
        ((groups, length, LANES), low),
        ((groups, length, LANES), low),
        ((length, wq.shape[1]), low),
        ((length, width), low),
        ((length, width // 2), low),
        ((length, width // 2), low),
    ]
    out_shape = [jax.ShapeDtypeStruct((micros,) + shape, kind) for shape, kind in shapes]
    out_specs = [by_micro(*shape) for shape, _ in shapes]
    out_shape += [jax.ShapeDtypeStruct((micros, length, hidden), low)] * 3
    out_specs += [by_block] * 3
    first = jax.ShapeDtypeStruct((1, length, width), low)
    out_shape += [jax.ShapeDtypeStruct(inputs.shape, low), first]
    out_specs += [whole(inputs), whole(first)]
    return pl.pallas_call(
        functools.partial(forward_kernel, micros),
        grid=(micros, FORWARD_STEPS + 1),
        out_shape=out_shape,
        in_specs=[
            whole(inputs),
            pl.BlockSpec(memory_space=pl.ANY),
            whole(gains),
            whole(tables),
        ]
        + [pl.BlockSpec(memory_space=pl.ANY)] * 7,
        out_specs=out_specs,
        scratch_shapes=[
            pltpu.VMEM((micros, length, width), low),
            pltpu.VMEM((1, length, width), low),
            pltpu.VMEM((1, length, width), low),
            pltpu.VMEM((micros, length, width), low),
            pltpu.VMEM((micros, length, width), low),
            pltpu.VMEM((length, width), low),
            pltpu.VMEM((2, length, width), low),
            pltpu.VMEM((length, width), wide),
            pltpu.VMEM((length, width), wide),
            pltpu.VMEM((length, width), low),
            pltpu.SemaphoreType.DMA((2 * micros, SEND_PIECES)),
            pltpu.SemaphoreType.DMA((2 * micros, SEND_PIECES)),
            pltpu.SemaphoreType.DMA((micros,)),
            pltpu.SemaphoreType.DMA((micros,)),
            pltpu.SemaphoreType.DMA((micros,)),
            pltpu.SemaphoreType.DMA((micros,)),
            pltpu.SemaphoreType.DMA,
            pltpu.SemaphoreType.DMA,
            pltpu.SemaphoreType.DMA,
            pltpu.SemaphoreType.DMA,
            pltpu.SemaphoreType.DMA((1, 4)),
            pltpu.SemaphoreType.DMA((7, FORWARD_STEPS)),
        ]
        + [pltpu.VMEM(item.shape, low) for item in weights],
        compiler_params=pltpu.CompilerParams(
            collective_id=0, has_side_effects=True, vmem_limit_bytes=VMEM_LIMIT
        ),
    )(inputs, cotangents, gains, tables, wq, wk, wv, wo, wg, wu, wd)


def backward(cotangents, other, far_first, gains, tables, n1, record, weights):
    micros, length, width = cotangents.shape
    wq, wk, wv, wo, wg, wu, wd = weights
    groups = wk.shape[1] // HEAD_SIZE
    hidden = wg.shape[1]
    block = hidden // BACKWARD_STEPS
    last = BACKWARD_STEPS - 1
    low, wide = jnp.bfloat16, jnp.float32

    def whole(array):
        return pl.BlockSpec(
            array.shape, lambda m, s: (0,) * array.ndim, pipeline_mode=pl.Buffered(1)
        )

    def by_micro(*shape):
        return pl.BlockSpec((1,) + shape, lambda m, s: (m,) + (0,) * len(shape))

    by_block = pl.BlockSpec((1, length, block), lambda m, s: (m, 0, jnp.minimum(s, last)))
    heads, pairs = wq.shape[1], wk.shape[1]
    half = width // 2
    any_space = pl.BlockSpec(memory_space=pl.ANY)
    columns = [width, half, half, hidden, hidden, heads, pairs, pairs] + [width] * 4
    specs = [by_micro(length, width)] + [by_micro(length, half)] * 2 + [by_block] * 2
    specs += [by_micro(length, heads)] + [by_micro(length, pairs)] * 2 + [any_space] * 4
    out_shape = [jax.ShapeDtypeStruct((micros, length, size), low) for size in columns]
    out_shape.append(jax.ShapeDtypeStruct(gains.shape, wide))
    row = pltpu.SemaphoreType.DMA((micros,))
    swaps = pltpu.SemaphoreType.DMA((2 * micros, SEND_PIECES))
    return pl.pallas_call(
        functools.partial(backward_kernel, micros),
        grid=(micros, BACKWARD_STEPS + 1),
        out_shape=out_shape,
        in_specs=[
            whole(cotangents),
            whole(other),
            whole(far_first),
            whole(gains),
            whole(tables),
            any_space,
            any_space,
            by_micro(length, width),
            by_micro(groups, 2 * length, LANES),
            by_micro(groups, length, LANES),
            by_micro(groups, length, LANES),
            by_micro(length, width),
            by_block,
            by_block,
        ]
        + [any_space] * 7,
        out_specs=specs + [whole(gains)],
        scratch_shapes=[pltpu.VMEM(item.shape, low) for item in weights]
        + [
            pltpu.VMEM((micros, length, width), low),
            pltpu.VMEM((micros, length, width), low),
            pltpu.VMEM((2 * micros, length, width), low),
            pltpu.VMEM((micros, length, width), low),
            pltpu.VMEM(gains.shape, wide),
            pltpu.VMEM((length, width), low),
            pltpu.VMEM((length, width), low),
            pltpu.VMEM((length, width), low),
            pltpu.VMEM((2, length, width), low),
            pltpu.VMEM((length, width), wide),
            pltpu.VMEM((length, width), wide),
            swaps,
            swaps,
            row,
            row,
            row,
            row,
            pltpu.SemaphoreType.DMA((2 * micros, 4)),
            pltpu.SemaphoreType.DMA,
            pltpu.SemaphoreType.DMA,
            pltpu.SemaphoreType.DMA((7, BACKWARD_STEPS)),
            pltpu.SemaphoreType.DMA((4, micros)),
        ],
        compiler_params=pltpu.CompilerParams(
            collective_id=1, has_side_effects=True, vmem_limit_bytes=VMEM_LIMIT
        ),
    )(cotangents, other, far_first, gains, tables, n1, record[4], *record, wq, wk, wv, wo, wg, wu, wd)


BLOCKS = 8
PART = 3 * LANES
LAG = 3


class Halving:
    def __init__(self, bits, local, got, sems, outputs):
        self.bits, self.local, self.got, self.sems, self.outputs = bits, local, got, sems, outputs
        me = lax.axis_index("dp")
        self.own = [lax.rem(lax.div(me, 2**bit), 2) for bit in range(bits)]
        self.flip = [me + (1 - 2 * self.own[bit]) * 2**bit for bit in range(bits)]
        plain = list(range(bits))
        self.orders = [plain, [1, 0] + plain[2:] if bits > 1 else plain]

    def copy(self, block, half, level):
        order = self.orders[half]
        done, now = order[:level], order[level]
        spot = []
        for bit in reversed(range(self.bits)):
            if bit in done:
                spot.append(self.own[bit])
            else:
                spot.append(1 - self.own[bit] if bit == now else slice(None))
        return pltpu.make_async_remote_copy(
            src_ref=self.local.at[(block, half) + tuple(spot)],
            dst_ref=self.got[level].at[block, half],
            send_sem=self.sems.at[block, half, level, 0],
            recv_sem=self.sems.at[block, half, level, 1],
            device_id={"dp": self.flip[now]},
            device_id_type=MESH,
        )

    def begin(self, block):
        for half in range(2):
            self.copy(block, half, 0).start()

    def advance(self, block, level):
        for half in range(2):
            order = self.orders[half]
            self.copy(block, half, level).wait()
            done = order[: level + 1]
            left = [bit for bit in reversed(range(self.bits)) if bit not in done]
            rows = self.local.shape[-2]
            piece = 64 if rows % 64 == 0 else rows
            for combo in range(2 ** len(left)):
                fixed = {bit: (combo >> index) & 1 for index, bit in enumerate(left)}
                from_spot = (block, half) + tuple(fixed[bit] for bit in left)
                for bit in done:
                    fixed[bit] = self.own[bit]
                spot = (block, half) + tuple(fixed[bit] for bit in reversed(range(self.bits)))

                def add(index, _):
                    where = pl.ds(pl.multiple_of(index * piece, piece), piece)
                    a = self.local[spot + (where, slice(None))].astype(jnp.float32)
                    b = self.got[level][from_spot + (where, slice(None))].astype(jnp.float32)
                    if level == self.bits - 1:
                        self.outputs(block, half, where, (a + b).astype(jnp.bfloat16))
                    else:
                        self.local[spot + (where, slice(None))] = (a + b).astype(jnp.bfloat16)
                    return 0

                lax.fori_loop(0, rows // piece, add, 0)
            if level < self.bits - 1:
                self.copy(block, half, level + 1).start()


def gradient_kernel(
    bits,
    micros,
    late,
    n2_rows,
    g_rows,
    act_own,
    dgate_own,
    dup_own,
    n2_far,
    g_far,
    gains,
    tables,
    gain_in,
    wg,
    wu,
    wd,
    *refs,
):
    heads_in, late_in, refs = refs[:4], refs[4 : 4 + late], refs[4 + late :]
    outs, refs = refs[:8], refs[8:]
    late_refs, refs = refs[:late], refs[late:]
    heads_own, late_sems, refs = refs[0], refs[1], refs[2:]
    moves, at = list(zip(late_in, late_refs)), 0
    for source in heads_in:
        moves.append((source, heads_own.at[:, at : at + source.shape[1]]))
        at += source.shape[1]
    kept = [
        pltpu.make_async_copy(source, target, late_sems.at[index])
        for index, (source, target) in enumerate(moves)
    ]
    gradient_steps(
        bits,
        micros,
        kept,
        *late_refs[:2],
        heads_own,
        *late_refs[2:],
        n2_rows,
        g_rows,
        act_own,
        dgate_own,
        dup_own,
        n2_far,
        g_far,
        gains,
        tables,
        gain_in,
        wg,
        wu,
        wd,
        *outs,
        *refs,
    )


def gradient_steps(
    bits,
    micros,
    kept,
    n1_rows,
    low_rows,
    heads_own,
    n1_far,
    middle_far,
    wq,
    wk,
    wv,
    wo,
    n2_rows,
    g_rows,
    act_own,
    dgate_own,
    dup_own,
    n2_far,
    g_far,
    gains,
    tables,
    gain_in,
    wg,
    wu,
    wd,
    gate_out,
    up_out,
    down_out,
    q_out,
    k_out,
    v_out,
    o_out,
    gain_out,
    acc,
    send,
    swapped,
    heads_far,
    small,
    small_got,
    local,
    *rest,
):
    step = pl.program_id(0)
    got = rest[:bits]
    sems, small_sems, send_sem, recv_sem = rest[bits:]
    tensor = lax.axis_index("tensor")
    tokens, width = g_far.shape
    length = tokens // micros
    rows = local.shape[-2]
    lanes = half_lanes(width)
    count = local.shape[0]
    swap = Exchange(0, send, swapped, send_sem, recv_sem)

    def output(block, half, where, value):
        if isinstance(block, int):
            target, at = [
                [(q_out, 0), (q_out, PART)],
                [(k_out, 0), (v_out, 0)],
                [(o_out, 0), (o_out, PART)],
            ][block - BLOCKS][half]
            target[where, at : at + PART] = value
        else:
            at = pl.ds(pl.multiple_of(block * 2 * LANES + half * LANES, LANES), LANES)
            for index, target in enumerate((gate_out, up_out, down_out)):
                target[where, at] = value[:, index * LANES : (index + 1) * LANES]

    halving = Halving(bits, local, got, sems, output)

    def gain_copy(level):
        return pltpu.make_async_remote_copy(
            src_ref=small.at[level],
            dst_ref=small_got.at[level],
            send_sem=small_sems.at[level, 0],
            recv_sem=small_sems.at[level, 1],
            device_id={"dp": halving.flip[level]},
            device_id_type=MESH,
        )

    @pl.when(step == 0)
    def _():
        for copy in kept:
            copy.start()
        greet([{"tensor": 1 - tensor}] + [{"dp": halving.flip[bit]} for bit in range(bits)])
        small[0] = gain_in[:, lanes]
        gain_copy(0).start()

    def blocked(value):
        return value.astype(jnp.bfloat16).reshape((2,) * bits + (rows, value.shape[1]))

    @pl.when(step < BLOCKS)
    def _():
        n2, g = n2_far[...], g_far[...]
        gate, up = dot(n2, wg[...]), dot(n2, wu[...])
        d_act = dot(g, wd[...])
        sig = jax.nn.sigmoid(gate)
        act = (gate * sig * up).astype(jnp.bfloat16)
        d_gate = (d_act * up * sig * (1.0 + gate * (1.0 - sig))).astype(jnp.bfloat16)
        d_up = (d_act * gate * sig).astype(jnp.bfloat16)
        parts = (
            (n2_rows, dgate_own, n2_far, d_gate),
            (n2_rows, dup_own, n2_far, d_up),
            (g_rows, act_own, g_far, act),
        )
        for index, (left, right, left_far, right_far) in enumerate(parts):
            total = over_rows(left[...], right[...]) + over_rows(left_far[:, lanes], right_far)
            for half in range(2):
                spot = (step, half) + (slice(None),) * (bits + 1)
                local[spot + (slice(index * LANES, (index + 1) * LANES),)] = blocked(
                    total[:, half * LANES : (half + 1) * LANES]
                )
        halving.begin(step)

        product = times_t(d_gate, wg[...]) + times_t(d_up, wu[...])

        @pl.when(step == 0)
        def _():
            acc[...] = product

        @pl.when((step > 0) & (step < BLOCKS - 1))
        def _():
            acc[...] += product

        @pl.when(step == BLOCKS - 1)
        def _():
            for piece in range(SEND_PIECES):
                part = slice(piece * swap.width, (piece + 1) * swap.width)
                swap.start(piece, acc[:, part] + product[:, part])

    @pl.when(step == BLOCKS)
    def _():
        for copy in kept:
            copy.wait()
        swap.wait()
        for which in range(micros):
            part = slice(which * length, (which + 1) * length)
            d_normed = send[part, :].astype(jnp.float32) + swapped[0, part, :].astype(jnp.float32)
            mid = middle_far[part, :].astype(jnp.float32)
            scale = rsqrt_mean(mid)
            weighted = d_normed * gains[1:2, :]
            inner = jnp.mean(weighted * mid, axis=-1, keepdims=True)
            total = g_far[part, :].astype(jnp.float32) + scale * weighted - mid * (scale**3 * inner)
            send[part, :] = total.astype(jnp.bfloat16)

    @pl.when((step >= BLOCKS) & (step < BLOCKS + micros))
    def _():
        which = step - BLOCKS
        part = pl.ds(pl.multiple_of(which * length, length), length)
        n1 = n1_far[part, :]
        query, keys, values = dot(n1, wq[...]), dot(n1, wk[...]), dot(n1, wv[...])
        d_mixed = dot(send[part, :], wo[...]).astype(jnp.bfloat16).astype(jnp.float32)
        trig, causal = trig_and_mask(tables, length)
        cosine, sine, cosine2, sine2 = trig
        d_queries, d_keys, d_values, outs = [], [], [], []
        for group in range(wk.shape[1] // HEAD_SIZE):
            q = jnp.concatenate([spread(query, 2 * group), spread(query, 2 * group + 1)], axis=0)
            q = turned(q, cosine2, sine2).astype(jnp.bfloat16)
            k = turned(spread(keys, group), cosine, sine).astype(jnp.bfloat16)
            v = spread(values, group).astype(jnp.bfloat16)
            parts = attention_backward(d_mixed, group, q, k, v, trig, causal, True)
            d_queries += parts[0]
            d_keys.append(parts[1])
            d_values.append(parts[2])
            outs += parts[3]
        at = 0
        for item in (d_queries, d_keys, d_values, outs):
            item = gathered(item).astype(jnp.bfloat16)
            heads_far[part, at : at + item.shape[1]] = item
            at += item.shape[1]

    @pl.when(step >= LAG)
    def _():
        halving.advance(step - LAG, 0)

    @pl.when(step == BLOCKS + micros)
    def _():
        def head_gradients(block, left, left_far):
            for half in range(2):
                at = pl.ds(pl.multiple_of((2 * (block - BLOCKS) + half) * PART, PART), PART)
                local[block, half] = blocked(
                    over_rows(left[...], heads_own[:, at]) + over_rows(left_far, heads_far[:, at])
                )
            halving.begin(block)
            return 0

        lax.fori_loop(
            BLOCKS, count - 1, lambda block, _: head_gradients(block, n1_rows, n1_far[:, lanes]), 0
        )
        head_gradients(count - 1, low_rows, send[:, lanes])
        for level in range(bits):
            gain_copy(level).wait()
            summed = small[level] + small_got[level]
            if level < bits - 1:
                small[level + 1] = summed
                gain_copy(level + 1).start()
            else:
                gain_out[...] = summed
        for level in range(1, bits):

            def advanced(block, _):
                halving.advance(block, level)
                return 0

            lax.fori_loop(0, BLOCKS, advanced, 0)
        for level in range(bits):
            for block in range(BLOCKS, count):
                halving.advance(block, level)


def gradients(bits, own, far, gains, tables, gain, weights):
    wq, wk, wv, wo, wg, wu, wd = weights
    n1_rows, n2_rows, g_rows, low_rows, act, d_gate, d_up, d_q, d_k, d_v, mixed = own
    micros = n1_rows.shape[0]
    hidden, width = wg.shape[1], wg.shape[0]
    block = hidden // BLOCKS
    rows = width // 2 ** (bits + 1)
    low = jnp.bfloat16
    total = d_q.shape[2] + d_k.shape[2] + d_v.shape[2] + mixed.shape[2]
    count = BLOCKS + total // (2 * PART)

    def whole(array):
        return pl.BlockSpec(array.shape, lambda s: (0,) * array.ndim, pipeline_mode=pl.Buffered(1))

    def streamed(array):
        return pl.BlockSpec((array.shape[0], block), lambda s: (0, jnp.minimum(s, BLOCKS - 1)))

    def flat(values):
        return values.reshape(-1, values.shape[-1])

    n1_far, n2_far, g_far, middle_far = (flat(item) for item in far)
    args = [(flat(item), whole) for item in (n2_rows, g_rows)]
    args += [(flat(item), streamed) for item in (act, d_gate, d_up)]
    args += [(item, whole) for item in (n2_far, g_far, gains, tables, gain)]
    args += [(item, streamed) for item in (wg, wu, wd)]
    heads = [flat(item) for item in (d_q, d_k, d_v, mixed)]
    late = [flat(item) for item in (n1_rows, low_rows)] + [n1_far, middle_far, wq, wk, wv, wo]
    sizes = [hidden] * 3 + [d_q.shape[2], d_k.shape[2], d_v.shape[2], mixed.shape[2]]
    out_shape = [jax.ShapeDtypeStruct((rows, size), low) for size in sizes]
    out_shape.append(jax.ShapeDtypeStruct((2, width // 2), jnp.float32))
    tokens = args[0][0].shape[0]
    scratch = [pltpu.VMEM(item.shape, low) for item in late]
    scratch += [
        pltpu.VMEM((tokens, total), low),
        pltpu.SemaphoreType.DMA((len(late) + len(heads),)),
        pltpu.VMEM((tokens, width), jnp.float32),
        pltpu.VMEM((tokens, width), low),
        pltpu.VMEM((1, tokens, width), low),
        pltpu.VMEM((tokens, total), low),
        pltpu.VMEM((bits, 2, width // 2), jnp.float32),
        pltpu.VMEM((bits, 2, width // 2), jnp.float32),
        pltpu.VMEM((count, 2) + (2,) * bits + (rows, PART), low),
    ]
    for level in range(bits):
        scratch.append(pltpu.VMEM((count, 2) + (2,) * (bits - 1 - level) + (rows, PART), low))
    scratch += [
        pltpu.SemaphoreType.DMA((count, 2, bits, 2)),
        pltpu.SemaphoreType.DMA((bits, 2)),
        pltpu.SemaphoreType.DMA((1, SEND_PIECES)),
        pltpu.SemaphoreType.DMA((1, SEND_PIECES)),
    ]
    return pl.pallas_call(
        functools.partial(gradient_kernel, bits, micros, len(late)),
        grid=(BLOCKS + micros + 1,),
        out_shape=out_shape,
        in_specs=[spec(array) for array, spec in args]
        + [pl.BlockSpec(memory_space=pl.ANY)] * (len(heads) + len(late)),
        out_specs=[whole(shape) for shape in out_shape],
        scratch_shapes=scratch,
        compiler_params=pltpu.CompilerParams(
            collective_id=2, has_side_effects=True, vmem_limit_bytes=VMEM_LIMIT
        ),
    )(*(array for array, _ in args), *heads, *late)


def finished(shards, plain):
    items = list(shards) + list(plain)
    kinds = [jnp.float32] * len(shards) + [jnp.bfloat16] * len(plain)
    steps = 4

    def kernel(*refs):
        for source, target in zip(refs[: len(items)], refs[len(items) :]):
            target[...] = source[...].astype(target.dtype)

    def spec(item):
        rows = item.shape[0]
        block = rows // steps if rows % (16 * steps) == 0 else 16
        return pl.BlockSpec(
            (block, item.shape[1]), lambda s: (jnp.minimum(s, rows // block - 1), 0)
        )

    return pl.pallas_call(
        kernel,
        grid=(steps,),
        out_shape=[jax.ShapeDtypeStruct(item.shape, kind) for item, kind in zip(items, kinds)],
        in_specs=[spec(item) for item in items],
        out_specs=[spec(item) for item in items],
    )(*items)


def body(
    inputs,
    cotangents,
    norm_scales,
    w_query,
    key_weight,
    value_weight,
    w_out,
    w_gate,
    w_up,
    down_weight,
):
    weights = (
        w_query[0],
        key_weight[0],
        value_weight[0],
        w_out[0],
        w_gate[0],
        w_up[0],
        down_weight[0],
    )
    _, _, length, width = inputs.shape
    gains = norm_scales[0].T
    tables = jnp.asarray(rope_tables(length))
    cots = cotangents[:, 0]
    (
        result,
        hidden,
        n1,
        q,
        k,
        v,
        mixed,
        middle,
        n1_rows,
        n2_rows,
        gate,
        up,
        act,
        other,
        far_first,
    ) = forward(inputs[:, 0], cots, gains, tables, weights)
    grad, g_rows, low_rows, d_gate, d_up, d_q, d_k, d_v, n1_far, n2_far, g_far, middle_far, gain = backward(
        cots, other, far_first, gains, tables, n1, (hidden, q, k, v, middle, gate, up), weights
    )
    peers = lax.axis_size("dp")
    *shards, gain = gradients(
        peers.bit_length() - 2,
        (n1_rows, n2_rows, g_rows, low_rows, act, d_gate, d_up, d_q, d_k, d_v, mixed),
        (n1_far, n2_far, g_far, middle_far),
        gains,
        tables,
        gain,
        weights,
    )
    (
        grad_gate,
        grad_up,
        grad_down,
        grad_query,
        grad_key,
        grad_value,
        grad_proj,
        result,
        grad,
    ) = (item[None] for item in finished(shards, [result.reshape(-1, width), grad.reshape(-1, width)]))
    rows = width // peers
    at = lax.rem(lax.axis_index("dp"), peers // 2) * rows
    grad_scales = lax.dynamic_slice_in_dim(gain, at, rows, 1).T[None]
    return (
        result.reshape(1, -1, 1, length, width),
        grad.reshape(1, -1, 1, length, width),
        grad_scales,
        grad_query,
        grad_key,
        grad_value,
        grad_proj,
        grad_gate,
        grad_up,
        grad_down,
    )


def solution(mesh):
    placed = (
        P(None, "dp", None, None),
        P(None, "dp", None, None),
        P("pipe", None, None),
        P("pipe", None, "tensor"),
        P("pipe", None, "tensor"),
        P("pipe", None, "tensor"),
        P("pipe", None, "tensor"),
        P("pipe", None, "tensor"),
        P("pipe", None, "tensor"),
        P("pipe", None, "tensor"),
    )
    return jax.shard_map(
        body,
        mesh=mesh,
        in_specs=placed,
        out_specs=(
            P("pipe", None, "dp", None, None),
            P("pipe", None, "dp", None, None),
            P("pipe", "dp", None),
            P("pipe", "dp", "tensor"),
            P("pipe", "dp", "tensor"),
            P("pipe", "dp", "tensor"),
            P("pipe", "dp", "tensor"),
            P("pipe", "dp", "tensor"),
            P("pipe", "dp", "tensor"),
            P("pipe", "dp", "tensor"),
        ),
        check_vma=False,
    )
```

```python
import functools

import jax
import jax.numpy as jnp
import numpy as np
from jax import lax
from jax.experimental import pallas as pl
from jax.experimental.pallas import tpu as pltpu
from jax.sharding import PartitionSpec as P

HEAD_SIZE = 96
HALF = HEAD_SIZE // 2
LANES = 128
FORWARD_STEPS = 2
BACKWARD_STEPS = 2
SEND_PIECES = 3

EPS = 1e-05
THETA = 100000.0
MESH = pl.DeviceIdType.MESH
VMEM_LIMIT = 67043328
SCALE = HEAD_SIZE ** (-0.5)


def rope_tables(length):
    freqs = (THETA ** (-(np.arange(HALF, dtype=np.float64) * 2.0 / HEAD_SIZE))).astype(np.float32)
    angles = np.arange(length, dtype=np.float32)[:, None] * freqs[None, :]
    cosine, sine = np.cos(angles), np.sin(angles)
    room = np.zeros((length, LANES // 2 - HALF), np.float32)
    return np.concatenate([cosine, room, sine, room], axis=1).astype(np.float32)


def dot(left, right):
    return lax.dot_general(
        left, right, (((1,), (0,)), ((), ())), preferred_element_type=jnp.float32
    )


def times_t(left, right):
    return lax.dot_general(
        left, right, (((1,), (1,)), ((), ())), preferred_element_type=jnp.float32
    )


def over_rows(left, right):
    return lax.dot_general(
        left, right, (((0,), (0,)), ((), ())), preferred_element_type=jnp.float32
    )


def spread(values, head):
    room = jnp.zeros((values.shape[0], LANES // 2 - HALF), values.dtype)
    at = head * HEAD_SIZE
    return jnp.concatenate(
        [values[:, at : at + HALF], room, values[:, at + HALF : at + HEAD_SIZE], room], axis=1
    )


def gathered(heads):
    parts = []
    for head in heads:
        parts += [head[:, :HALF], head[:, LANES // 2 : LANES // 2 + HALF]]
    return jnp.concatenate(parts, axis=1)


def turned(values, cosine, sine):
    return values * cosine + pltpu.roll(values, LANES // 2, 1) * sine


def turned_back(values, cosine, sine):
    return values * cosine - pltpu.roll(values, LANES // 2, 1) * sine


def rsqrt_mean(values):
    return lax.rsqrt(jnp.mean(values * values, axis=-1, keepdims=True) + EPS)


def normed(source, gain, target):
    rows = 64

    def part(index, _):
        where = pl.ds(pl.multiple_of(index * rows, rows), rows)
        wide = source[where, :].astype(jnp.float32)
        target[where, :] = (wide * rsqrt_mean(wide) * gain).astype(jnp.bfloat16)
        return 0

    lax.fori_loop(0, source.shape[0] // rows, part, 0)


class Exchange:
    def __init__(self, number, send, got, send_sem, recv_sem):
        self.number, self.send, self.got = number, send, got
        self.send_sem, self.recv_sem = send_sem, recv_sem
        self.width = send.shape[1] // SEND_PIECES
        self.slot = lax.rem(number, got.shape[0])

    def copy(self, piece):
        columns = pl.ds(piece * self.width, self.width)
        return pltpu.make_async_remote_copy(
            src_ref=self.send.at[:, columns],
            dst_ref=self.got.at[self.slot, :, columns],
            send_sem=self.send_sem.at[self.number, piece],
            recv_sem=self.recv_sem.at[self.number, piece],
            device_id={"tensor": 1 - lax.axis_index("tensor")},
            device_id_type=MESH,
        )

    def start(self, piece, partial_value):
        columns = pl.ds(piece * self.width, self.width)
        self.send[:, columns] = partial_value.astype(jnp.bfloat16)
        self.copy(piece).start()

    def wait(self):
        for piece in range(SEND_PIECES):
            self.copy(piece).wait()

    def total(self):
        return self.send[...].astype(jnp.float32) + self.got[self.slot].astype(jnp.float32)


def half_copy(source, target, rows, send_sem, recv_sem, device):
    return pltpu.make_async_remote_copy(
        src_ref=source.at[rows],
        dst_ref=target.at[rows],
        send_sem=send_sem,
        recv_sem=recv_sem,
        device_id=device,
        device_id_type=MESH,
    )


def passed_on(xin, micro, sems, stage_from, meanwhile=None):
    tensor = lax.axis_index("tensor")
    rows = xin.shape[1] // 2
    send_sem, recv_sem, pair_send, pair_recv = sems
    slot = xin.at[micro]
    mine = pl.ds(pl.multiple_of(tensor * rows, rows), rows)
    theirs = pl.ds(pl.multiple_of((1 - tensor) * rows, rows), rows)
    half_copy(
        slot, slot, mine, send_sem.at[micro], recv_sem.at[micro], {"pipe": stage_from}
    ).wait_recv()
    copy = half_copy(
        slot, slot, mine, pair_send.at[micro], pair_recv.at[micro], {"tensor": 1 - tensor}
    )
    copy.start()
    if meanwhile:
        meanwhile()
    half_copy(
        slot, slot, theirs, pair_send.at[micro], pair_recv.at[micro], {"tensor": 1 - tensor}
    ).wait_recv()
    copy.wait_send()


def sent_on(source, xin, micro, sems, stage_to):
    tensor = lax.axis_index("tensor")
    rows = xin.shape[1] // 2
    mine = pl.ds(pl.multiple_of(tensor * rows, rows), rows)
    return half_copy(
        source.at[micro], xin.at[micro], mine, sems[0].at[micro], sems[1].at[micro], {"pipe": stage_to}
    )


class Resident:
    def __init__(self, sources, targets, sems, steps):
        attention, hidden = range(4), range(4, len(sources))
        block = targets[4].shape[1] // steps
        self.copies = {}
        for index in attention:
            self.copies[index, 0] = pltpu.make_async_copy(
                sources[index], targets[index], sems.at[index, 0]
            )
        for index in hidden:
            for step in range(steps):
                columns = pl.ds(step * block, block)
                self.copies[index, step] = pltpu.make_async_copy(
                    sources[index].at[:, columns], targets[index].at[:, columns], sems.at[index, step]
                )
        self.parts = {"attention": [(index, 0) for index in attention]}
        for step in range(steps):
            self.parts[step] = [(index, step) for index in reversed(hidden)]
            self.parts["down", step] = self.parts[step][:1]
            self.parts["others", step] = self.parts[step][1:]

    def start(self, *parts):
        for part in parts:
            for key in self.parts[part]:
                self.copies[key].start()

    def wait(self, part):
        for key in self.parts[part]:
            self.copies[key].wait()


def half_lanes(width):
    top = lax.div(lax.axis_index("dp"), lax.axis_size("dp") // 2)
    return pl.ds(pl.multiple_of(top * (width // 2), LANES), width // 2)


def greet(devices):
    barrier = pltpu.get_barrier_semaphore()
    for device in devices:
        pl.semaphore_signal(barrier, inc=1, device_id=device, device_id_type=MESH)
    pl.semaphore_wait(barrier, len(devices))


class FarCopies:
    def __init__(self, sources, buffers, sems, partner):
        self.sources, self.buffers, self.sems, self.partner = sources, buffers, sems, partner
        tensor = lax.axis_index("tensor")
        self.pair = {"tensor": 1 - tensor}
        rows = buffers.shape[1] // 2
        self.mine = pl.ds(pl.multiple_of(tensor * rows, rows), rows)
        self.theirs = pl.ds(pl.multiple_of((1 - tensor) * rows, rows), rows)

    def far(self, which, source=None):
        source = self.sources.at[which] if source is None else source
        sems = self.sems.at[which, 0], self.sems.at[which, 1]
        return half_copy(source, self.buffers.at[which], self.mine, *sems, {"dp": self.partner})

    def near(self, which, rows):
        slot = self.buffers.at[which]
        sems = self.sems.at[which, 2], self.sems.at[which, 3]
        return half_copy(slot, slot, rows, *sems, self.pair)

    def start(self, which, source=None):
        self.far(which, source).start()

    def relay(self, which):
        self.far(which, self.buffers.at[which]).wait_recv()
        self.near(which, self.mine).start()

    def settle(self, which):
        self.far(which, self.buffers.at[which]).wait_send()
        self.near(which, self.theirs).wait_recv()
        self.near(which, self.mine).wait_send()

    def receive(self, which):
        self.relay(which)
        self.settle(which)


def forward_kernel(
    micros,
    inp,
    cot,
    gains,
    tables,
    *refs,
):
    weights_in, refs = refs[:7], refs[7:]
    forward_steps(micros, inp, cot, gains, tables, weights_in, *refs)


def forward_steps(
    micros,
    inp,
    cot,
    gains,
    tables,
    weights_in,
    result_out,
    hidden_out,
    n1_out,
    q_out,
    k_out,
    v_out,
    o_out,
    middle_out,
    n1_rows,
    n2_rows,
    gate_out,
    up_out,
    act_out,
    other_out,
    far_out,
    other,
    first_buf,
    far_buf,
    xin,
    res,
    send,
    got,
    middle,
    acc,
    n2_buf,
    send_sem,
    recv_sem,
    x_send,
    x_recv,
    xp_send,
    xp_recv,
    far_send,
    far_recv,
    near_send,
    near_recv,
    far_sems,
    weight_sems,
    wq,
    wk,
    wv,
    wo,
    wg,
    wu,
    wd,
):
    micro, step = pl.program_id(0), pl.program_id(1)
    pipe, tensor, data = lax.axis_index("pipe"), lax.axis_index("tensor"), lax.axis_index("dp")
    peers = lax.axis_size("dp")
    partner = lax.rem(data + peers // 2, peers)
    sems = (x_send, x_recv, xp_send, xp_recv)
    length = inp.shape[1]
    lanes = half_lanes(inp.shape[2])

    def far_copy(source):
        return pltpu.make_async_remote_copy(
            src_ref=source.at[tensor],
            dst_ref=other.at[tensor],
            send_sem=far_send,
            recv_sem=far_recv,
            device_id={"dp": partner},
            device_id_type=MESH,
        )

    def near_copy(which):
        return pltpu.make_async_remote_copy(
            src_ref=other.at[which],
            dst_ref=other.at[which],
            send_sem=near_send,
            recv_sem=near_recv,
            device_id={"tensor": 1 - tensor},
            device_id_type=MESH,
        )

    far = FarCopies(first_buf, far_buf, far_sems, partner)

    resident = Resident(weights_in, (wq, wk, wv, wo, wg, wu, wd), weight_sems, FORWARD_STEPS)

    @pl.when((micro == 0) & (step == 0))
    def _():
        resident.start("attention", *range(FORWARD_STEPS))
        greet([{"tensor": 1 - tensor}, {"pipe": 1 - pipe}, {"dp": partner}])

        @pl.when(pipe == 0)
        def _():
            far_copy(inp).start()

        @pl.when(pipe == 1)
        def _():
            far_copy(cot).start()

    @pl.when((micro == 0) & (step == 0))
    def _():
        resident.wait("attention")

    for number in range(FORWARD_STEPS):

        @pl.when((micro == 0) & (step == number + 1))
        def _():
            resident.wait(number)

    @pl.when(step == 0)
    def _():
        @pl.when(pipe == 0)
        def _():
            hidden_out[0] = inp[micro]

        @pl.when(pipe == 1)
        def _():
            passed_on(xin, micro, sems, 0)
            hidden_out[0] = xin[micro]

        wide = hidden_out[0].astype(jnp.float32)
        n1 = (wide * rsqrt_mean(wide) * gains[0:1, :]).astype(jnp.bfloat16)
        n1_out[0] = n1
        n1_rows[0] = n1_out[0, :, lanes]

        @pl.when((pipe == 1) & (micro == 0))
        def _():
            first_buf[0] = n1
            far.start(0)

        query = dot(n1, wq[...])
        keys = dot(n1, wk[...])
        values = dot(n1, wv[...])
        trig, causal = trig_and_mask(tables, length)
        cosine, sine, cosine2, sine2 = trig
        groups = k_out.shape[1]
        outs = []
        for group in range(groups):
            q = jnp.concatenate([spread(query, 2 * group), spread(query, 2 * group + 1)], axis=0)
            q = turned(q, cosine2, sine2).astype(jnp.bfloat16)
            k = turned(spread(keys, group), cosine, sine).astype(jnp.bfloat16)
            v = spread(values, group).astype(jnp.bfloat16)
            q_out[0, group] = q
            k_out[0, group] = k
            v_out[0, group] = v
            probs = attention_weights(q, k, causal).astype(jnp.bfloat16)
            mixed = over_rows(probs, v)
            outs += [mixed[:length], mixed[length:]]
        mixed = gathered(outs).astype(jnp.bfloat16)
        o_out[0] = mixed
        swap = Exchange(2 * micro, send, got, send_sem, recv_sem)
        for piece in range(SEND_PIECES):
            swap.start(piece, times_t(mixed, wo[piece * swap.width : (piece + 1) * swap.width, :]))
        swap.wait()
        both = hidden_out[0].astype(jnp.float32) + swap.total()
        middle[...] = both
        middle_low = both.astype(jnp.bfloat16)
        middle_out[0] = middle_low
        n2 = (both * rsqrt_mean(both) * gains[1:2, :]).astype(jnp.bfloat16)
        n2_buf[...] = n2
        n2_rows[0] = n2_buf[:, lanes]

        @pl.when((pipe == 0) & (micro == 0))
        def _():
            first_buf[0] = middle_low
            far.start(0)


    @pl.when(step > 0)
    def _():
        n2 = n2_buf[...]
        block = wg.shape[1] // FORWARD_STEPS
        columns = pl.ds(pl.multiple_of((step - 1) * block, block), block)
        gate = dot(n2, wg[:, columns])
        up = dot(n2, wu[:, columns])
        act = (gate * jax.nn.sigmoid(gate) * up).astype(jnp.bfloat16)
        gate_out[0] = gate.astype(jnp.bfloat16)
        up_out[0] = up.astype(jnp.bfloat16)
        act_out[0] = act
        product = times_t(act, wd[:, columns])

        @pl.when(step == 1)
        def _():
            acc[...] = product

        @pl.when((step > 1) & (step < FORWARD_STEPS))
        def _():
            acc[...] += product

        @pl.when(step == FORWARD_STEPS)
        def _():
            swap = Exchange(2 * micro + 1, send, got, send_sem, recv_sem)
            for piece in range(SEND_PIECES):
                part = slice(piece * swap.width, (piece + 1) * swap.width)
                swap.start(piece, acc[:, part] + product[:, part])
            swap.wait()
            result = (middle[...] + swap.total()).astype(jnp.bfloat16)
            result_out[0] = result

            @pl.when(pipe == 0)
            def _():
                res[micro] = result
                sent_on(res, xin, micro, sems, 1).start()


    @pl.when((micro == micros - 1) & (step == FORWARD_STEPS))
    def _():
        far_copy(inp).wait()
        near_copy(tensor).start()
        near_copy(1 - tensor).wait_recv()
        near_copy(tensor).wait_send()
        other_out[...] = other[...]
        far.receive(0)
        far_out[...] = far_buf[...]

    @pl.when((pipe == 0) & (micro == micros - 1) & (step == FORWARD_STEPS))
    def _():
        for which in range(micros):
            sent_on(res, xin, which, sems, 1).wait_send()


def attention_weights(q, k, causal):
    weights = jnp.where(causal, jnp.exp(times_t(k, q) * SCALE), 0.0)
    return weights * (1.0 / jnp.sum(weights, axis=0, keepdims=True))


def attention_backward(d_mixed, group, q, k, v, trig, probs, with_output):
    cosine, sine, cosine2, sine2 = trig
    d_head = jnp.concatenate(
        [spread(d_mixed, 2 * group), spread(d_mixed, 2 * group + 1)], axis=0
    ).astype(jnp.bfloat16)
    rounded = probs.astype(jnp.bfloat16)
    probs = probs.astype(jnp.float32)
    moved = probs * times_t(v, d_head)
    delta = jnp.sum(moved, axis=0, keepdims=True)
    d_scores = ((moved - probs * delta) * SCALE).astype(jnp.bfloat16)
    d_value = dot(rounded, d_head)
    d_key = turned_back(dot(d_scores, q), cosine, sine)
    d_query = turned_back(over_rows(d_scores, k), cosine2, sine2)
    length = k.shape[0]
    mixed = over_rows(rounded, v) if with_output else d_query
    return (
        [d_query[:length], d_query[length:]],
        d_key,
        d_value,
        [mixed[:length], mixed[length:]],
    )


def backward_kernel(
    micros,
    cot,
    other,
    far_first,
    gains,
    tables,
    n1_own,
    middle_own,
    hidden,
    q_in,
    k_in,
    v_in,
    middle,
    gate_in,
    up_in,
    *refs,
):
    weights_in, refs = refs[:7], refs[7:]
    backward_steps(
        micros,
        cot,
        other,
        far_first,
        gains,
        tables,
        n1_own,
        middle_own,
        hidden,
        q_in,
        k_in,
        v_in,
        middle,
        gate_in,
        up_in,
        weights_in,
        *refs,
    )


def backward_steps(
    micros,
    cot,
    other,
    far_first,
    gains,
    tables,
    n1_own,
    middle_own,
    hidden,
    q_in,
    k_in,
    v_in,
    middle,
    gate_in,
    up_in,
    weights_in,
    grad_out,
    g_rows,
    low_rows,
    dgate_out,
    dup_out,
    dq_out,
    dk_out,
    dv_out,
    n1_far,
    n2_far,
    g_far,
    middle_far,
    gain_out,
    wq,
    wk,
    wv,
    wo,
    wg,
    wu,
    wd,
    xin,
    res,
    far_buf,
    n2_buf,
    far_gain,
    g_buf,
    low_buf,
    probs_buf,
    send,
    got,
    d_middle,
    acc,
    send_sem,
    recv_sem,
    x_send,
    x_recv,
    xp_send,
    xp_recv,
    far_sems,
    gain_send,
    gain_recv,
    in_sems,
    out_sems,
    first_sem,
):
    micro, step = pl.program_id(0), pl.program_id(1)
    pipe, tensor, data = lax.axis_index("pipe"), lax.axis_index("tensor"), lax.axis_index("dp")
    peers = lax.axis_size("dp")
    partner = lax.rem(data + peers // 2, peers)
    sems = (x_send, x_recv, xp_send, xp_recv)
    length = hidden.shape[1]
    lanes = half_lanes(hidden.shape[2])
    last = micros - 1
    far = FarCopies(xin, far_buf, far_sems, partner)

    def gain_copy():
        return pltpu.make_async_remote_copy(
            src_ref=gain_out,
            dst_ref=far_gain,
            send_sem=gain_send,
            recv_sem=gain_recv,
            device_id={"dp": partner},
            device_id_type=MESH,
        )

    resident = Resident(weights_in, (wq, wk, wv, wo, wg, wu, wd), in_sems, BACKWARD_STEPS)

    first_slot = micros * (1 - pipe)
    first_copy = pltpu.make_async_copy(far_first.at[0], far_buf.at[first_slot], first_sem)

    def write(kind, which, source):
        target = (n1_far, n2_far, g_far, middle_far)[kind]
        return pltpu.make_async_copy(source, target.at[which], out_sems.at[kind, which])

    def far_middle(which, source):
        write(3, which, source).start()
        normed(source, gains[1:2, :], n2_buf.at[which])
        write(1, which, n2_buf.at[which]).start()

    @pl.when((micro == 0) & (step == 0))
    def _():
        resident.start(*range(BACKWARD_STEPS), "attention")
        first_copy.start()
        greet([{"tensor": 1 - tensor}, {"pipe": 1 - pipe}, {"dp": partner}])
        gain_out[...] = jnp.zeros_like(gain_out)

        @pl.when(pipe == 1)
        def _():
            for which in range(micros):
                if which:
                    far.start(which, n1_own.at[which])
                far.start(micros + which, middle_own.at[which])
            for which in range(micros):
                write(2, which, other.at[which]).start()

        @pl.when(pipe == 0)
        def _():
            for which in range(1, micros):
                far.start(micros + which, middle_own.at[which])
            for which in range(micros):
                normed(other.at[which], gains[0:1, :], res.at[which])
                write(0, which, res.at[which]).start()
            first_copy.wait()
            far_middle(0, far_buf.at[micros])

    @pl.when(step == 0)
    def _():
        @pl.when(pipe == 1)
        def _():
            g_buf[...] = cot[micro]

        @pl.when((pipe == 0) & (micro == last))
        def _():
            for which in range(1, micros):
                far.settle(micros + which)
                far_middle(which, far_buf.at[micros + which])

        @pl.when(pipe == 0)
        def _():
            passed_on(xin, micro, sems, 1, lambda: far.start(micro))
            g_buf[...] = xin[micro]

        g_rows[0] = g_buf[:, lanes]

    @pl.when((micro == 0) & (step == BACKWARD_STEPS))
    def _():
        resident.wait("attention")

    def arrived(name):
        for number in range(BACKWARD_STEPS):

            @pl.when((micro == 0) & (step == number))
            def _():
                resident.wait((name, number))

    @pl.when((pipe == 1) & (micro == 0) & (step == 1))
    def _():
        first_copy.wait()
        write(0, 0, far_buf.at[0]).start()

    @pl.when((pipe == 0) & (micro == 0) & (step == 1))
    def _():
        for which in range(1, micros):
            far.relay(micros + which)

    @pl.when((pipe == 0) & (micro == last) & (step == BACKWARD_STEPS))
    def _():
        for which in range(last):
            far.relay(which)

    @pl.when(step < BACKWARD_STEPS)
    def _():
        arrived("down")
        gate, up = gate_in[0].astype(jnp.float32), up_in[0].astype(jnp.float32)
        block = wg.shape[1] // BACKWARD_STEPS
        columns = pl.ds(pl.multiple_of(step * block, block), block)
        d_act = dot(g_buf[...], wd[:, columns])
        sig = jax.nn.sigmoid(gate)
        d_gate = (d_act * up * sig * (1.0 + gate * (1.0 - sig))).astype(jnp.bfloat16)
        d_up = (d_act * gate * sig).astype(jnp.bfloat16)
        dgate_out[0] = d_gate
        dup_out[0] = d_up

        arrived("others")
        product = times_t(d_gate, wg[:, columns]) + times_t(d_up, wu[:, columns])

        @pl.when(step == 0)
        def _():
            acc[...] = product

        @pl.when((step > 0) & (step < BACKWARD_STEPS - 1))
        def _():
            acc[...] += product

        @pl.when(step == BACKWARD_STEPS - 1)
        def _():
            swap = Exchange(2 * micro, send, got, send_sem, recv_sem)
            for piece in range(SEND_PIECES):
                part = slice(piece * swap.width, (piece + 1) * swap.width)
                swap.start(piece, acc[:, part] + product[:, part])
            causal = trig_and_mask(tables, length)[1]
            for group in range(k_in.shape[1]):
                probs = attention_weights(q_in[0, group], k_in[0, group], causal)
                probs_buf[group] = probs.astype(jnp.bfloat16)
            swap.wait()
            d_normed = swap.total()
            mid = middle[0].astype(jnp.float32)
            scale = rsqrt_mean(mid)
            gain_out[1:2, :] += jnp.sum(d_normed * mid * scale, axis=0, keepdims=True)
            weighted = d_normed * gains[1:2, :]
            inner = jnp.mean(weighted * mid, axis=-1, keepdims=True)
            total = g_buf[...].astype(jnp.float32) + scale * weighted - mid * (scale**3 * inner)
            d_middle[...] = total
            low_buf[...] = total.astype(jnp.bfloat16)
            low_rows[0] = low_buf[:, lanes]

    @pl.when(step == BACKWARD_STEPS)
    def _():
        d_mixed = dot(low_buf[...], wo[...]).astype(jnp.bfloat16).astype(jnp.float32)
        trig, causal = trig_and_mask(tables, length)
        d_queries, d_keys, d_values = [], [], []
        for group in range(k_in.shape[1]):
            parts = attention_backward(
                d_mixed,
                group,
                q_in[0, group],
                k_in[0, group],
                v_in[0, group],
                trig,
                probs_buf[group],
                False,
            )
            d_queries += parts[0]
            d_keys.append(parts[1])
            d_values.append(parts[2])
        d_query = gathered(d_queries).astype(jnp.bfloat16)
        d_key = gathered(d_keys).astype(jnp.bfloat16)
        d_value = gathered(d_values).astype(jnp.bfloat16)
        dq_out[0] = d_query
        dk_out[0] = d_key
        dv_out[0] = d_value
        swap = Exchange(2 * micro + 1, send, got, send_sem, recv_sem)
        for piece in range(SEND_PIECES):
            part = slice(piece * swap.width, (piece + 1) * swap.width)
            swap.start(
                piece,
                times_t(d_query, wq[part, :]) + times_t(d_key, wk[part, :]) + times_t(d_value, wv[part, :]),
            )
        swap.wait()
        d_first = swap.total()
        wide = hidden[0].astype(jnp.float32)
        scale = rsqrt_mean(wide)
        gain_out[0:1, :] += jnp.sum(d_first * wide * scale, axis=0, keepdims=True)
        weighted = d_first * gains[0:1, :]
        inner = jnp.mean(weighted * wide, axis=-1, keepdims=True)
        d_hidden = (d_middle[...] + scale * weighted - wide * (scale**3 * inner)).astype(jnp.bfloat16)
        grad_out[0] = d_hidden

        @pl.when(pipe == 1)
        def _():
            res[micro] = d_hidden
            sent_on(res, xin, micro, sems, 0).start()

        @pl.when(micro == last)
        def _():
            gain_copy().start()

            @pl.when(pipe == 1)
            def _():
                for which in range(micros):
                    far.receive(micros + which)
                    far_middle(which, far_buf.at[micros + which])
                for which in range(1, micros):
                    far.receive(which)
                    write(0, which, far_buf.at[which]).start()

            @pl.when(pipe == 0)
            def _():
                for which in range(last):
                    far.settle(which)
                    write(2, which, far_buf.at[which]).start()
                far.receive(last)
                write(2, last, far_buf.at[last]).start()

            for kind in range(4):
                for which in range(micros):
                    write(kind, which, far_buf.at[which]).wait()
            gain_copy().wait()
            gain_out[...] += far_gain[...]

            @pl.when(pipe == 1)
            def _():
                for which in range(micros):
                    sent_on(res, xin, which, sems, 0).wait_send()


def trig_and_mask(tables, length):
    both = tables[...]
    swapped = pltpu.roll(both, LANES // 2, 1)
    first = lax.broadcasted_iota(jnp.int32, both.shape, 1) < LANES // 2
    cosine, sine = jnp.where(first, both, swapped), jnp.where(first, -swapped, both)
    trig = (
        cosine,
        sine,
        jnp.concatenate([cosine, cosine], axis=0),
        jnp.concatenate([sine, sine], axis=0),
    )
    at_k = lax.broadcasted_iota(jnp.int32, (length, 2 * length), 0)
    at_q = lax.rem(lax.broadcasted_iota(jnp.int32, (length, 2 * length), 1), length)
    return trig, at_q >= at_k


def forward(inputs, cotangents, gains, tables, weights):
    micros, length, width = inputs.shape
    wq, wk, wv, wo, wg, wu, wd = weights
    groups = wk.shape[1] // HEAD_SIZE
    hidden = wg.shape[1]
    block = hidden // FORWARD_STEPS
    low, wide = jnp.bfloat16, jnp.float32

    def whole(array):
        return pl.BlockSpec(
            array.shape, lambda m, s: (0,) * array.ndim, pipeline_mode=pl.Buffered(1)
        )

    def by_micro(*shape):
        return pl.BlockSpec((1,) + shape, lambda m, s: (m,) + (0,) * len(shape))

    by_block = pl.BlockSpec((1, length, block), lambda m, s: (m, 0, jnp.maximum(s - 1, 0)))
    shapes = [
        ((length, width), low),
        ((length, width), low),
        ((length, width), low),
        ((groups, 2 * length, LANES), low),
        ((groups, length, LANES), low),
        ((groups, length, LANES), low),
        ((length, wq.shape[1]), low),
        ((length, width), low),
        ((length, width // 2), low),
        ((length, width // 2), low),
    ]
    out_shape = [jax.ShapeDtypeStruct((micros,) + shape, kind) for shape, kind in shapes]
    out_specs = [by_micro(*shape) for shape, _ in shapes]
    out_shape += [jax.ShapeDtypeStruct((micros, length, hidden), low)] * 3
    out_specs += [by_block] * 3
    first = jax.ShapeDtypeStruct((1, length, width), low)
    out_shape += [jax.ShapeDtypeStruct(inputs.shape, low), first]
    out_specs += [whole(inputs), whole(first)]
    return pl.pallas_call(
        functools.partial(forward_kernel, micros),
        grid=(micros, FORWARD_STEPS + 1),
        out_shape=out_shape,
        in_specs=[
            whole(inputs),
            pl.BlockSpec(memory_space=pl.ANY),
            whole(gains),
            whole(tables),
        ]
        + [pl.BlockSpec(memory_space=pl.ANY)] * 7,
        out_specs=out_specs,
        scratch_shapes=[
            pltpu.VMEM((micros, length, width), low),
            pltpu.VMEM((1, length, width), low),
            pltpu.VMEM((1, length, width), low),
            pltpu.VMEM((micros, length, width), low),
            pltpu.VMEM((micros, length, width), low),
            pltpu.VMEM((length, width), low),
            pltpu.VMEM((2, length, width), low),
            pltpu.VMEM((length, width), wide),
            pltpu.VMEM((length, width), wide),
            pltpu.VMEM((length, width), low),
            pltpu.SemaphoreType.DMA((2 * micros, SEND_PIECES)),
            pltpu.SemaphoreType.DMA((2 * micros, SEND_PIECES)),
            pltpu.SemaphoreType.DMA((micros,)),
            pltpu.SemaphoreType.DMA((micros,)),
            pltpu.SemaphoreType.DMA((micros,)),
            pltpu.SemaphoreType.DMA((micros,)),
            pltpu.SemaphoreType.DMA,
            pltpu.SemaphoreType.DMA,
            pltpu.SemaphoreType.DMA,
            pltpu.SemaphoreType.DMA,
            pltpu.SemaphoreType.DMA((1, 4)),
            pltpu.SemaphoreType.DMA((7, FORWARD_STEPS)),
        ]
        + [pltpu.VMEM(item.shape, low) for item in weights],
        compiler_params=pltpu.CompilerParams(
            collective_id=0, has_side_effects=True, vmem_limit_bytes=VMEM_LIMIT
        ),
    )(inputs, cotangents, gains, tables, wq, wk, wv, wo, wg, wu, wd)


def backward(cotangents, other, far_first, gains, tables, n1, record, weights):
    micros, length, width = cotangents.shape
    wq, wk, wv, wo, wg, wu, wd = weights
    groups = wk.shape[1] // HEAD_SIZE
    hidden = wg.shape[1]
    block = hidden // BACKWARD_STEPS
    last = BACKWARD_STEPS - 1
    low, wide = jnp.bfloat16, jnp.float32

    def whole(array):
        return pl.BlockSpec(
            array.shape, lambda m, s: (0,) * array.ndim, pipeline_mode=pl.Buffered(1)
        )

    def by_micro(*shape):
        return pl.BlockSpec((1,) + shape, lambda m, s: (m,) + (0,) * len(shape))

    by_block = pl.BlockSpec((1, length, block), lambda m, s: (m, 0, jnp.minimum(s, last)))
    heads, pairs = wq.shape[1], wk.shape[1]
    half = width // 2
    any_space = pl.BlockSpec(memory_space=pl.ANY)
    columns = [width, half, half, hidden, hidden, heads, pairs, pairs] + [width] * 4
    specs = [by_micro(length, width)] + [by_micro(length, half)] * 2 + [by_block] * 2
    specs += [by_micro(length, heads)] + [by_micro(length, pairs)] * 2 + [any_space] * 4
    out_shape = [jax.ShapeDtypeStruct((micros, length, size), low) for size in columns]
    out_shape.append(jax.ShapeDtypeStruct(gains.shape, wide))
    row = pltpu.SemaphoreType.DMA((micros,))
    swaps = pltpu.SemaphoreType.DMA((2 * micros, SEND_PIECES))
    return pl.pallas_call(
        functools.partial(backward_kernel, micros),
        grid=(micros, BACKWARD_STEPS + 1),
        out_shape=out_shape,
        in_specs=[
            whole(cotangents),
            whole(other),
            any_space,
            whole(gains),
            whole(tables),
            any_space,
            any_space,
            by_micro(length, width),
            by_micro(groups, 2 * length, LANES),
            by_micro(groups, length, LANES),
            by_micro(groups, length, LANES),
            by_micro(length, width),
            by_block,
            by_block,
        ]
        + [any_space] * 7,
        out_specs=specs + [whole(gains)],
        scratch_shapes=[pltpu.VMEM(item.shape, low) for item in weights]
        + [
            pltpu.VMEM((micros, length, width), low),
            pltpu.VMEM((micros, length, width), low),
            pltpu.VMEM((2 * micros, length, width), low),
            pltpu.VMEM((micros, length, width), low),
            pltpu.VMEM(gains.shape, wide),
            pltpu.VMEM((length, width), low),
            pltpu.VMEM((length, width), low),
            pltpu.VMEM((groups, length, 2 * length), low),
            pltpu.VMEM((length, width), low),
            pltpu.VMEM((2, length, width), low),
            pltpu.VMEM((length, width), wide),
            pltpu.VMEM((length, width), wide),
            swaps,
            swaps,
            row,
            row,
            row,
            row,
            pltpu.SemaphoreType.DMA((2 * micros, 4)),
            pltpu.SemaphoreType.DMA,
            pltpu.SemaphoreType.DMA,
            pltpu.SemaphoreType.DMA((7, BACKWARD_STEPS)),
            pltpu.SemaphoreType.DMA((4, micros)),
            pltpu.SemaphoreType.DMA,
        ],
        compiler_params=pltpu.CompilerParams(
            collective_id=1, has_side_effects=True, vmem_limit_bytes=VMEM_LIMIT
        ),
    )(cotangents, other, far_first, gains, tables, n1, record[4], *record, wq, wk, wv, wo, wg, wu, wd)


BLOCKS = 8
PART = 3 * LANES
LAG = 3


class Halving:
    def __init__(self, bits, local, got, sems, outputs):
        self.bits, self.local, self.got, self.sems, self.outputs = bits, local, got, sems, outputs
        me = lax.axis_index("dp")
        self.own = [lax.rem(lax.div(me, 2**bit), 2) for bit in range(bits)]
        self.flip = [me + (1 - 2 * self.own[bit]) * 2**bit for bit in range(bits)]
        plain = list(range(bits))
        self.orders = [plain, [1, 0] + plain[2:] if bits > 1 else plain]

    def copy(self, block, half, level):
        order = self.orders[half]
        done, now = order[:level], order[level]
        spot = []
        for bit in reversed(range(self.bits)):
            if bit in done:
                spot.append(self.own[bit])
            else:
                spot.append(1 - self.own[bit] if bit == now else slice(None))
        return pltpu.make_async_remote_copy(
            src_ref=self.local.at[(block, half) + tuple(spot)],
            dst_ref=self.got[level].at[block, half],
            send_sem=self.sems.at[block, half, level, 0],
            recv_sem=self.sems.at[block, half, level, 1],
            device_id={"dp": self.flip[now]},
            device_id_type=MESH,
        )

    def begin(self, block):
        for half in range(2):
            self.copy(block, half, 0).start()

    def advance(self, block, level):
        for half in range(2):
            order = self.orders[half]
            self.copy(block, half, level).wait()
            done = order[: level + 1]
            left = [bit for bit in reversed(range(self.bits)) if bit not in done]
            rows = self.local.shape[-2]
            piece = 64 if rows % 64 == 0 else rows
            for combo in range(2 ** len(left)):
                fixed = {bit: (combo >> index) & 1 for index, bit in enumerate(left)}
                from_spot = (block, half) + tuple(fixed[bit] for bit in left)
                for bit in done:
                    fixed[bit] = self.own[bit]
                spot = (block, half) + tuple(fixed[bit] for bit in reversed(range(self.bits)))

                def add(index, _):
                    where = pl.ds(pl.multiple_of(index * piece, piece), piece)
                    a = self.local[spot + (where, slice(None))].astype(jnp.float32)
                    b = self.got[level][from_spot + (where, slice(None))].astype(jnp.float32)
                    if level == self.bits - 1:
                        self.outputs(block, half, where, (a + b).astype(jnp.bfloat16))
                    else:
                        self.local[spot + (where, slice(None))] = (a + b).astype(jnp.bfloat16)
                    return 0

                lax.fori_loop(0, rows // piece, add, 0)
            if level < self.bits - 1:
                self.copy(block, half, level + 1).start()


def gradient_kernel(
    bits,
    micros,
    late,
    n2_rows,
    g_rows,
    act_own,
    dgate_own,
    dup_own,
    n2_far,
    g_far,
    gains,
    tables,
    gain_in,
    wg,
    wu,
    wd,
    *refs,
):
    heads_in, late_in, refs = refs[:4], refs[4 : 4 + late], refs[4 + late :]
    outs, refs = refs[:8], refs[8:]
    late_refs, refs = refs[:late], refs[late:]
    heads_own, late_sems, refs = refs[0], refs[1], refs[2:]
    moves, at = list(zip(late_in, late_refs)), 0
    for source in heads_in:
        moves.append((source, heads_own.at[:, at : at + source.shape[1]]))
        at += source.shape[1]
    kept = [
        pltpu.make_async_copy(source, target, late_sems.at[index])
        for index, (source, target) in enumerate(moves)
    ]
    gradient_steps(
        bits,
        micros,
        kept,
        *late_refs[:2],
        heads_own,
        *late_refs[2:],
        n2_rows,
        g_rows,
        act_own,
        dgate_own,
        dup_own,
        n2_far,
        g_far,
        gains,
        tables,
        gain_in,
        wg,
        wu,
        wd,
        *outs,
        *refs,
    )


def gradient_steps(
    bits,
    micros,
    kept,
    n1_rows,
    low_rows,
    heads_own,
    n1_far,
    middle_far,
    wq,
    wk,
    wv,
    wo,
    n2_rows,
    g_rows,
    act_own,
    dgate_own,
    dup_own,
    n2_far,
    g_far,
    gains,
    tables,
    gain_in,
    wg,
    wu,
    wd,
    gate_out,
    up_out,
    down_out,
    q_out,
    k_out,
    v_out,
    o_out,
    gain_out,
    acc,
    send,
    swapped,
    heads_far,
    small,
    small_got,
    local,
    *rest,
):
    step = pl.program_id(0)
    got = rest[:bits]
    sems, small_sems, send_sem, recv_sem = rest[bits:]
    tensor = lax.axis_index("tensor")
    tokens, width = g_far.shape
    length = tokens // micros
    rows = local.shape[-2]
    lanes = half_lanes(width)
    count = local.shape[0]
    swap = Exchange(0, send, swapped, send_sem, recv_sem)

    def output(block, half, where, value):
        if isinstance(block, int):
            target, at = [
                [(q_out, 0), (q_out, PART)],
                [(k_out, 0), (v_out, 0)],
                [(o_out, 0), (o_out, PART)],
            ][block - BLOCKS][half]
            target[where, at : at + PART] = value
        else:
            at = pl.ds(pl.multiple_of(block * 2 * LANES + half * LANES, LANES), LANES)
            for index, target in enumerate((gate_out, up_out, down_out)):
                target[where, at] = value[:, index * LANES : (index + 1) * LANES]

    halving = Halving(bits, local, got, sems, output)

    def gain_copy(level):
        return pltpu.make_async_remote_copy(
            src_ref=small.at[level],
            dst_ref=small_got.at[level],
            send_sem=small_sems.at[level, 0],
            recv_sem=small_sems.at[level, 1],
            device_id={"dp": halving.flip[level]},
            device_id_type=MESH,
        )

    @pl.when(step == 0)
    def _():
        for copy in kept:
            copy.start()
        greet([{"tensor": 1 - tensor}] + [{"dp": halving.flip[bit]} for bit in range(bits)])
        small[0] = gain_in[:, lanes]
        gain_copy(0).start()

    def blocked(value):
        return value.astype(jnp.bfloat16).reshape((2,) * bits + (rows, value.shape[1]))

    @pl.when(step < BLOCKS)
    def _():
        n2, g = n2_far[...], g_far[...]
        gate, up = dot(n2, wg[...]), dot(n2, wu[...])
        d_act = dot(g, wd[...])
        sig = jax.nn.sigmoid(gate)
        act = (gate * sig * up).astype(jnp.bfloat16)
        d_gate = (d_act * up * sig * (1.0 + gate * (1.0 - sig))).astype(jnp.bfloat16)
        d_up = (d_act * gate * sig).astype(jnp.bfloat16)
        parts = (
            (n2_rows, dgate_own, n2_far, d_gate),
            (n2_rows, dup_own, n2_far, d_up),
            (g_rows, act_own, g_far, act),
        )
        for index, (left, right, left_far, right_far) in enumerate(parts):
            total = over_rows(left[...], right[...]) + over_rows(left_far[:, lanes], right_far)
            for half in range(2):
                spot = (step, half) + (slice(None),) * (bits + 1)
                local[spot + (slice(index * LANES, (index + 1) * LANES),)] = blocked(
                    total[:, half * LANES : (half + 1) * LANES]
                )
        halving.begin(step)

        product = times_t(d_gate, wg[...]) + times_t(d_up, wu[...])

        @pl.when(step == 0)
        def _():
            acc[...] = product

        @pl.when((step > 0) & (step < BLOCKS - 1))
        def _():
            acc[...] += product

        @pl.when(step == BLOCKS - 1)
        def _():
            for piece in range(SEND_PIECES):
                part = slice(piece * swap.width, (piece + 1) * swap.width)
                swap.start(piece, acc[:, part] + product[:, part])

    @pl.when(step == BLOCKS)
    def _():
        for copy in kept:
            copy.wait()
        swap.wait()
        for which in range(micros):
            part = slice(which * length, (which + 1) * length)
            d_normed = send[part, :].astype(jnp.float32) + swapped[0, part, :].astype(jnp.float32)
            mid = middle_far[part, :].astype(jnp.float32)
            scale = rsqrt_mean(mid)
            weighted = d_normed * gains[1:2, :]
            inner = jnp.mean(weighted * mid, axis=-1, keepdims=True)
            total = g_far[part, :].astype(jnp.float32) + scale * weighted - mid * (scale**3 * inner)
            send[part, :] = total.astype(jnp.bfloat16)

    @pl.when((step >= BLOCKS) & (step < BLOCKS + micros))
    def _():
        which = step - BLOCKS
        part = pl.ds(pl.multiple_of(which * length, length), length)
        n1 = n1_far[part, :]
        query, keys, values = dot(n1, wq[...]), dot(n1, wk[...]), dot(n1, wv[...])
        d_mixed = dot(send[part, :], wo[...]).astype(jnp.bfloat16).astype(jnp.float32)
        trig, causal = trig_and_mask(tables, length)
        cosine, sine, cosine2, sine2 = trig
        d_queries, d_keys, d_values, outs = [], [], [], []
        for group in range(wk.shape[1] // HEAD_SIZE):
            q = jnp.concatenate([spread(query, 2 * group), spread(query, 2 * group + 1)], axis=0)
            q = turned(q, cosine2, sine2).astype(jnp.bfloat16)
            k = turned(spread(keys, group), cosine, sine).astype(jnp.bfloat16)
            v = spread(values, group).astype(jnp.bfloat16)
            probs = attention_weights(q, k, causal)
            parts = attention_backward(d_mixed, group, q, k, v, trig, probs, True)
            d_queries += parts[0]
            d_keys.append(parts[1])
            d_values.append(parts[2])
            outs += parts[3]
        at = 0
        for item in (d_queries, d_keys, d_values, outs):
            item = gathered(item).astype(jnp.bfloat16)
            heads_far[part, at : at + item.shape[1]] = item
            at += item.shape[1]

    @pl.when(step >= LAG)
    def _():
        halving.advance(step - LAG, 0)

    @pl.when(step == BLOCKS + micros)
    def _():
        def head_gradients(block, left, left_far):
            for half in range(2):
                at = pl.ds(pl.multiple_of((2 * (block - BLOCKS) + half) * PART, PART), PART)
                local[block, half] = blocked(
                    over_rows(left[...], heads_own[:, at]) + over_rows(left_far, heads_far[:, at])
                )
            halving.begin(block)
            return 0

        lax.fori_loop(
            BLOCKS, count - 1, lambda block, _: head_gradients(block, n1_rows, n1_far[:, lanes]), 0
        )
        head_gradients(count - 1, low_rows, send[:, lanes])
        for level in range(bits):
            gain_copy(level).wait()
            summed = small[level] + small_got[level]
            if level < bits - 1:
                small[level + 1] = summed
                gain_copy(level + 1).start()
            else:
                gain_out[...] = summed
        for level in range(1, bits):

            def advanced(block, _):
                halving.advance(block, level)
                return 0

            lax.fori_loop(0, BLOCKS, advanced, 0)
        for level in range(bits):
            for block in range(BLOCKS, count):
                halving.advance(block, level)


def gradients(bits, own, far, gains, tables, gain, weights):
    wq, wk, wv, wo, wg, wu, wd = weights
    n1_rows, n2_rows, g_rows, low_rows, act, d_gate, d_up, d_q, d_k, d_v, mixed = own
    micros = n1_rows.shape[0]
    hidden, width = wg.shape[1], wg.shape[0]
    block = hidden // BLOCKS
    rows = width // 2 ** (bits + 1)
    low = jnp.bfloat16
    total = d_q.shape[2] + d_k.shape[2] + d_v.shape[2] + mixed.shape[2]
    count = BLOCKS + total // (2 * PART)

    def whole(array):
        return pl.BlockSpec(array.shape, lambda s: (0,) * array.ndim, pipeline_mode=pl.Buffered(1))

    def streamed(array):
        return pl.BlockSpec((array.shape[0], block), lambda s: (0, jnp.minimum(s, BLOCKS - 1)))

    def flat(values):
        return values.reshape(-1, values.shape[-1])

    n1_far, n2_far, g_far, middle_far = (flat(item) for item in far)
    args = [(flat(item), whole) for item in (n2_rows, g_rows)]
    args += [(flat(item), streamed) for item in (act, d_gate, d_up)]
    args += [(item, whole) for item in (n2_far, g_far, gains, tables, gain)]
    args += [(item, streamed) for item in (wg, wu, wd)]
    heads = [flat(item) for item in (d_q, d_k, d_v, mixed)]
    late = [flat(item) for item in (n1_rows, low_rows)] + [n1_far, middle_far, wq, wk, wv, wo]
    sizes = [hidden] * 3 + [d_q.shape[2], d_k.shape[2], d_v.shape[2], mixed.shape[2]]
    out_shape = [jax.ShapeDtypeStruct((rows, size), low) for size in sizes]
    out_shape.append(jax.ShapeDtypeStruct((2, width // 2), jnp.float32))
    tokens = args[0][0].shape[0]
    scratch = [pltpu.VMEM(item.shape, low) for item in late]
    scratch += [
        pltpu.VMEM((tokens, total), low),
        pltpu.SemaphoreType.DMA((len(late) + len(heads),)),
        pltpu.VMEM((tokens, width), jnp.float32),
        pltpu.VMEM((tokens, width), low),
        pltpu.VMEM((1, tokens, width), low),
        pltpu.VMEM((tokens, total), low),
        pltpu.VMEM((bits, 2, width // 2), jnp.float32),
        pltpu.VMEM((bits, 2, width // 2), jnp.float32),
        pltpu.VMEM((count, 2) + (2,) * bits + (rows, PART), low),
    ]
    for level in range(bits):
        scratch.append(pltpu.VMEM((count, 2) + (2,) * (bits - 1 - level) + (rows, PART), low))
    scratch += [
        pltpu.SemaphoreType.DMA((count, 2, bits, 2)),
        pltpu.SemaphoreType.DMA((bits, 2)),
        pltpu.SemaphoreType.DMA((1, SEND_PIECES)),
        pltpu.SemaphoreType.DMA((1, SEND_PIECES)),
    ]
    return pl.pallas_call(
        functools.partial(gradient_kernel, bits, micros, len(late)),
        grid=(BLOCKS + micros + 1,),
        out_shape=out_shape,
        in_specs=[spec(array) for array, spec in args]
        + [pl.BlockSpec(memory_space=pl.ANY)] * (len(heads) + len(late)),
        out_specs=[whole(shape) for shape in out_shape],
        scratch_shapes=scratch,
        compiler_params=pltpu.CompilerParams(
            collective_id=2, has_side_effects=True, vmem_limit_bytes=VMEM_LIMIT
        ),
    )(*(array for array, _ in args), *heads, *late)


def finished(shards, plain):
    items = list(shards) + list(plain)
    kinds = [jnp.float32] * len(shards) + [jnp.bfloat16] * len(plain)
    steps = 4

    def kernel(*refs):
        for source, target in zip(refs[: len(items)], refs[len(items) :]):
            target[...] = source[...].astype(target.dtype)

    def spec(item):
        rows = item.shape[0]
        block = rows // steps if rows % (16 * steps) == 0 else 16
        return pl.BlockSpec(
            (block, item.shape[1]), lambda s: (jnp.minimum(s, rows // block - 1), 0)
        )

    return pl.pallas_call(
        kernel,
        grid=(steps,),
        out_shape=[jax.ShapeDtypeStruct(item.shape, kind) for item, kind in zip(items, kinds)],
        in_specs=[spec(item) for item in items],
        out_specs=[spec(item) for item in items],
    )(*items)


def body(
    inputs,
    cotangents,
    norm_scales,
    w_query,
    key_weight,
    value_weight,
    w_out,
    w_gate,
    w_up,
    down_weight,
):
    weights = (
        w_query[0],
        key_weight[0],
        value_weight[0],
        w_out[0],
        w_gate[0],
        w_up[0],
        down_weight[0],
    )
    _, _, length, width = inputs.shape
    gains = norm_scales[0].T
    tables = jnp.asarray(rope_tables(length))
    cots = cotangents[:, 0]
    (
        result,
        hidden,
        n1,
        q,
        k,
        v,
        mixed,
        middle,
        n1_rows,
        n2_rows,
        gate,
        up,
        act,
        other,
        far_first,
    ) = forward(inputs[:, 0], cots, gains, tables, weights)
    grad, g_rows, low_rows, d_gate, d_up, d_q, d_k, d_v, n1_far, n2_far, g_far, middle_far, gain = backward(
        cots, other, far_first, gains, tables, n1, (hidden, q, k, v, middle, gate, up), weights
    )
    peers = lax.axis_size("dp")
    *shards, gain = gradients(
        peers.bit_length() - 2,
        (n1_rows, n2_rows, g_rows, low_rows, act, d_gate, d_up, d_q, d_k, d_v, mixed),
        (n1_far, n2_far, g_far, middle_far),
        gains,
        tables,
        gain,
        weights,
    )
    (
        grad_gate,
        grad_up,
        grad_down,
        grad_query,
        grad_key,
        grad_value,
        grad_proj,
        result,
        grad,
    ) = (item[None] for item in finished(shards, [result.reshape(-1, width), grad.reshape(-1, width)]))
    rows = width // peers
    at = lax.rem(lax.axis_index("dp"), peers // 2) * rows
    grad_scales = lax.dynamic_slice_in_dim(gain, at, rows, 1).T[None]
    return (
        result.reshape(1, -1, 1, length, width),
        grad.reshape(1, -1, 1, length, width),
        grad_scales,
        grad_query,
        grad_key,
        grad_value,
        grad_proj,
        grad_gate,
        grad_up,
        grad_down,
    )


def solution(mesh):
    placed = (
        P(None, "dp", None, None),
        P(None, "dp", None, None),
        P("pipe", None, None),
        P("pipe", None, "tensor"),
        P("pipe", None, "tensor"),
        P("pipe", None, "tensor"),
        P("pipe", None, "tensor"),
        P("pipe", None, "tensor"),
        P("pipe", None, "tensor"),
        P("pipe", None, "tensor"),
    )
    return jax.shard_map(
        body,
        mesh=mesh,
        in_specs=placed,
        out_specs=(
            P("pipe", None, "dp", None, None),
            P("pipe", None, "dp", None, None),
            P("pipe", "dp", None),
            P("pipe", "dp", "tensor"),
            P("pipe", "dp", "tensor"),
            P("pipe", "dp", "tensor"),
            P("pipe", "dp", "tensor"),
            P("pipe", "dp", "tensor"),
            P("pipe", "dp", "tensor"),
            P("pipe", "dp", "tensor"),
        ),
        check_vma=False,
    )
```

```python
import functools

import jax
import jax.numpy as jnp
import numpy as np
from jax import lax
from jax.experimental import pallas as pl
from jax.experimental.pallas import tpu as pltpu
from jax.sharding import PartitionSpec as P

HEAD_SIZE = 96
HALF = HEAD_SIZE // 2
LANES = 128
FORWARD_STEPS = 2
BACKWARD_STEPS = 2
SEND_PIECES = 3

EPS = 1e-05
THETA = 100000.0
MESH = pl.DeviceIdType.MESH
VMEM_LIMIT = 67043328
SCALE = HEAD_SIZE ** (-0.5)


def rope_tables(length):
    freqs = (THETA ** (-(np.arange(HALF, dtype=np.float64) * 2.0 / HEAD_SIZE))).astype(np.float32)
    angles = np.arange(length, dtype=np.float32)[:, None] * freqs[None, :]
    cosine, sine = np.cos(angles), np.sin(angles)
    room = np.zeros((length, LANES // 2 - HALF), np.float32)
    return np.concatenate([cosine, room, sine, room], axis=1).astype(np.float32)


def dot(left, right):
    return lax.dot_general(
        left, right, (((1,), (0,)), ((), ())), preferred_element_type=jnp.float32
    )


def times_t(left, right):
    return lax.dot_general(
        left, right, (((1,), (1,)), ((), ())), preferred_element_type=jnp.float32
    )


def over_rows(left, right):
    return lax.dot_general(
        left, right, (((0,), (0,)), ((), ())), preferred_element_type=jnp.float32
    )


def spread(values, head):
    room = jnp.zeros((values.shape[0], LANES // 2 - HALF), values.dtype)
    at = head * HEAD_SIZE
    return jnp.concatenate(
        [values[:, at : at + HALF], room, values[:, at + HALF : at + HEAD_SIZE], room], axis=1
    )


def gathered(heads):
    parts = []
    for head in heads:
        parts += [head[:, :HALF], head[:, LANES // 2 : LANES // 2 + HALF]]
    return jnp.concatenate(parts, axis=1)


def turned(values, cosine, sine):
    return values * cosine + pltpu.roll(values, LANES // 2, 1) * sine


def turned_back(values, cosine, sine):
    return values * cosine - pltpu.roll(values, LANES // 2, 1) * sine


def rsqrt_mean(values):
    return lax.rsqrt(jnp.mean(values * values, axis=-1, keepdims=True) + EPS)


class Exchange:
    def __init__(self, number, send, got, send_sem, recv_sem):
        self.number, self.send, self.got = number, send, got
        self.send_sem, self.recv_sem = send_sem, recv_sem
        self.width = send.shape[1] // SEND_PIECES
        self.slot = lax.rem(number, got.shape[0])

    def copy(self, piece):
        columns = pl.ds(piece * self.width, self.width)
        return pltpu.make_async_remote_copy(
            src_ref=self.send.at[:, columns],
            dst_ref=self.got.at[self.slot, :, columns],
            send_sem=self.send_sem.at[self.number, piece],
            recv_sem=self.recv_sem.at[self.number, piece],
            device_id={"tensor": 1 - lax.axis_index("tensor")},
            device_id_type=MESH,
        )

    def start(self, piece, partial_value):
        columns = pl.ds(piece * self.width, self.width)
        self.send[:, columns] = partial_value.astype(jnp.bfloat16)
        self.copy(piece).start()

    def wait(self):
        for piece in range(SEND_PIECES):
            self.copy(piece).wait()

    def total(self):
        return self.send[...].astype(jnp.float32) + self.got[self.slot].astype(jnp.float32)


def half_copy(source, target, rows, send_sem, recv_sem, device):
    return pltpu.make_async_remote_copy(
        src_ref=source.at[rows],
        dst_ref=target.at[rows],
        send_sem=send_sem,
        recv_sem=recv_sem,
        device_id=device,
        device_id_type=MESH,
    )


def passed_on(xin, micro, sems, stage_from, meanwhile=None):
    tensor = lax.axis_index("tensor")
    rows = xin.shape[1] // 2
    send_sem, recv_sem, pair_send, pair_recv = sems
    slot = xin.at[micro]
    mine = pl.ds(pl.multiple_of(tensor * rows, rows), rows)
    theirs = pl.ds(pl.multiple_of((1 - tensor) * rows, rows), rows)
    half_copy(
        slot, slot, mine, send_sem.at[micro], recv_sem.at[micro], {"pipe": stage_from}
    ).wait_recv()
    copy = half_copy(
        slot, slot, mine, pair_send.at[micro], pair_recv.at[micro], {"tensor": 1 - tensor}
    )
    copy.start()
    if meanwhile:
        meanwhile()
    half_copy(
        slot, slot, theirs, pair_send.at[micro], pair_recv.at[micro], {"tensor": 1 - tensor}
    ).wait_recv()
    copy.wait_send()


def sent_on(source, xin, micro, sems, stage_to):
    tensor = lax.axis_index("tensor")
    rows = xin.shape[1] // 2
    mine = pl.ds(pl.multiple_of(tensor * rows, rows), rows)
    return half_copy(
        source.at[micro], xin.at[micro], mine, sems[0].at[micro], sems[1].at[micro], {"pipe": stage_to}
    )


class Resident:
    def __init__(self, sources, targets, sems, steps):
        attention, hidden = range(4), range(4, len(sources))
        block = targets[4].shape[1] // steps
        self.copies = {}
        for index in attention:
            self.copies[index, 0] = pltpu.make_async_copy(
                sources[index], targets[index], sems.at[index, 0]
            )
        for index in hidden:
            for step in range(steps):
                columns = pl.ds(step * block, block)
                self.copies[index, step] = pltpu.make_async_copy(
                    sources[index].at[:, columns], targets[index].at[:, columns], sems.at[index, step]
                )
        self.parts = {"attention": [(index, 0) for index in attention]}
        for step in range(steps):
            self.parts[step] = [(index, step) for index in hidden]

    def start(self, *parts):
        for part in parts:
            for key in self.parts[part]:
                self.copies[key].start()

    def wait(self, part):
        for key in self.parts[part]:
            self.copies[key].wait()


def half_lanes(width):
    top = lax.div(lax.axis_index("dp"), lax.axis_size("dp") // 2)
    return pl.ds(pl.multiple_of(top * (width // 2), LANES), width // 2)


def greet(devices):
    barrier = pltpu.get_barrier_semaphore()
    for device in devices:
        pl.semaphore_signal(barrier, inc=1, device_id=device, device_id_type=MESH)
    pl.semaphore_wait(barrier, len(devices))


class FarCopies:
    def __init__(self, sources, buffers, sems, partner):
        self.sources, self.buffers, self.sems, self.partner = sources, buffers, sems, partner
        tensor = lax.axis_index("tensor")
        self.pair = {"tensor": 1 - tensor}
        rows = buffers.shape[1] // 2
        self.mine = pl.ds(pl.multiple_of(tensor * rows, rows), rows)
        self.theirs = pl.ds(pl.multiple_of((1 - tensor) * rows, rows), rows)

    def far(self, which, source=None):
        source = self.sources.at[which] if source is None else source
        sems = self.sems.at[which, 0], self.sems.at[which, 1]
        return half_copy(source, self.buffers.at[which], self.mine, *sems, {"dp": self.partner})

    def near(self, which, rows):
        slot = self.buffers.at[which]
        sems = self.sems.at[which, 2], self.sems.at[which, 3]
        return half_copy(slot, slot, rows, *sems, self.pair)

    def start(self, which, source=None):
        self.far(which, source).start()

    def receive(self, which):
        self.far(which, self.buffers.at[which]).wait()
        self.near(which, self.mine).start()
        self.near(which, self.theirs).wait_recv()
        self.near(which, self.mine).wait_send()


def forward_kernel(
    micros,
    inp,
    cot,
    gains,
    tables,
    *refs,
):
    weights_in, refs = refs[:7], refs[7:]
    forward_steps(micros, inp, cot, gains, tables, weights_in, *refs)


def forward_steps(
    micros,
    inp,
    cot,
    gains,
    tables,
    weights_in,
    result_out,
    hidden_out,
    n1_out,
    q_out,
    k_out,
    v_out,
    o_out,
    middle_out,
    n1_rows,
    n2_rows,
    gate_out,
    up_out,
    act_out,
    other_out,
    far_out,
    other,
    first_buf,
    far_buf,
    xin,
    res,
    send,
    got,
    middle,
    acc,
    n2_buf,
    send_sem,
    recv_sem,
    x_send,
    x_recv,
    xp_send,
    xp_recv,
    far_send,
    far_recv,
    near_send,
    near_recv,
    far_sems,
    weight_sems,
    wq,
    wk,
    wv,
    wo,
    wg,
    wu,
    wd,
):
    micro, step = pl.program_id(0), pl.program_id(1)
    pipe, tensor, data = lax.axis_index("pipe"), lax.axis_index("tensor"), lax.axis_index("dp")
    peers = lax.axis_size("dp")
    partner = lax.rem(data + peers // 2, peers)
    sems = (x_send, x_recv, xp_send, xp_recv)
    length = inp.shape[1]
    lanes = half_lanes(inp.shape[2])

    def far_copy(source):
        return pltpu.make_async_remote_copy(
            src_ref=source.at[tensor],
            dst_ref=other.at[tensor],
            send_sem=far_send,
            recv_sem=far_recv,
            device_id={"dp": partner},
            device_id_type=MESH,
        )

    def near_copy(which):
        return pltpu.make_async_remote_copy(
            src_ref=other.at[which],
            dst_ref=other.at[which],
            send_sem=near_send,
            recv_sem=near_recv,
            device_id={"tensor": 1 - tensor},
            device_id_type=MESH,
        )

    far = FarCopies(first_buf, far_buf, far_sems, partner)

    resident = Resident(weights_in, (wq, wk, wv, wo, wg, wu, wd), weight_sems, FORWARD_STEPS)

    @pl.when((micro == 0) & (step == 0))
    def _():
        resident.start("attention", *range(FORWARD_STEPS))
        greet([{"tensor": 1 - tensor}, {"pipe": 1 - pipe}, {"dp": partner}])

        @pl.when(pipe == 0)
        def _():
            far_copy(inp).start()

        @pl.when(pipe == 1)
        def _():
            far_copy(cot).start()

    @pl.when((micro == 0) & (step == 0))
    def _():
        resident.wait("attention")

    for number in range(FORWARD_STEPS):

        @pl.when((micro == 0) & (step == number + 1))
        def _():
            resident.wait(number)

    @pl.when(step == 0)
    def _():
        @pl.when(pipe == 0)
        def _():
            hidden_out[0] = inp[micro]

        @pl.when(pipe == 1)
        def _():
            passed_on(xin, micro, sems, 0)
            hidden_out[0] = xin[micro]

        wide = hidden_out[0].astype(jnp.float32)
        n1 = (wide * rsqrt_mean(wide) * gains[0:1, :]).astype(jnp.bfloat16)
        n1_out[0] = n1
        n1_rows[0] = n1_out[0, :, lanes]

        @pl.when((pipe == 1) & (micro == 0))
        def _():
            first_buf[0] = n1
            far.start(0)

        query = dot(n1, wq[...])
        keys = dot(n1, wk[...])
        values = dot(n1, wv[...])
        trig, causal = trig_and_mask(tables, length)
        cosine, sine, cosine2, sine2 = trig
        groups = k_out.shape[1]
        outs = []
        for group in range(groups):
            q = jnp.concatenate([spread(query, 2 * group), spread(query, 2 * group + 1)], axis=0)
            q = turned(q, cosine2, sine2).astype(jnp.bfloat16)
            k = turned(spread(keys, group), cosine, sine).astype(jnp.bfloat16)
            v = spread(values, group).astype(jnp.bfloat16)
            q_out[0, group] = q
            k_out[0, group] = k
            v_out[0, group] = v
            weights = jnp.where(causal, jnp.exp(times_t(k, q) * SCALE), 0.0)
            total = jnp.sum(weights, axis=0, keepdims=True)
            probs = (weights * (1.0 / total)).astype(jnp.bfloat16)
            mixed = over_rows(probs, v)
            outs += [mixed[:length], mixed[length:]]
        mixed = gathered(outs).astype(jnp.bfloat16)
        o_out[0] = mixed
        swap = Exchange(2 * micro, send, got, send_sem, recv_sem)
        for piece in range(SEND_PIECES):
            swap.start(piece, times_t(mixed, wo[piece * swap.width : (piece + 1) * swap.width, :]))
        swap.wait()
        both = hidden_out[0].astype(jnp.float32) + swap.total()
        middle[...] = both
        middle_low = both.astype(jnp.bfloat16)
        middle_out[0] = middle_low
        n2 = (both * rsqrt_mean(both) * gains[1:2, :]).astype(jnp.bfloat16)
        n2_buf[...] = n2
        n2_rows[0] = n2_buf[:, lanes]

        @pl.when((pipe == 0) & (micro == 0))
        def _():
            first_buf[0] = middle_low
            far.start(0)


    @pl.when(step > 0)
    def _():
        n2 = n2_buf[...]
        block = wg.shape[1] // FORWARD_STEPS
        columns = pl.ds(pl.multiple_of((step - 1) * block, block), block)
        gate = dot(n2, wg[:, columns])
        up = dot(n2, wu[:, columns])
        act = (gate * jax.nn.sigmoid(gate) * up).astype(jnp.bfloat16)
        gate_out[0] = gate.astype(jnp.bfloat16)
        up_out[0] = up.astype(jnp.bfloat16)
        act_out[0] = act
        product = times_t(act, wd[:, columns])

        @pl.when(step == 1)
        def _():
            acc[...] = product

        @pl.when((step > 1) & (step < FORWARD_STEPS))
        def _():
            acc[...] += product

        @pl.when(step == FORWARD_STEPS)
        def _():
            swap = Exchange(2 * micro + 1, send, got, send_sem, recv_sem)
            for piece in range(SEND_PIECES):
                part = slice(piece * swap.width, (piece + 1) * swap.width)
                swap.start(piece, acc[:, part] + product[:, part])
            swap.wait()
            result = (middle[...] + swap.total()).astype(jnp.bfloat16)
            result_out[0] = result

            @pl.when(pipe == 0)
            def _():
                res[micro] = result
                sent_on(res, xin, micro, sems, 1).start()


    @pl.when((micro == micros - 1) & (step == FORWARD_STEPS))
    def _():
        far_copy(inp).wait()
        near_copy(tensor).start()
        near_copy(1 - tensor).wait_recv()
        near_copy(tensor).wait_send()
        other_out[...] = other[...]
        far.receive(0)
        far_out[...] = far_buf[...]

    @pl.when((pipe == 0) & (micro == micros - 1) & (step == FORWARD_STEPS))
    def _():
        for which in range(micros):
            sent_on(res, xin, which, sems, 1).wait_send()


def attention_backward(d_mixed, group, q, k, v, trig, causal, with_output):
    cosine, sine, cosine2, sine2 = trig
    d_head = jnp.concatenate(
        [spread(d_mixed, 2 * group), spread(d_mixed, 2 * group + 1)], axis=0
    ).astype(jnp.bfloat16)
    weights = jnp.where(causal, jnp.exp(times_t(k, q) * SCALE), 0.0)
    probs = weights * (1.0 / jnp.sum(weights, axis=0, keepdims=True))
    moved = probs * times_t(v, d_head)
    delta = jnp.sum(moved, axis=0, keepdims=True)
    d_scores = ((moved - probs * delta) * SCALE).astype(jnp.bfloat16)
    rounded = probs.astype(jnp.bfloat16)
    d_value = dot(rounded, d_head)
    d_key = turned_back(dot(d_scores, q), cosine, sine)
    d_query = turned_back(over_rows(d_scores, k), cosine2, sine2)
    length = k.shape[0]
    mixed = over_rows(rounded, v) if with_output else d_query
    return (
        [d_query[:length], d_query[length:]],
        d_key,
        d_value,
        [mixed[:length], mixed[length:]],
    )


def backward_kernel(
    micros,
    cot,
    other,
    far_first,
    gains,
    tables,
    n1_own,
    middle_own,
    hidden,
    q_in,
    k_in,
    v_in,
    middle,
    gate_in,
    up_in,
    *refs,
):
    weights_in, refs = refs[:7], refs[7:]
    backward_steps(
        micros,
        cot,
        other,
        far_first,
        gains,
        tables,
        n1_own,
        middle_own,
        hidden,
        q_in,
        k_in,
        v_in,
        middle,
        gate_in,
        up_in,
        weights_in,
        *refs,
    )


def backward_steps(
    micros,
    cot,
    other,
    far_first,
    gains,
    tables,
    n1_own,
    middle_own,
    hidden,
    q_in,
    k_in,
    v_in,
    middle,
    gate_in,
    up_in,
    weights_in,
    grad_out,
    g_rows,
    low_rows,
    dgate_out,
    dup_out,
    dq_out,
    dk_out,
    dv_out,
    n1_far,
    n2_far,
    g_far,
    middle_far,
    gain_out,
    wq,
    wk,
    wv,
    wo,
    wg,
    wu,
    wd,
    xin,
    res,
    far_buf,
    n2_buf,
    far_gain,
    g_buf,
    low_buf,
    send,
    got,
    d_middle,
    acc,
    send_sem,
    recv_sem,
    x_send,
    x_recv,
    xp_send,
    xp_recv,
    far_sems,
    gain_send,
    gain_recv,
    in_sems,
    out_sems,
):
    micro, step = pl.program_id(0), pl.program_id(1)
    pipe, tensor, data = lax.axis_index("pipe"), lax.axis_index("tensor"), lax.axis_index("dp")
    peers = lax.axis_size("dp")
    partner = lax.rem(data + peers // 2, peers)
    sems = (x_send, x_recv, xp_send, xp_recv)
    length = hidden.shape[1]
    lanes = half_lanes(hidden.shape[2])
    last = micros - 1
    far = FarCopies(xin, far_buf, far_sems, partner)

    def gain_copy():
        return pltpu.make_async_remote_copy(
            src_ref=gain_out,
            dst_ref=far_gain,
            send_sem=gain_send,
            recv_sem=gain_recv,
            device_id={"dp": partner},
            device_id_type=MESH,
        )

    resident = Resident(weights_in, (wq, wk, wv, wo, wg, wu, wd), in_sems, BACKWARD_STEPS)

    def write(kind, which, source):
        target = (n1_far, n2_far, g_far, middle_far)[kind]
        return pltpu.make_async_copy(source, target.at[which], out_sems.at[kind, which])

    def far_middle(which, source):
        write(3, which, source).start()
        mid = source[...].astype(jnp.float32)
        n2_buf[which] = (mid * rsqrt_mean(mid) * gains[1:2, :]).astype(jnp.bfloat16)
        write(1, which, n2_buf.at[which]).start()

    @pl.when((micro == 0) & (step == 0))
    def _():
        resident.start(*range(BACKWARD_STEPS), "attention")
        greet([{"tensor": 1 - tensor}, {"pipe": 1 - pipe}, {"dp": partner}])
        gain_out[...] = jnp.zeros_like(gain_out)

        @pl.when(pipe == 1)
        def _():
            for which in range(micros):
                if which:
                    far.start(which, n1_own.at[which])
                far.start(micros + which, middle_own.at[which])
            write(0, 0, far_first.at[0]).start()
            for which in range(micros):
                write(2, which, other.at[which]).start()

        @pl.when(pipe == 0)
        def _():
            for which in range(1, micros):
                far.start(micros + which, middle_own.at[which])
            far_middle(0, far_first.at[0])
            for which in range(micros):
                wide = other[which].astype(jnp.float32)
                res[which] = (wide * rsqrt_mean(wide) * gains[0:1, :]).astype(jnp.bfloat16)
                write(0, which, res.at[which]).start()

    @pl.when(step == 0)
    def _():
        @pl.when(pipe == 1)
        def _():
            g_buf[...] = cot[micro]

        @pl.when(pipe == 0)
        def _():
            passed_on(xin, micro, sems, 1, lambda: far.start(micro))
            g_buf[...] = xin[micro]

        g_rows[0] = g_buf[:, lanes]

    @pl.when((micro == 0) & (step == BACKWARD_STEPS))
    def _():
        resident.wait("attention")

    for number in range(BACKWARD_STEPS):

        @pl.when((micro == 0) & (step == number))
        def _():
            resident.wait(number)

    @pl.when(step < BACKWARD_STEPS)
    def _():
        gate, up = gate_in[0].astype(jnp.float32), up_in[0].astype(jnp.float32)
        block = wg.shape[1] // BACKWARD_STEPS
        columns = pl.ds(pl.multiple_of(step * block, block), block)
        d_act = dot(g_buf[...], wd[:, columns])
        sig = jax.nn.sigmoid(gate)
        d_gate = (d_act * up * sig * (1.0 + gate * (1.0 - sig))).astype(jnp.bfloat16)
        d_up = (d_act * gate * sig).astype(jnp.bfloat16)
        dgate_out[0] = d_gate
        dup_out[0] = d_up

        product = times_t(d_gate, wg[:, columns]) + times_t(d_up, wu[:, columns])

        @pl.when(step == 0)
        def _():
            acc[...] = product

        @pl.when((step > 0) & (step < BACKWARD_STEPS - 1))
        def _():
            acc[...] += product

        @pl.when(step == BACKWARD_STEPS - 1)
        def _():
            swap = Exchange(2 * micro, send, got, send_sem, recv_sem)
            for piece in range(SEND_PIECES):
                part = slice(piece * swap.width, (piece + 1) * swap.width)
                swap.start(piece, acc[:, part] + product[:, part])
            swap.wait()
            d_normed = swap.total()
            mid = middle[0].astype(jnp.float32)
            scale = rsqrt_mean(mid)
            gain_out[1:2, :] += jnp.sum(d_normed * mid * scale, axis=0, keepdims=True)
            weighted = d_normed * gains[1:2, :]
            inner = jnp.mean(weighted * mid, axis=-1, keepdims=True)
            total = g_buf[...].astype(jnp.float32) + scale * weighted - mid * (scale**3 * inner)
            d_middle[...] = total
            low_buf[...] = total.astype(jnp.bfloat16)
            low_rows[0] = low_buf[:, lanes]

    @pl.when(step == BACKWARD_STEPS)
    def _():
        d_mixed = dot(low_buf[...], wo[...]).astype(jnp.bfloat16).astype(jnp.float32)
        trig, causal = trig_and_mask(tables, length)
        d_queries, d_keys, d_values = [], [], []
        for group in range(k_in.shape[1]):
            parts = attention_backward(
                d_mixed, group, q_in[0, group], k_in[0, group], v_in[0, group], trig, causal, False
            )
            d_queries += parts[0]
            d_keys.append(parts[1])
            d_values.append(parts[2])
        d_query = gathered(d_queries).astype(jnp.bfloat16)
        d_key = gathered(d_keys).astype(jnp.bfloat16)
        d_value = gathered(d_values).astype(jnp.bfloat16)
        dq_out[0] = d_query
        dk_out[0] = d_key
        dv_out[0] = d_value
        swap = Exchange(2 * micro + 1, send, got, send_sem, recv_sem)
        for piece in range(SEND_PIECES):
            part = slice(piece * swap.width, (piece + 1) * swap.width)
            swap.start(
                piece,
                times_t(d_query, wq[part, :]) + times_t(d_key, wk[part, :]) + times_t(d_value, wv[part, :]),
            )
        swap.wait()
        d_first = swap.total()
        wide = hidden[0].astype(jnp.float32)
        scale = rsqrt_mean(wide)
        gain_out[0:1, :] += jnp.sum(d_first * wide * scale, axis=0, keepdims=True)
        weighted = d_first * gains[0:1, :]
        inner = jnp.mean(weighted * wide, axis=-1, keepdims=True)
        d_hidden = (d_middle[...] + scale * weighted - wide * (scale**3 * inner)).astype(jnp.bfloat16)
        grad_out[0] = d_hidden

        @pl.when(pipe == 1)
        def _():
            res[micro] = d_hidden
            sent_on(res, xin, micro, sems, 0).start()

        @pl.when(micro == last)
        def _():
            gain_copy().start()
            for which in range(1, micros):
                far.receive(micros + which)
                far_middle(which, far_buf.at[micros + which])

            @pl.when(pipe == 1)
            def _():
                far.receive(micros)
                far_middle(0, far_buf.at[micros])
                for which in range(1, micros):
                    far.receive(which)
                    write(0, which, far_buf.at[which]).start()

            @pl.when(pipe == 0)
            def _():
                for which in range(micros):
                    far.receive(which)
                    write(2, which, far_buf.at[which]).start()

            for kind in range(4):
                for which in range(micros):
                    write(kind, which, far_buf.at[which]).wait()
            gain_copy().wait()
            gain_out[...] += far_gain[...]

            @pl.when(pipe == 1)
            def _():
                for which in range(micros):
                    sent_on(res, xin, which, sems, 0).wait_send()


def trig_and_mask(tables, length):
    both = tables[...]
    swapped = pltpu.roll(both, LANES // 2, 1)
    first = lax.broadcasted_iota(jnp.int32, both.shape, 1) < LANES // 2
    cosine, sine = jnp.where(first, both, swapped), jnp.where(first, -swapped, both)
    trig = (
        cosine,
        sine,
        jnp.concatenate([cosine, cosine], axis=0),
        jnp.concatenate([sine, sine], axis=0),
    )
    at_k = lax.broadcasted_iota(jnp.int32, (length, 2 * length), 0)
    at_q = lax.rem(lax.broadcasted_iota(jnp.int32, (length, 2 * length), 1), length)
    return trig, at_q >= at_k


def forward(inputs, cotangents, gains, tables, weights):
    micros, length, width = inputs.shape
    wq, wk, wv, wo, wg, wu, wd = weights
    groups = wk.shape[1] // HEAD_SIZE
    hidden = wg.shape[1]
    block = hidden // FORWARD_STEPS
    low, wide = jnp.bfloat16, jnp.float32

    def whole(array):
        return pl.BlockSpec(
            array.shape, lambda m, s: (0,) * array.ndim, pipeline_mode=pl.Buffered(1)
        )

    def by_micro(*shape):
        return pl.BlockSpec((1,) + shape, lambda m, s: (m,) + (0,) * len(shape))

    by_block = pl.BlockSpec((1, length, block), lambda m, s: (m, 0, jnp.maximum(s - 1, 0)))
    shapes = [
        ((length, width), low),
        ((length, width), low),
        ((length, width), low),
        ((groups, 2 * length, LANES), low),
        ((groups, length, LANES), low),
        ((groups, length, LANES), low),
        ((length, wq.shape[1]), low),
        ((length, width), low),
        ((length, width // 2), low),
        ((length, width // 2), low),
    ]
    out_shape = [jax.ShapeDtypeStruct((micros,) + shape, kind) for shape, kind in shapes]
    out_specs = [by_micro(*shape) for shape, _ in shapes]
    out_shape += [jax.ShapeDtypeStruct((micros, length, hidden), low)] * 3
    out_specs += [by_block] * 3
    first = jax.ShapeDtypeStruct((1, length, width), low)
    out_shape += [jax.ShapeDtypeStruct(inputs.shape, low), first]
    out_specs += [whole(inputs), whole(first)]
    return pl.pallas_call(
        functools.partial(forward_kernel, micros),
        grid=(micros, FORWARD_STEPS + 1),
        out_shape=out_shape,
        in_specs=[
            whole(inputs),
            pl.BlockSpec(memory_space=pl.ANY),
            whole(gains),
            whole(tables),
        ]
        + [pl.BlockSpec(memory_space=pl.ANY)] * 7,
        out_specs=out_specs,
        scratch_shapes=[
            pltpu.VMEM((micros, length, width), low),
            pltpu.VMEM((1, length, width), low),
            pltpu.VMEM((1, length, width), low),
            pltpu.VMEM((micros, length, width), low),
            pltpu.VMEM((micros, length, width), low),
            pltpu.VMEM((length, width), low),
            pltpu.VMEM((2, length, width), low),
            pltpu.VMEM((length, width), wide),
            pltpu.VMEM((length, width), wide),
            pltpu.VMEM((length, width), low),
            pltpu.SemaphoreType.DMA((2 * micros, SEND_PIECES)),
            pltpu.SemaphoreType.DMA((2 * micros, SEND_PIECES)),
            pltpu.SemaphoreType.DMA((micros,)),
            pltpu.SemaphoreType.DMA((micros,)),
            pltpu.SemaphoreType.DMA((micros,)),
            pltpu.SemaphoreType.DMA((micros,)),
            pltpu.SemaphoreType.DMA,
            pltpu.SemaphoreType.DMA,
            pltpu.SemaphoreType.DMA,
            pltpu.SemaphoreType.DMA,
            pltpu.SemaphoreType.DMA((1, 4)),
            pltpu.SemaphoreType.DMA((7, FORWARD_STEPS)),
        ]
        + [pltpu.VMEM(item.shape, low) for item in weights],
        compiler_params=pltpu.CompilerParams(
            collective_id=0, has_side_effects=True, vmem_limit_bytes=VMEM_LIMIT
        ),
    )(inputs, cotangents, gains, tables, wq, wk, wv, wo, wg, wu, wd)


def backward(cotangents, other, far_first, gains, tables, n1, record, weights):
    micros, length, width = cotangents.shape
    wq, wk, wv, wo, wg, wu, wd = weights
    groups = wk.shape[1] // HEAD_SIZE
    hidden = wg.shape[1]
    block = hidden // BACKWARD_STEPS
    last = BACKWARD_STEPS - 1
    low, wide = jnp.bfloat16, jnp.float32

    def whole(array):
        return pl.BlockSpec(
            array.shape, lambda m, s: (0,) * array.ndim, pipeline_mode=pl.Buffered(1)
        )

    def by_micro(*shape):
        return pl.BlockSpec((1,) + shape, lambda m, s: (m,) + (0,) * len(shape))

    by_block = pl.BlockSpec((1, length, block), lambda m, s: (m, 0, jnp.minimum(s, last)))
    heads, pairs = wq.shape[1], wk.shape[1]
    half = width // 2
    any_space = pl.BlockSpec(memory_space=pl.ANY)
    columns = [width, half, half, hidden, hidden, heads, pairs, pairs] + [width] * 4
    specs = [by_micro(length, width)] + [by_micro(length, half)] * 2 + [by_block] * 2
    specs += [by_micro(length, heads)] + [by_micro(length, pairs)] * 2 + [any_space] * 4
    out_shape = [jax.ShapeDtypeStruct((micros, length, size), low) for size in columns]
    out_shape.append(jax.ShapeDtypeStruct(gains.shape, wide))
    row = pltpu.SemaphoreType.DMA((micros,))
    swaps = pltpu.SemaphoreType.DMA((2 * micros, SEND_PIECES))
    return pl.pallas_call(
        functools.partial(backward_kernel, micros),
        grid=(micros, BACKWARD_STEPS + 1),
        out_shape=out_shape,
        in_specs=[
            whole(cotangents),
            whole(other),
            whole(far_first),
            whole(gains),
            whole(tables),
            any_space,
            any_space,
            by_micro(length, width),
            by_micro(groups, 2 * length, LANES),
            by_micro(groups, length, LANES),
            by_micro(groups, length, LANES),
            by_micro(length, width),
            by_block,
            by_block,
        ]
        + [any_space] * 7,
        out_specs=specs + [whole(gains)],
        scratch_shapes=[pltpu.VMEM(item.shape, low) for item in weights]
        + [
            pltpu.VMEM((micros, length, width), low),
            pltpu.VMEM((micros, length, width), low),
            pltpu.VMEM((2 * micros, length, width), low),
            pltpu.VMEM((micros, length, width), low),
            pltpu.VMEM(gains.shape, wide),
            pltpu.VMEM((length, width), low),
            pltpu.VMEM((length, width), low),
            pltpu.VMEM((length, width), low),
            pltpu.VMEM((2, length, width), low),
            pltpu.VMEM((length, width), wide),
            pltpu.VMEM((length, width), wide),
            swaps,
            swaps,
            row,
            row,
            row,
            row,
            pltpu.SemaphoreType.DMA((2 * micros, 4)),
            pltpu.SemaphoreType.DMA,
            pltpu.SemaphoreType.DMA,
            pltpu.SemaphoreType.DMA((7, BACKWARD_STEPS)),
            pltpu.SemaphoreType.DMA((4, micros)),
        ],
        compiler_params=pltpu.CompilerParams(
            collective_id=1, has_side_effects=True, vmem_limit_bytes=VMEM_LIMIT
        ),
    )(cotangents, other, far_first, gains, tables, n1, record[4], *record, wq, wk, wv, wo, wg, wu, wd)


BLOCKS = 8
PART = 3 * LANES
LAG = 3


class Halving:
    def __init__(self, bits, local, got, sems, outputs):
        self.bits, self.local, self.got, self.sems, self.outputs = bits, local, got, sems, outputs
        me = lax.axis_index("dp")
        self.own = [lax.rem(lax.div(me, 2**bit), 2) for bit in range(bits)]
        self.flip = [me + (1 - 2 * self.own[bit]) * 2**bit for bit in range(bits)]
        plain = list(range(bits))
        self.orders = [plain, [1, 0] + plain[2:] if bits > 1 else plain]

    def copy(self, block, half, level):
        order = self.orders[half]
        done, now = order[:level], order[level]
        spot = []
        for bit in reversed(range(self.bits)):
            if bit in done:
                spot.append(self.own[bit])
            else:
                spot.append(1 - self.own[bit] if bit == now else slice(None))
        return pltpu.make_async_remote_copy(
            src_ref=self.local.at[(block, half) + tuple(spot)],
            dst_ref=self.got[level].at[block, half],
            send_sem=self.sems.at[block, half, level, 0],
            recv_sem=self.sems.at[block, half, level, 1],
            device_id={"dp": self.flip[now]},
            device_id_type=MESH,
        )

    def begin(self, block):
        for half in range(2):
            self.copy(block, half, 0).start()

    def advance(self, block, level):
        for half in range(2):
            order = self.orders[half]
            self.copy(block, half, level).wait()
            done = order[: level + 1]
            left = [bit for bit in reversed(range(self.bits)) if bit not in done]
            rows = self.local.shape[-2]
            piece = 64 if rows % 64 == 0 else rows
            for combo in range(2 ** len(left)):
                fixed = {bit: (combo >> index) & 1 for index, bit in enumerate(left)}
                from_spot = (block, half) + tuple(fixed[bit] for bit in left)
                for bit in done:
                    fixed[bit] = self.own[bit]
                spot = (block, half) + tuple(fixed[bit] for bit in reversed(range(self.bits)))

                def add(index, _):
                    where = pl.ds(pl.multiple_of(index * piece, piece), piece)
                    a = self.local[spot + (where, slice(None))].astype(jnp.float32)
                    b = self.got[level][from_spot + (where, slice(None))].astype(jnp.float32)
                    if level == self.bits - 1:
                        self.outputs(block, half, where, (a + b).astype(jnp.bfloat16))
                    else:
                        self.local[spot + (where, slice(None))] = (a + b).astype(jnp.bfloat16)
                    return 0

                lax.fori_loop(0, rows // piece, add, 0)
            if level < self.bits - 1:
                self.copy(block, half, level + 1).start()


def gradient_kernel(
    bits,
    micros,
    late,
    n2_rows,
    g_rows,
    act_own,
    dgate_own,
    dup_own,
    n2_far,
    g_far,
    gains,
    tables,
    gain_in,
    wg,
    wu,
    wd,
    *refs,
):
    heads_in, late_in, refs = refs[:4], refs[4 : 4 + late], refs[4 + late :]
    outs, refs = refs[:8], refs[8:]
    late_refs, refs = refs[:late], refs[late:]
    heads_own, late_sems, refs = refs[0], refs[1], refs[2:]
    moves, at = list(zip(late_in, late_refs)), 0
    for source in heads_in:
        moves.append((source, heads_own.at[:, at : at + source.shape[1]]))
        at += source.shape[1]
    kept = [
        pltpu.make_async_copy(source, target, late_sems.at[index])
        for index, (source, target) in enumerate(moves)
    ]
    gradient_steps(
        bits,
        micros,
        kept,
        *late_refs[:2],
        heads_own,
        *late_refs[2:],
        n2_rows,
        g_rows,
        act_own,
        dgate_own,
        dup_own,
        n2_far,
        g_far,
        gains,
        tables,
        gain_in,
        wg,
        wu,
        wd,
        *outs,
        *refs,
    )


def gradient_steps(
    bits,
    micros,
    kept,
    n1_rows,
    low_rows,
    heads_own,
    n1_far,
    middle_far,
    wq,
    wk,
    wv,
    wo,
    n2_rows,
    g_rows,
    act_own,
    dgate_own,
    dup_own,
    n2_far,
    g_far,
    gains,
    tables,
    gain_in,
    wg,
    wu,
    wd,
    gate_out,
    up_out,
    down_out,
    q_out,
    k_out,
    v_out,
    o_out,
    gain_out,
    acc,
    send,
    swapped,
    heads_far,
    small,
    small_got,
    local,
    *rest,
):
    step = pl.program_id(0)
    got = rest[:bits]
    sems, small_sems, send_sem, recv_sem = rest[bits:]
    tensor = lax.axis_index("tensor")
    tokens, width = g_far.shape
    length = tokens // micros
    rows = local.shape[-2]
    lanes = half_lanes(width)
    count = local.shape[0]
    swap = Exchange(0, send, swapped, send_sem, recv_sem)

    def output(block, half, where, value):
        if isinstance(block, int):
            target, at = [
                [(q_out, 0), (q_out, PART)],
                [(k_out, 0), (v_out, 0)],
                [(o_out, 0), (o_out, PART)],
            ][block - BLOCKS][half]
            target[where, at : at + PART] = value
        else:
            at = pl.ds(pl.multiple_of(block * 2 * LANES + half * LANES, LANES), LANES)
            for index, target in enumerate((gate_out, up_out, down_out)):
                target[where, at] = value[:, index * LANES : (index + 1) * LANES]

    halving = Halving(bits, local, got, sems, output)

    def gain_copy(level):
        return pltpu.make_async_remote_copy(
            src_ref=small.at[level],
            dst_ref=small_got.at[level],
            send_sem=small_sems.at[level, 0],
            recv_sem=small_sems.at[level, 1],
            device_id={"dp": halving.flip[level]},
            device_id_type=MESH,
        )

    @pl.when(step == 0)
    def _():
        for copy in kept:
            copy.start()
        greet([{"tensor": 1 - tensor}] + [{"dp": halving.flip[bit]} for bit in range(bits)])
        small[0] = gain_in[:, lanes]
        gain_copy(0).start()

    def blocked(value):
        return value.astype(jnp.bfloat16).reshape((2,) * bits + (rows, value.shape[1]))

    @pl.when(step < BLOCKS)
    def _():
        n2, g = n2_far[...], g_far[...]
        gate, up = dot(n2, wg[...]), dot(n2, wu[...])
        d_act = dot(g, wd[...])
        sig = jax.nn.sigmoid(gate)
        act = (gate * sig * up).astype(jnp.bfloat16)
        d_gate = (d_act * up * sig * (1.0 + gate * (1.0 - sig))).astype(jnp.bfloat16)
        d_up = (d_act * gate * sig).astype(jnp.bfloat16)
        parts = (
            (n2_rows, dgate_own, n2_far, d_gate),
            (n2_rows, dup_own, n2_far, d_up),
            (g_rows, act_own, g_far, act),
        )
        for index, (left, right, left_far, right_far) in enumerate(parts):
            total = over_rows(left[...], right[...]) + over_rows(left_far[:, lanes], right_far)
            for half in range(2):
                spot = (step, half) + (slice(None),) * (bits + 1)
                local[spot + (slice(index * LANES, (index + 1) * LANES),)] = blocked(
                    total[:, half * LANES : (half + 1) * LANES]
                )
        halving.begin(step)

        product = times_t(d_gate, wg[...]) + times_t(d_up, wu[...])

        @pl.when(step == 0)
        def _():
            acc[...] = product

        @pl.when((step > 0) & (step < BLOCKS - 1))
        def _():
            acc[...] += product

        @pl.when(step == BLOCKS - 1)
        def _():
            for piece in range(SEND_PIECES):
                part = slice(piece * swap.width, (piece + 1) * swap.width)
                swap.start(piece, acc[:, part] + product[:, part])

    @pl.when(step == BLOCKS)
    def _():
        for copy in kept:
            copy.wait()
        swap.wait()
        for which in range(micros):
            part = slice(which * length, (which + 1) * length)
            d_normed = send[part, :].astype(jnp.float32) + swapped[0, part, :].astype(jnp.float32)
            mid = middle_far[part, :].astype(jnp.float32)
            scale = rsqrt_mean(mid)
            weighted = d_normed * gains[1:2, :]
            inner = jnp.mean(weighted * mid, axis=-1, keepdims=True)
            total = g_far[part, :].astype(jnp.float32) + scale * weighted - mid * (scale**3 * inner)
            send[part, :] = total.astype(jnp.bfloat16)

    @pl.when((step >= BLOCKS) & (step < BLOCKS + micros))
    def _():
        which = step - BLOCKS
        part = pl.ds(pl.multiple_of(which * length, length), length)
        n1 = n1_far[part, :]
        query, keys, values = dot(n1, wq[...]), dot(n1, wk[...]), dot(n1, wv[...])
        d_mixed = dot(send[part, :], wo[...]).astype(jnp.bfloat16).astype(jnp.float32)
        trig, causal = trig_and_mask(tables, length)
        cosine, sine, cosine2, sine2 = trig
        d_queries, d_keys, d_values, outs = [], [], [], []
        for group in range(wk.shape[1] // HEAD_SIZE):
            q = jnp.concatenate([spread(query, 2 * group), spread(query, 2 * group + 1)], axis=0)
            q = turned(q, cosine2, sine2).astype(jnp.bfloat16)
            k = turned(spread(keys, group), cosine, sine).astype(jnp.bfloat16)
            v = spread(values, group).astype(jnp.bfloat16)
            parts = attention_backward(d_mixed, group, q, k, v, trig, causal, True)
            d_queries += parts[0]
            d_keys.append(parts[1])
            d_values.append(parts[2])
            outs += parts[3]
        at = 0
        for item in (d_queries, d_keys, d_values, outs):
            item = gathered(item).astype(jnp.bfloat16)
            heads_far[part, at : at + item.shape[1]] = item
            at += item.shape[1]

    @pl.when(step >= LAG)
    def _():
        halving.advance(step - LAG, 0)

    @pl.when(step == BLOCKS + micros)
    def _():
        def head_gradients(block, left, left_far):
            for half in range(2):
                at = pl.ds(pl.multiple_of((2 * (block - BLOCKS) + half) * PART, PART), PART)
                local[block, half] = blocked(
                    over_rows(left[...], heads_own[:, at]) + over_rows(left_far, heads_far[:, at])
                )
            halving.begin(block)
            return 0

        lax.fori_loop(
            BLOCKS, count - 1, lambda block, _: head_gradients(block, n1_rows, n1_far[:, lanes]), 0
        )
        head_gradients(count - 1, low_rows, send[:, lanes])
        for level in range(bits):
            gain_copy(level).wait()
            summed = small[level] + small_got[level]
            if level < bits - 1:
                small[level + 1] = summed
                gain_copy(level + 1).start()
            else:
                gain_out[...] = summed
        for level in range(1, bits):

            def advanced(block, _):
                halving.advance(block, level)
                return 0

            lax.fori_loop(0, BLOCKS, advanced, 0)
        for level in range(bits):
            for block in range(BLOCKS, count):
                halving.advance(block, level)


def gradients(bits, own, far, gains, tables, gain, weights):
    wq, wk, wv, wo, wg, wu, wd = weights
    n1_rows, n2_rows, g_rows, low_rows, act, d_gate, d_up, d_q, d_k, d_v, mixed = own
    micros = n1_rows.shape[0]
    hidden, width = wg.shape[1], wg.shape[0]
    block = hidden // BLOCKS
    rows = width // 2 ** (bits + 1)
    low = jnp.bfloat16
    total = d_q.shape[2] + d_k.shape[2] + d_v.shape[2] + mixed.shape[2]
    count = BLOCKS + total // (2 * PART)

    def whole(array):
        return pl.BlockSpec(array.shape, lambda s: (0,) * array.ndim, pipeline_mode=pl.Buffered(1))

    def streamed(array):
        return pl.BlockSpec((array.shape[0], block), lambda s: (0, jnp.minimum(s, BLOCKS - 1)))

    def flat(values):
        return values.reshape(-1, values.shape[-1])

    n1_far, n2_far, g_far, middle_far = (flat(item) for item in far)
    args = [(flat(item), whole) for item in (n2_rows, g_rows)]
    args += [(flat(item), streamed) for item in (act, d_gate, d_up)]
    args += [(item, whole) for item in (n2_far, g_far, gains, tables, gain)]
    args += [(item, streamed) for item in (wg, wu, wd)]
    heads = [flat(item) for item in (d_q, d_k, d_v, mixed)]
    late = [flat(item) for item in (n1_rows, low_rows)] + [n1_far, middle_far, wq, wk, wv, wo]
    sizes = [hidden] * 3 + [d_q.shape[2], d_k.shape[2], d_v.shape[2], mixed.shape[2]]
    out_shape = [jax.ShapeDtypeStruct((rows, size), low) for size in sizes]
    out_shape.append(jax.ShapeDtypeStruct((2, width // 2), jnp.float32))
    tokens = args[0][0].shape[0]
    scratch = [pltpu.VMEM(item.shape, low) for item in late]
    scratch += [
        pltpu.VMEM((tokens, total), low),
        pltpu.SemaphoreType.DMA((len(late) + len(heads),)),
        pltpu.VMEM((tokens, width), jnp.float32),
        pltpu.VMEM((tokens, width), low),
        pltpu.VMEM((1, tokens, width), low),
        pltpu.VMEM((tokens, total), low),
        pltpu.VMEM((bits, 2, width // 2), jnp.float32),
        pltpu.VMEM((bits, 2, width // 2), jnp.float32),
        pltpu.VMEM((count, 2) + (2,) * bits + (rows, PART), low),
    ]
    for level in range(bits):
        scratch.append(pltpu.VMEM((count, 2) + (2,) * (bits - 1 - level) + (rows, PART), low))
    scratch += [
        pltpu.SemaphoreType.DMA((count, 2, bits, 2)),
        pltpu.SemaphoreType.DMA((bits, 2)),
        pltpu.SemaphoreType.DMA((1, SEND_PIECES)),
        pltpu.SemaphoreType.DMA((1, SEND_PIECES)),
    ]
    return pl.pallas_call(
        functools.partial(gradient_kernel, bits, micros, len(late)),
        grid=(BLOCKS + micros + 1,),
        out_shape=out_shape,
        in_specs=[spec(array) for array, spec in args]
        + [pl.BlockSpec(memory_space=pl.ANY)] * (len(heads) + len(late)),
        out_specs=[whole(shape) for shape in out_shape],
        scratch_shapes=scratch,
        compiler_params=pltpu.CompilerParams(
            collective_id=2, has_side_effects=True, vmem_limit_bytes=VMEM_LIMIT
        ),
    )(*(array for array, _ in args), *heads, *late)


def finished(shards, plain):
    items = list(shards) + list(plain)
    kinds = [jnp.float32] * len(shards) + [jnp.bfloat16] * len(plain)
    steps = 4

    def kernel(*refs):
        for source, target in zip(refs[: len(items)], refs[len(items) :]):
            target[...] = source[...].astype(target.dtype)

    def spec(item):
        rows = item.shape[0]
        block = rows // steps if rows % (16 * steps) == 0 else 16
        return pl.BlockSpec(
            (block, item.shape[1]), lambda s: (jnp.minimum(s, rows // block - 1), 0)
        )

    return pl.pallas_call(
        kernel,
        grid=(steps,),
        out_shape=[jax.ShapeDtypeStruct(item.shape, kind) for item, kind in zip(items, kinds)],
        in_specs=[spec(item) for item in items],
        out_specs=[spec(item) for item in items],
    )(*items)


def body(
    inputs,
    cotangents,
    norm_scales,
    w_query,
    key_weight,
    value_weight,
    w_out,
    w_gate,
    w_up,
    down_weight,
):
    weights = (
        w_query[0],
        key_weight[0],
        value_weight[0],
        w_out[0],
        w_gate[0],
        w_up[0],
        down_weight[0],
    )
    _, _, length, width = inputs.shape
    gains = norm_scales[0].T
    tables = jnp.asarray(rope_tables(length))
    cots = cotangents[:, 0]
    (
        result,
        hidden,
        n1,
        q,
        k,
        v,
        mixed,
        middle,
        n1_rows,
        n2_rows,
        gate,
        up,
        act,
        other,
        far_first,
    ) = forward(inputs[:, 0], cots, gains, tables, weights)
    grad, g_rows, low_rows, d_gate, d_up, d_q, d_k, d_v, n1_far, n2_far, g_far, middle_far, gain = backward(
        cots, other, far_first, gains, tables, n1, (hidden, q, k, v, middle, gate, up), weights
    )
    peers = lax.axis_size("dp")
    *shards, gain = gradients(
        peers.bit_length() - 2,
        (n1_rows, n2_rows, g_rows, low_rows, act, d_gate, d_up, d_q, d_k, d_v, mixed),
        (n1_far, n2_far, g_far, middle_far),
        gains,
        tables,
        gain,
        weights,
    )
    (
        grad_gate,
        grad_up,
        grad_down,
        grad_query,
        grad_key,
        grad_value,
        grad_proj,
        result,
        grad,
    ) = (item[None] for item in finished(shards, [result.reshape(-1, width), grad.reshape(-1, width)]))
    rows = width // peers
    at = lax.rem(lax.axis_index("dp"), peers // 2) * rows
    grad_scales = lax.dynamic_slice_in_dim(gain, at, rows, 1).T[None]
    return (
        result.reshape(1, -1, 1, length, width),
        grad.reshape(1, -1, 1, length, width),
        grad_scales,
        grad_query,
        grad_key,
        grad_value,
        grad_proj,
        grad_gate,
        grad_up,
        grad_down,
    )


def solution(mesh):
    placed = (
        P(None, "dp", None, None),
        P(None, "dp", None, None),
        P("pipe", None, None),
        P("pipe", None, "tensor"),
        P("pipe", None, "tensor"),
        P("pipe", None, "tensor"),
        P("pipe", None, "tensor"),
        P("pipe", None, "tensor"),
        P("pipe", None, "tensor"),
        P("pipe", None, "tensor"),
    )
    return jax.shard_map(
        body,
        mesh=mesh,
        in_specs=placed,
        out_specs=(
            P("pipe", None, "dp", None, None),
            P("pipe", None, "dp", None, None),
            P("pipe", "dp", None),
            P("pipe", "dp", "tensor"),
            P("pipe", "dp", "tensor"),
            P("pipe", "dp", "tensor"),
            P("pipe", "dp", "tensor"),
            P("pipe", "dp", "tensor"),
            P("pipe", "dp", "tensor"),
            P("pipe", "dp", "tensor"),
        ),
        check_vma=False,
    )
```
